32 devices in a mesh: section: 4 (over x, core), expert: 8 (over z, y).
Axes of the slice: x: 2, y: 2, z: 4, core: 2. Of those that a mesh axis runs over, the one named last changes fastest.
Arguments:
- x_fwd: bfloat16 [4, 1024, 3584], P('section', 'expert'), may hold values from -6 to 6
- routes_fwd: int32 [4, 1024, 2], P('section', 'expert'), may hold values from 0 to 3, all different within a row; in each aligned block of 128 rows (0 to 127, 128 to 255, ..., all dimensions but the last counted through in order) at most 96 rows name the same one
- affinity_fwd: float32 [4, 1024, 2], P('section', 'expert'), may hold values from 0.1 to 1
- x_bwd: bfloat16 [4, 1024, 3584], P('section', 'expert'), may hold values from -6 to 6
- grad_bwd: bfloat16 [4, 1024, 3584], P('section', 'expert'), may hold values from -6 to 6
- routes_bwd: int32 [4, 1024, 2], P('section', 'expert'), may hold values from 0 to 3, all different within a row; in each aligned block of 128 rows (0 to 127, 128 to 255, ..., all dimensions but the last counted through in order) at most 96 rows name the same one
- affinity_bwd: float32 [4, 1024, 2], P('section', 'expert'), may hold values from 0.1 to 1
- up_weight: bfloat16 [4, 3584, 4096], P('section', None, 'expert'), may hold values from -0.09375 to 0.09375
- down_weight: bfloat16 [4, 4096, 3584], P('section', 'expert'), may hold values from -0.1875 to 0.1875
Outputs:
- fwd_next: bfloat16 [4, 1024, 3584], P('section', 'expert')
- bwd_next: bfloat16 [4, 1024, 3584], P('section', 'expert')
The draws below stay inside these ranges and needn't reach their ends.
Inputs may be any that keep to these rules, and one draw needn't show every extreme that they name: `routes_fwd`: each row names 2 different experts; in each section, among the 128 rows of one device (aligned blocks), no expert is named more than 96 times, a bound that some block reaches. `routes_bwd`: each row names 2 different experts; in each section, among the 128 rows of one device (aligned blocks), no expert is named more than 96 times, a bound that some block reaches.
All inputs are finite; a program needn't handle non-finite values.
Results may differ from the reference program's by a relative error of at most 0.0041.
Values may be sent and summed in bfloat16 or wider, within the bound.
A program may use at most 128 MiB of HBM per device.

```python
import math
import jax
import jax.numpy as jnp
import numpy as np
from jax import lax

D = 3584
HID = 1024
TOP = 2
TOK_DEV = 128
SECTIONS = 4
EXPERTS = 4
TOKENS = 1024
CAP = 96
N_EXPERT = 8


def steps_of(key, shape, split, least, high):
    level, own = 1.0, jax.random.fold_in(key, 6)
    for position, shards_of in split:
        steps = jnp.exp(jax.random.uniform(jax.random.fold_in(own, position), (shards_of,), jnp.float32, least / len(split), high / len(split)))
        level = level * jnp.repeat(steps, shape[position] // shards_of).reshape([-1 if axis == position else 1 for axis in range(len(shape))])
    return level


def assign_block(stream_key, own, number, rows, count, top, limit, lean):
    sequence = jax.random.permutation(stream_key, count)
    crowded, ordinary = portions_of(count, rows * top, limit, lean, True), portions_of(count, rows * top, limit, lean, False)
    places = jnp.arange(count)

    def named(tallies, rotation):
        used = int((tallies > 0).sum())
        fixed = max(1, used // 4)
        passed = fixed + (places - fixed + rotation * (used - fixed)) % max(1, count - fixed)
        return jnp.zeros((count,), jnp.int32).at[sequence[jnp.where(places < fixed, places, passed)]].set(jnp.asarray(tallies, jnp.int32))

    tallies = jnp.where(number % 4 == 0, named(crowded, number // 4), named(ordinary, number - number // 4 - 1))
    mixed = jax.random.permutation(jax.random.fold_in(own, 3), count)
    giver, sink = mixed[0:count // 2 * 2:2], mixed[1:count // 2 * 2:2]
    slack = jnp.minimum(tallies[giver] - 1, limit - tallies[sink]) // 2
    slack = jnp.where((giver == sequence[0]) | (sink == sequence[0]) | (tallies[sink] == 0), 0, jnp.maximum(slack, 0))
    passed = jax.random.randint(jax.random.fold_in(own, 4), (count // 2,), 0, 1 << 20) % (slack + 1)
    tallies = tallies.at[giver].add(-passed).at[sink].add(passed)
    labels = jnp.searchsorted(jnp.cumsum(tallies), jnp.arange(rows * top), side="right").astype(jnp.int32)
    listing = labels.reshape(top, rows).T
    listing = listing[jax.random.permutation(jax.random.fold_in(own, 1), rows)]
    rotation = jax.random.randint(jax.random.fold_in(own, 2), (rows, 1), 0, top)
    return jnp.take_along_axis(listing, (jnp.arange(top)[None, :] + rotation) % top, axis=1)


def portions_of(count, total, limit, skew, full):
    portions = [(1 << 20) // math.isqrt(standing ** skew) + 1 for standing in range(1, count + 1)]
    largest = limit if full else min(limit, max(-(-total // count), total * portions[0] // sum(portions)))
    least = 1 if total - largest >= count - 1 else 0
    holding, surplus = [largest] + [least] * (count - 1), total - largest - least * (count - 1)
    while surplus > 0:
        free = [i for i in range(1, count) if holding[i] < largest] or [i for i in range(1, count) if holding[i] < limit]
        whole, left = sum([portions[i] for i in free]), surplus
        for i in free:
            extra = min(limit - holding[i], max(1, left * portions[i] // whole), surplus)
            holding[i] = holding[i] + extra
            surplus = surplus - extra
    return np.array(holding)


def gaussian(key, dims, deviation, bound, split=(), kind=jnp.bfloat16):
    array = deviation * jax.random.normal(key, dims, jnp.float32)
    if split:
        array = array * steps_of(key, dims, split, -0.22, 0.18)
    return jnp.clip(array, -bound, bound).astype(kind)


def setup_inputs(seed: int = 0) -> dict:
    keys = jax.random.split(jax.random.key(seed), 10)
    x_fwd = gaussian(keys[0], (SECTIONS, TOKENS, D), 1.0, 6.0, ((0, 4), (1, 8)))
    routes_fwd_keys = jax.random.split(jax.random.fold_in(keys[1], 1), SECTIONS * TOKENS // TOK_DEV)
    routes_fwd_turns = jax.random.permutation(jax.random.fold_in(keys[1], 3), SECTIONS * TOKENS // TOK_DEV)
    routes_fwd = jax.vmap(lambda own, number: assign_block(jax.random.fold_in(keys[1], 2), own, number, TOK_DEV, EXPERTS, TOP, CAP, 2))(routes_fwd_keys, routes_fwd_turns).reshape((SECTIONS, TOKENS, TOP))
    affinity_fwd = jnp.clip(jnp.exp(math.log(1.0) - 2.3025851 * jax.random.uniform(keys[2], (SECTIONS, TOKENS, TOP), jnp.float32) ** steps_of(keys[2], (SECTIONS, TOKENS, TOP), ((0, 4), (1, 8)), -0.2, 0.2)), 0.1, 1.0)
    x_bwd = gaussian(keys[3], (SECTIONS, TOKENS, D), 1.0, 6.0, ((0, 4), (1, 8)))
    grad_bwd = gaussian(keys[4], (SECTIONS, TOKENS, D), 1.0, 6.0, ((0, 4), (1, 8)))
    routes_bwd_keys = jax.random.split(jax.random.fold_in(keys[5], 1), SECTIONS * TOKENS // TOK_DEV)
    routes_bwd_turns = jax.random.permutation(jax.random.fold_in(keys[5], 3), SECTIONS * TOKENS // TOK_DEV)
    routes_bwd = jax.vmap(lambda own, number: assign_block(jax.random.fold_in(keys[5], 2), own, number, TOK_DEV, EXPERTS, TOP, CAP, 2))(routes_bwd_keys, routes_bwd_turns).reshape((SECTIONS, TOKENS, TOP))
    affinity_bwd = jnp.clip(jnp.exp(math.log(1.0) - 2.3025851 * jax.random.uniform(keys[6], (SECTIONS, TOKENS, TOP), jnp.float32) ** steps_of(keys[6], (SECTIONS, TOKENS, TOP), ((0, 4), (1, 8)), -0.2, 0.2)), 0.1, 1.0)
    up_weight = gaussian(keys[7], (SECTIONS, D, EXPERTS * HID), D ** -0.5, 0.09375, ((0, 4), (2, 8)))
    down_weight = gaussian(keys[8], (SECTIONS, EXPERTS * HID, D), HID ** -0.5, 0.1875, ((0, 4), (1, 8)))
    return {"x_fwd": x_fwd, "routes_fwd": routes_fwd, "affinity_fwd": affinity_fwd, "x_bwd": x_bwd, "grad_bwd": grad_bwd, "routes_bwd": routes_bwd, "affinity_bwd": affinity_bwd, "up_weight": up_weight, "down_weight": down_weight}


def silu_grad(values):
    sigma = jax.nn.sigmoid(values)
    return sigma * (1.0 + values * (1.0 - sigma))

def expert_pass(rows_fwd, rows_saved, rows_grad, up_block, down_block):
    half_count = HID // 2
    sums_fwd = jnp.zeros((rows_fwd.shape[0], D), jnp.float32)
    sums_bwd = jnp.zeros((rows_fwd.shape[0], D), jnp.float32)
    for half_id in range(2):
        up_part = up_block[:, half_id * half_count:(half_id + 1) * half_count]
        down_part = down_block[half_id * half_count:(half_id + 1) * half_count, :]
        hidden = jax.nn.silu(jnp.dot(rows_fwd, up_part, preferred_element_type=jnp.float32)).astype(jnp.bfloat16)
        part_fwd = jnp.dot(hidden, down_part, preferred_element_type=jnp.float32).astype(jnp.bfloat16)
        pre_act = jnp.dot(rows_saved, up_part, preferred_element_type=jnp.float32)
        hidden_grad = jnp.dot(rows_grad, down_part.T, preferred_element_type=jnp.float32)
        pre_grad = (hidden_grad * silu_grad(pre_act)).astype(jnp.bfloat16)
        part_bwd = jnp.dot(pre_grad, up_part.T, preferred_element_type=jnp.float32).astype(jnp.bfloat16)
        sums_fwd = sums_fwd + part_fwd.astype(jnp.float32)
        sums_bwd = sums_bwd + part_bwd.astype(jnp.float32)
    return (sums_fwd.astype(jnp.bfloat16), sums_bwd.astype(jnp.bfloat16))

def combine(inputs, results, affinity):
    weights = affinity / lax.optimization_barrier(jnp.sum(affinity, -1, keepdims=True))
    routed = results.reshape(TOKENS, TOP, D).astype(jnp.float32)
    return (inputs.astype(jnp.float32) + lax.optimization_barrier(jnp.sum(weights[..., None] * routed, 1))).astype(jnp.bfloat16)

def reference(x_fwd, routes_fwd, affinity_fwd, x_bwd, grad_bwd, routes_bwd, affinity_bwd, up_weight, down_weight):
    total = TOKENS * TOP
    rows = N_EXPERT * CAP
    zero_row = jnp.zeros((1, D), jnp.bfloat16)
    layer_outs = []
    input_grads = []
    for section_id in range(SECTIONS):
        inputs_fwd = jnp.concatenate([x_fwd[section_id], zero_row], 0)
        inputs_saved = jnp.concatenate([x_bwd[section_id], zero_row], 0)
        inputs_grad = jnp.concatenate([grad_bwd[section_id], zero_row], 0)
        flat_fwd = routes_fwd[section_id].reshape(-1)
        flat_bwd = routes_bwd[section_id].reshape(-1)
        up_section = up_weight[section_id]
        down_section = down_weight[section_id]

        def one_expert(carry, expert_id):
            results_fwd, results_bwd = carry
            index_fwd = jnp.nonzero(flat_fwd == expert_id, size=rows, fill_value=total)[0].astype(jnp.int32)
            index_bwd = jnp.nonzero(flat_bwd == expert_id, size=rows, fill_value=total)[0].astype(jnp.int32)
            up_block = lax.dynamic_slice_in_dim(up_section, (expert_id * HID).astype(jnp.int32), HID, 1)
            down_block = lax.dynamic_slice_in_dim(down_section, (expert_id * HID).astype(jnp.int32), HID, 0)
            token_fwd = index_fwd // TOP
            token_bwd = index_bwd // TOP
            outs_fwd, outs_bwd = expert_pass(inputs_fwd[token_fwd], inputs_saved[token_bwd], inputs_grad[token_bwd], up_block, down_block)
            results_fwd = results_fwd.at[index_fwd].set(outs_fwd)
            results_bwd = results_bwd.at[index_bwd].set(outs_bwd)
            return ((results_fwd, results_bwd), None)
        start = jnp.zeros((total + 1, D), jnp.bfloat16)
        (results_fwd, results_bwd), _ = lax.scan(one_expert, (start, start), jnp.arange(EXPERTS, dtype=jnp.int32))
        layer_outs.append(combine(x_fwd[section_id], results_fwd[:total], affinity_fwd[section_id]))
        input_grads.append(combine(grad_bwd[section_id], results_bwd[:total], affinity_bwd[section_id]))
    layer_out = jnp.stack(layer_outs)
    input_grad = jnp.stack(input_grads)
    return (jnp.roll(layer_out, 1, 0), jnp.roll(input_grad, -1, 0))
```

```python
import functools

import jax
import jax.numpy as jnp
from jax import lax
from jax.experimental import pallas as pl
from jax.experimental.pallas import tpu as pltpu
from jax.sharding import PartitionSpec as P

AGAINST_ROWS = (((1,), (1,)), ((), ()))


def from_partner_2(block, axis, apart):
    count = lax.axis_size(axis)
    route = []
    for low in range(count):
        high = low | 1 << apart
        if high != low and high < count:
            route += [(low, high), (high, low)]
    return lax.ppermute(block, axis, route)


def shifted(shard, axis, by):
    size = lax.axis_size(axis)
    return lax.ppermute(shard, axis, [(i, (i + by) % size) for i in range(size)])


def silu_grad(values):
    sigma = jax.nn.sigmoid(values)
    return sigma * (1.0 + values * (1.0 - sigma))


def slot_table(routes, experts, capacity):
    flat_routes = routes.reshape(-1)
    entries = flat_routes.shape[0]
    onehot = (flat_routes[:, None] == jnp.arange(experts, dtype=jnp.int32)[None, :]).astype(
        jnp.int32
    )
    before = jnp.cumsum(onehot, 0) - onehot
    position = jnp.sum(before * onehot, 1)
    slot_of = flat_routes * capacity + position
    source = (
        jnp.full((experts * capacity,), entries, jnp.int32)
        .at[slot_of]
        .set(jnp.arange(entries, dtype=jnp.int32))
    )
    return (slot_of, source)


def serve_rows(received, up_half, down_half):
    sources = received.shape[0]
    slots = received.shape[2]
    model_width = received.shape[3]
    row_count = sources * slots
    rows_fwd = received[:, 0].reshape(row_count, model_width)
    rows_saved = received[:, 1].reshape(row_count, model_width)
    rows_grad = received[:, 2].reshape(row_count, model_width)
    against_rows = (((1,), (1,)), ((), ()))
    hidden = jax.nn.silu(jnp.dot(rows_fwd, up_half, preferred_element_type=jnp.float32)).astype(
        jnp.bfloat16
    )
    part_fwd = jnp.dot(hidden, down_half, preferred_element_type=jnp.float32).astype(jnp.bfloat16)
    pre_act = jnp.dot(rows_saved, up_half, preferred_element_type=jnp.float32)
    hidden_grad = lax.dot_general(
        rows_grad, down_half, against_rows, preferred_element_type=jnp.float32
    )
    pre_grad = (hidden_grad * silu_grad(pre_act)).astype(jnp.bfloat16)
    part_bwd = lax.dot_general(
        pre_grad, up_half, against_rows, preferred_element_type=jnp.float32
    ).astype(jnp.bfloat16)
    return jnp.stack(
        [
            part_fwd.reshape(sources, slots, model_width),
            part_bwd.reshape(sources, slots, model_width),
        ],
        1,
    )


def combine(inputs, routed_rows, affinity):
    tokens = inputs.shape[0]
    top_count = affinity.shape[1]
    weights = affinity / jnp.sum(affinity, -1, keepdims=True)
    routed = routed_rows.reshape(tokens, top_count, inputs.shape[1]).astype(jnp.float32)
    return (inputs.astype(jnp.float32) + jnp.sum(weights[..., None] * routed, 1)).astype(
        jnp.bfloat16
    )


def general_path(
    x_fwd,
    routes_fwd,
    affinity_fwd,
    x_bwd,
    grad_bwd,
    routes_bwd,
    affinity_bwd,
    up_weight,
    down_weight,
):
    devices = lax.axis_size("expert")
    experts = devices // 2
    tokens = x_fwd.shape[1]
    model_width = x_fwd.shape[2]
    top_count = routes_fwd.shape[2]
    capacity = 3 * tokens * top_count // devices
    half_slots = capacity // 2
    up_half = up_weight[0]
    down_half = down_weight[0]
    slot_fwd, source_fwd = slot_table(routes_fwd[0], experts, capacity)
    slot_bwd, source_bwd = slot_table(routes_bwd[0], experts, capacity)
    zero_row = jnp.zeros((1, model_width), jnp.bfloat16)
    row_table = jnp.concatenate([x_fwd[0], zero_row, x_bwd[0], zero_row, grad_bwd[0], zero_row], 0)
    stride = tokens + 1
    token_fwd = (source_fwd // top_count).reshape(experts, capacity)
    token_bwd = (source_bwd // top_count).reshape(experts, capacity)
    gather_index = jnp.stack([token_fwd, token_bwd + stride, token_bwd + 2 * stride], 1)
    send_index = (
        gather_index.reshape(experts, 3, 2, half_slots)
        .transpose(0, 2, 1, 3)
        .reshape(devices, 3, half_slots)
    )
    outgoing = row_table[send_index]
    received = lax.all_to_all(outgoing, "expert", split_axis=0, concat_axis=0, tiled=True)
    partner = from_partner_2(received, "expert", 0)
    result = serve_rows(jnp.concatenate([received, partner], 2), up_half, down_half)
    piece_slots = received.shape[2]
    from_partner = from_partner_2(result[:, :, piece_slots:], "expert", 0)
    summed = (
        result[:, :, :piece_slots].astype(jnp.float32) + from_partner.astype(jnp.float32)
    ).astype(jnp.bfloat16)
    returned = lax.all_to_all(summed, "expert", split_axis=0, concat_axis=0, tiled=True)
    flat_back = returned.reshape(-1, model_width)

    def back_index(slot_of, member):
        expert_id = slot_of // capacity
        within = slot_of % capacity
        return (
            (2 * expert_id + within // half_slots) * 2 + member
        ) * half_slots + within % half_slots

    index_fwd = back_index(slot_fwd, 0)
    index_bwd = back_index(slot_bwd, 1)
    layer_out = combine(x_fwd[0], flat_back[index_fwd], affinity_fwd[0])
    input_grad = combine(grad_bwd[0], flat_back[index_bwd], affinity_bwd[0])
    fwd_next = shifted(layer_out[None], "section", 1)
    bwd_next = shifted(input_grad[None], "section", -1)
    return (fwd_next, bwd_next)


def line_kernel(
    sizes,
    routes_fwd,
    affinity_fwd,
    routes_bwd,
    affinity_bwd,
    x_fwd,
    x_bwd,
    grad_bwd,
    up,
    down,
    out_fwd,
    out_bwd,
    blocks,
    ups,
    downs,
    tables,
    total,
    slope,
    hidden_grad,
    hidden,
    pre_grad,
    returned,
    final,
    picked,
    piece,
    local_sem,
    table_send,
    table_recv,
    own_send,
    across_send,
    outer_send,
    block_recv,
    up_send,
    up_recv,
    down_send,
    down_recv,
    back_send,
    back_recv,
    shift_send,
    shift_recv,
):
    sections, experts, tokens, capacity, pieces, cut = sizes
    half_rows = tokens // 2
    streams = (x_fwd, x_bwd, grad_bwd)
    section = lax.axis_index("section")
    device = lax.axis_index("expert")
    place, side = device // 2, device % 2
    last = experts - 1
    is_inner = (place > 0) & (place < last)
    is_end = (place == 0) | (place == last)
    across = jnp.where(place < experts // 2, 1, -1)

    def at_place(where):
        return {"expert": where * 2 + side}

    def remote(src, dst, send, recv, target):
        return pltpu.make_async_remote_copy(
            src_ref=src,
            dst_ref=dst,
            send_sem=send,
            recv_sem=recv,
            device_id=target,
            device_id_type=pl.DeviceIdType.MESH,
        )

    partner = {"expert": place * 2 + 1 - side}
    next_section = {"section": lax.rem(section + 1, sections)}
    previous_section = {"section": lax.rem(section + sections - 1, sections)}
    column = [at_place(lax.rem(place + ahead, experts)) for ahead in range(1, experts)]

    barrier = pltpu.get_barrier_semaphore()
    peers = column + [partner, next_section, previous_section]
    for peer in peers:
        pl.semaphore_signal(
            barrier, inc=1, device_id=peer, device_id_type=pl.DeviceIdType.MESH
        )
    pl.semaphore_wait(barrier, len(peers))

    def rows_of(origin):
        return pl.ds(pl.multiple_of(origin * tokens, tokens), tokens)

    def half_of(origin, half):
        return pl.ds(pl.multiple_of(origin * tokens + half * half_rows, half_rows), half_rows)

    def columns_of(index):
        return pl.ds(pl.multiple_of(index * cut, cut), cut)

    def own_copy(stream, way, half):
        return remote(
            streams[stream].at[pl.ds(half * half_rows, half_rows)],
            blocks.at[stream, half_of(place, half)],
            own_send.at[stream, way, half],
            block_recv.at[stream, place, half],
            at_place(place + 1 - 2 * way),
        )

    def send_own(stream):
        for half in range(2):
            for way, allowed in ((0, place < last), (1, place > 0)):

                @pl.when(allowed)
                def _(way=way, half=half):
                    own_copy(stream, way, half).start()

    def wait_half(stream, origin, half):
        block = blocks.at[stream, half_of(origin, half)]
        remote(
            block, block, own_send.at[stream, 0, half], block_recv.at[stream, origin, half], partner
        ).wait_recv()

    def across_copy(stream, half):
        origin = place - across
        block = blocks.at[stream, half_of(origin, half)]
        return remote(
            block,
            block,
            across_send.at[stream, half],
            block_recv.at[stream, origin, half],
            at_place(place + across),
        )

    def send_across(stream, half):
        @pl.when(is_inner)
        def _():
            wait_half(stream, place - across, half)
            across_copy(stream, half).start()

    def outer_copy(stream, steps):
        origin = place + across * steps
        return remote(
            picked.at[stream, steps - 1],
            blocks.at[stream, pl.ds(pl.multiple_of(origin * tokens, tokens), capacity)],
            outer_send.at[stream, steps - 1],
            block_recv.at[stream, origin, 0],
            at_place(place - across),
        )

    def table_row(member, kind, origin, expert):
        return tables[origin, pl.ds((member * 2 + kind) * experts + expert, 1), :]

    def send_outer(stream, steps):
        @pl.when(is_inner)
        def _():
            origin = place + across * steps
            for half in range(2):
                wait_half(stream, origin, half)
            ranks = table_row(min(stream, 1), 1, origin, place - across)
            slots = lax.broadcasted_iota(jnp.int32, (capacity, tokens), 0).astype(jnp.float32)
            pick = jnp.where(slots == ranks, 1.0, 0.0).astype(jnp.bfloat16)

            @pl.loop(0, pieces)
            def _(index):
                picked[stream, steps - 1, :, columns_of(index)] = jnp.dot(
                    pick,
                    blocks[stream, rows_of(origin), columns_of(index)],
                    preferred_element_type=jnp.float32,
                ).astype(jnp.bfloat16)

            outer_copy(stream, steps).start()

    def wait_at_end(stream):
        @pl.when(is_end)
        def _():
            for half in range(2):
                wait_half(stream, place + across, half)
            for steps in (2, 3):
                origin = place + across * steps
                landed = blocks.at[
                    stream, pl.ds(pl.multiple_of(origin * tokens, tokens), capacity)
                ]
                remote(
                    landed,
                    landed,
                    own_send.at[stream, 0, 0],
                    block_recv.at[stream, origin, 0],
                    partner,
                ).wait_recv()

    def up_copy(index):
        rows = columns_of(index)
        return remote(
            up.at[rows], ups.at[1, rows], up_send.at[index], up_recv.at[index], partner
        )

    def down_copy(index):
        rows = columns_of(index)
        return remote(
            down.at[:, rows],
            downs.at[1, :, rows],
            down_send.at[index],
            down_recv.at[index],
            partner,
        )

    send_own(0)

    @pl.loop(0, pieces)
    def _(index):
        up_copy(index).start()

    @pl.loop(0, pieces)
    def _(index):
        down_copy(index).start()

    local = [
        pltpu.make_async_copy(
            streams[stream], blocks.at[stream, rows_of(place)], local_sem.at[stream]
        )
        for stream in range(3)
    ]
    local.append(pltpu.make_async_copy(up, ups.at[0], local_sem.at[3]))
    local.append(pltpu.make_async_copy(down, downs.at[0], local_sem.at[4]))
    for copy in local:
        copy.start()

    row_id = lax.broadcasted_iota(jnp.int32, (tokens, tokens), 0)
    lane_id = lax.broadcasted_iota(jnp.int32, (tokens, tokens), 1)
    earlier = jnp.where(lane_id < row_id, 1.0, 0.0).astype(jnp.bfloat16)
    for member, (routes, affinity) in enumerate(
        ((routes_fwd, affinity_fwd), (routes_bwd, affinity_bwd))
    ):
        weights = affinity[...] / jnp.sum(affinity[...], -1, keepdims=True)
        share = jnp.zeros((tokens, tokens), jnp.float32)
        named = jnp.zeros((tokens, tokens), jnp.float32)
        for choice in range(routes.shape[1]):
            same = routes[:, choice : choice + 1] == lane_id
            share += jnp.where(same, weights[:, choice : choice + 1], 0.0)
            named += jnp.where(same, 1.0, 0.0)
        rank = jnp.dot(earlier, named.astype(jnp.bfloat16), preferred_element_type=jnp.float32)
        rank = jnp.where(named > 0.5, rank, -1.0)
        base = member * 2 * experts
        tables[place, base : base + experts, :] = share.T[:experts]
        tables[place, base + experts : base + 2 * experts, :] = rank.T[:experts]

    table_copies = [
        remote(
            tables.at[place],
            tables.at[place],
            table_send.at[ahead],
            table_recv.at[place],
            column[ahead],
        )
        for ahead in range(experts - 1)
    ]
    for copy in table_copies:
        copy.start()

    @pl.when(is_end)
    def _():
        for stream in range(3):
            for steps in (2, 3):
                start = pl.multiple_of((place + across * steps) * tokens + capacity, 16)
                blocks[stream, pl.ds(start, tokens - capacity), :] = jnp.zeros(
                    (tokens - capacity, blocks.shape[2]), jnp.bfloat16
                )

    for ahead in range(1, experts):
        origin = lax.rem(place + ahead, experts)
        remote(
            tables.at[origin],
            tables.at[origin],
            table_send.at[0],
            table_recv.at[origin],
            partner,
        ).wait_recv()

    def placing(member, origin):
        slots = row_id.astype(jnp.float32)
        lanes = lane_id.astype(jnp.float32)
        distance = jnp.abs(origin - place)
        packed = is_end & (distance > 1)
        ranks = jnp.where(packed, table_row(member, 1, origin, place), lanes[:1])
        share = table_row(member, 0, origin, place)
        weight = jnp.sum(jnp.where(slots == ranks, share, 0.0), 1, keepdims=True)
        rank = jnp.sum(jnp.where(row_id == lane_id, ranks, 0.0), 1, keepdims=True)
        spread = jnp.where(lanes == rank, 1.0, 0.0).astype(jnp.bfloat16)
        return weight, spread

    def project(stream, half):
        total[...] = jnp.zeros(total.shape, jnp.float32)

        @pl.loop(0, pieces)
        def _(index):
            total[...] += jnp.dot(
                blocks[stream, :, columns_of(index)],
                ups[half, columns_of(index), :],
                preferred_element_type=jnp.float32,
            )

    def make_hidden():
        @pl.loop(0, 2)
        def _(half):
            project(0, half)

            @pl.loop(0, experts)
            def _(origin):
                weight, spread = placing(0, origin)
                act = total[rows_of(origin), :]
                value = (act / (1.0 + jnp.exp(-act)) * weight).astype(jnp.bfloat16)
                hidden[half, rows_of(origin), :] = jnp.dot(
                    spread, value, preferred_element_type=jnp.float32
                ).astype(jnp.bfloat16)

    def make_slope():
        @pl.loop(0, 2)
        def _(half):
            project(1, half)

            @pl.loop(0, experts)
            def _(origin):
                weight, _ = placing(1, origin)
                act = total[rows_of(origin), :]
                sigma = 1.0 / (1.0 + jnp.exp(-act))
                slope[half, rows_of(origin), :] = (
                    sigma * (1.0 + act * (1.0 - sigma))
                ) * weight

    def add_hidden_grad(half, index):
        hidden_grad[half] += lax.dot_general(
            blocks[2, :, columns_of(index)],
            downs[half, :, columns_of(index)],
            AGAINST_ROWS,
            preferred_element_type=jnp.float32,
        )

    def start_hidden_grad():
        hidden_grad[...] = jnp.zeros(hidden_grad.shape, jnp.float32)

        @pl.loop(0, 2 * pieces - 1)
        def _(index):
            half = index // pieces
            add_hidden_grad(half, index - half * pieces)

    def make_pre_grad():
        add_hidden_grad(1, pieces - 1)

        @pl.loop(0, 2 * experts)
        def _(index):
            half = index // experts
            origin = index - half * experts
            _, spread = placing(1, origin)
            rows = rows_of(origin)
            value = (hidden_grad[half, rows, :] * slope[half, rows, :]).astype(jnp.bfloat16)
            pre_grad[half, rows, :] = jnp.dot(
                spread, value, preferred_element_type=jnp.float32
            ).astype(jnp.bfloat16)

    def back_copy(member, target, index):
        way = jnp.where(target > place, 1, -1)
        there = place + way
        slot = jnp.where((way < 0) & (target == there), experts, target)
        return remote(
            returned.at[member, target, index],
            returned.at[member, slot, index],
            back_send.at[member, target, index],
            back_recv.at[member, slot, index],
            at_place(there),
        )

    def wait_back(member, slot, index):
        landed = returned.at[member, slot, index]
        remote(
            landed,
            landed,
            back_send.at[member, 0, index],
            back_recv.at[member, slot, index],
            partner,
        ).wait_recv()

    def shift_copy(member, index):
        return remote(
            final.at[member, index],
            (out_fwd, out_bwd)[member].at[:, columns_of(index)],
            shift_send.at[member, index],
            shift_recv.at[member, index],
            (next_section, previous_section)[member],
        )

    def serve(target, member, index):
        rows = rows_of(target)

        @pl.when(member == 0)
        def _():
            piece[...] = jnp.dot(
                hidden[0, rows, :],
                downs[0, :, columns_of(index)],
                preferred_element_type=jnp.float32,
            ) + jnp.dot(
                hidden[1, rows, :],
                downs[1, :, columns_of(index)],
                preferred_element_type=jnp.float32,
            )

        @pl.when(member == 1)
        def _():
            piece[...] = lax.dot_general(
                pre_grad[0, rows, :],
                ups[0, columns_of(index), :],
                AGAINST_ROWS,
                preferred_element_type=jnp.float32,
            ) + lax.dot_general(
                pre_grad[1, rows, :],
                ups[1, columns_of(index), :],
                AGAINST_ROWS,
                preferred_element_type=jnp.float32,
            )

        @pl.when(target != place)
        def _():
            @pl.when(is_inner)
            def _():
                wait_back(member, target, index)
                returned[member, target, index] = (
                    piece[...] + returned[member, target, index].astype(jnp.float32)
                ).astype(jnp.bfloat16)

            @pl.when(is_end)
            def _():
                returned[member, target, index] = piece[...].astype(jnp.bfloat16)

            back_copy(member, target, index).start()

        @pl.when(target == place)
        def _():
            @pl.when(place > 0)
            def _():
                wait_back(member, target, index)
                piece[...] += returned[member, target, index].astype(jnp.float32)

            @pl.when(place < last)
            def _():
                wait_back(member, experts, index)
                piece[...] += returned[member, experts, index].astype(jnp.float32)

            for each in range(2):

                @pl.when(member == each)
                def _(each=each):
                    final[each, index] = (
                        piece[...]
                        + blocks[2 * each, rows, columns_of(index)].astype(jnp.float32)
                    ).astype(jnp.bfloat16)
                    shift_copy(each, index).start()

    send_across(0, 0)
    send_across(0, 1)
    send_own(1)
    send_outer(0, 1)
    send_across(1, 0)
    send_outer(0, 2)
    send_across(1, 1)
    send_own(2)
    send_outer(1, 1)
    send_across(2, 0)
    send_across(2, 1)
    send_outer(1, 2)
    for copy in local:
        copy.wait()
    wait_at_end(0)

    @pl.loop(0, pieces)
    def _(index):
        up_copy(index).wait_recv()

    make_hidden()

    @pl.loop(0, 2 * pieces + last)
    def _(turn):
        @pl.when(turn < pieces)
        def _():
            down_copy(turn).wait_recv()

        @pl.when(turn == 1)
        def _():
            send_outer(2, 1)

        @pl.when(turn == 3)
        def _():
            send_outer(2, 2)

        @pl.when(turn == pieces)
        def _():
            make_pre_grad()

        @pl.loop(0, experts)
        def _(order):
            target = jnp.where(
                order < last - place,
                last - order,
                jnp.where(order < last, order - (last - place), place),
            )
            late = jnp.where(
                target > place,
                place,
                jnp.where(target < place, last - place, jnp.maximum(place, last - place)),
            )
            step = turn - late

            @pl.when((step >= 0) & (step < 2 * pieces))
            def _():
                member = jnp.where(step >= pieces, 1, 0)
                serve(target, member, step - member * pieces)

        @pl.when(turn == pieces - 3)
        def _():
            wait_at_end(1)
            make_slope()

        @pl.when(turn == pieces - 2)
        def _():
            wait_at_end(2)
            start_hidden_grad()

    for stream in range(3):
        for half in range(2):
            for way, allowed in ((0, place < last), (1, place > 0)):

                @pl.when(allowed)
                def _(stream=stream, way=way, half=half):
                    own_copy(stream, way, half).wait_send()

    @pl.when(is_inner)
    def _():
        for stream in range(3):
            for half in range(2):
                across_copy(stream, half).wait_send()
            for steps in (1, 2):
                outer_copy(stream, steps).wait_send()

    for copy in table_copies:
        copy.wait_send()

    @pl.loop(0, pieces)
    def _(index):
        up_copy(index).wait_send()
        down_copy(index).wait_send()
        for member in range(2):

            @pl.loop(1, experts)
            def _(ahead):
                back_copy(member, lax.rem(place + ahead, experts), index).wait_send()

            shift_copy(member, index).wait()


def line_path(
    x_fwd,
    routes_fwd,
    affinity_fwd,
    x_bwd,
    grad_bwd,
    routes_bwd,
    affinity_bwd,
    up_weight,
    down_weight,
):
    devices = lax.axis_size("expert")
    sections = lax.axis_size("section")
    experts = devices // 2
    tokens, width = x_fwd.shape[1:]
    top_count = routes_fwd.shape[2]
    units = up_weight.shape[2]
    capacity = 3 * tokens * top_count // devices
    cut = piece_width(width)
    pieces = width // cut
    rows = experts * tokens
    bf16, f32 = jnp.bfloat16, jnp.float32
    dma = pltpu.SemaphoreType.DMA
    in_vmem = pl.BlockSpec(memory_space=pltpu.VMEM)
    anywhere = pl.BlockSpec(memory_space=pl.ANY)
    outs = pl.pallas_call(
        functools.partial(line_kernel, (sections, experts, tokens, capacity, pieces, cut)),
        name="expert_line",
        out_shape=[jax.ShapeDtypeStruct((tokens, width), bf16)] * 2,
        in_specs=[in_vmem] * 4 + [anywhere] * 5,
        out_specs=[anywhere] * 2,
        scratch_shapes=[
            pltpu.VMEM((3, rows, width), bf16),
            pltpu.VMEM((2, width, units), bf16),
            pltpu.VMEM((2, units, width), bf16),
            pltpu.VMEM((experts, 4 * experts, tokens), f32),
            pltpu.VMEM((rows, units), f32),
            pltpu.VMEM((2, rows, units), f32),
            pltpu.VMEM((2, rows, units), f32),
            pltpu.VMEM((2, rows, units), bf16),
            pltpu.VMEM((2, rows, units), bf16),
            pltpu.VMEM((2, experts + 1, pieces, tokens, cut), bf16),
            pltpu.VMEM((2, pieces, tokens, cut), bf16),
            pltpu.VMEM((3, 2, capacity, width), bf16),
            pltpu.VMEM((tokens, cut), f32),
            dma((5,)),
            dma((experts - 1,)),
            dma((experts,)),
            dma((3, 2, 2)),
            dma((3, 2)),
            dma((3, 2)),
            dma((3, experts, 2)),
            dma((pieces,)),
            dma((pieces,)),
            dma((pieces,)),
            dma((pieces,)),
            dma((2, experts, pieces)),
            dma((2, experts + 1, pieces)),
            dma((2, pieces)),
            dma((2, pieces)),
        ],
        compiler_params=pltpu.CompilerParams(
            collective_id=0, has_side_effects=True, vmem_limit_bytes=60 << 20
        ),
    )(
        routes_fwd[0],
        affinity_fwd[0],
        routes_bwd[0],
        affinity_bwd[0],
        x_fwd[0],
        x_bwd[0],
        grad_bwd[0],
        up_weight[0],
        down_weight[0],
    )
    return tuple(out[None] for out in outs)


def piece_width(width):
    for cut in (512, 256, 128):
        if width % cut == 0:
            return cut
    return 0


def per_device(*args):
    experts = lax.axis_size("expert") // 2
    tokens, width = args[0].shape[1:]
    if experts == 4 and tokens == 128 and piece_width(width):
        return line_path(*args)
    return general_path(*args)


def solution(mesh):
    in_specs = (
        P("section", "expert", None),
        P("section", "expert", None),
        P("section", "expert", None),
        P("section", "expert", None),
        P("section", "expert", None),
        P("section", "expert", None),
        P("section", "expert", None),
        P("section", None, "expert"),
        P("section", "expert", None),
    )
    out_specs = (P("section", "expert", None), P("section", "expert", None))
    return jax.shard_map(
        per_device, mesh=mesh, in_specs=in_specs, out_specs=out_specs, check_vma=False
    )
```

```python
import functools

import jax
import jax.numpy as jnp
from jax import lax
from jax.experimental import pallas as pl
from jax.experimental.pallas import tpu as pltpu
from jax.sharding import PartitionSpec as P

AGAINST_ROWS = (((1,), (1,)), ((), ()))


def from_partner_2(block, axis, apart):
    count = lax.axis_size(axis)
    route = []
    for low in range(count):
        high = low | 1 << apart
        if high != low and high < count:
            route += [(low, high), (high, low)]
    return lax.ppermute(block, axis, route)


def shifted(shard, axis, by):
    size = lax.axis_size(axis)
    return lax.ppermute(shard, axis, [(i, (i + by) % size) for i in range(size)])


def silu_grad(values):
    sigma = jax.nn.sigmoid(values)
    return sigma * (1.0 + values * (1.0 - sigma))


def slot_table(routes, experts, capacity):
    flat_routes = routes.reshape(-1)
    entries = flat_routes.shape[0]
    onehot = (flat_routes[:, None] == jnp.arange(experts, dtype=jnp.int32)[None, :]).astype(
        jnp.int32
    )
    before = jnp.cumsum(onehot, 0) - onehot
    position = jnp.sum(before * onehot, 1)
    slot_of = flat_routes * capacity + position
    source = (
        jnp.full((experts * capacity,), entries, jnp.int32)
        .at[slot_of]
        .set(jnp.arange(entries, dtype=jnp.int32))
    )
    return (slot_of, source)


def serve_rows(received, up_half, down_half):
    sources = received.shape[0]
    slots = received.shape[2]
    model_width = received.shape[3]
    row_count = sources * slots
    rows_fwd = received[:, 0].reshape(row_count, model_width)
    rows_saved = received[:, 1].reshape(row_count, model_width)
    rows_grad = received[:, 2].reshape(row_count, model_width)
    against_rows = (((1,), (1,)), ((), ()))
    hidden = jax.nn.silu(jnp.dot(rows_fwd, up_half, preferred_element_type=jnp.float32)).astype(
        jnp.bfloat16
    )
    part_fwd = jnp.dot(hidden, down_half, preferred_element_type=jnp.float32).astype(jnp.bfloat16)
    pre_act = jnp.dot(rows_saved, up_half, preferred_element_type=jnp.float32)
    hidden_grad = lax.dot_general(
        rows_grad, down_half, against_rows, preferred_element_type=jnp.float32
    )
    pre_grad = (hidden_grad * silu_grad(pre_act)).astype(jnp.bfloat16)
    part_bwd = lax.dot_general(
        pre_grad, up_half, against_rows, preferred_element_type=jnp.float32
    ).astype(jnp.bfloat16)
    return jnp.stack(
        [
            part_fwd.reshape(sources, slots, model_width),
            part_bwd.reshape(sources, slots, model_width),
        ],
        1,
    )


def combine(inputs, routed_rows, affinity):
    tokens = inputs.shape[0]
    top_count = affinity.shape[1]
    weights = affinity / jnp.sum(affinity, -1, keepdims=True)
    routed = routed_rows.reshape(tokens, top_count, inputs.shape[1]).astype(jnp.float32)
    return (inputs.astype(jnp.float32) + jnp.sum(weights[..., None] * routed, 1)).astype(
        jnp.bfloat16
    )


def general_path(
    x_fwd,
    routes_fwd,
    affinity_fwd,
    x_bwd,
    grad_bwd,
    routes_bwd,
    affinity_bwd,
    up_weight,
    down_weight,
):
    devices = lax.axis_size("expert")
    experts = devices // 2
    tokens = x_fwd.shape[1]
    model_width = x_fwd.shape[2]
    top_count = routes_fwd.shape[2]
    capacity = 3 * tokens * top_count // devices
    half_slots = capacity // 2
    up_half = up_weight[0]
    down_half = down_weight[0]
    slot_fwd, source_fwd = slot_table(routes_fwd[0], experts, capacity)
    slot_bwd, source_bwd = slot_table(routes_bwd[0], experts, capacity)
    zero_row = jnp.zeros((1, model_width), jnp.bfloat16)
    row_table = jnp.concatenate([x_fwd[0], zero_row, x_bwd[0], zero_row, grad_bwd[0], zero_row], 0)
    stride = tokens + 1
    token_fwd = (source_fwd // top_count).reshape(experts, capacity)
    token_bwd = (source_bwd // top_count).reshape(experts, capacity)
    gather_index = jnp.stack([token_fwd, token_bwd + stride, token_bwd + 2 * stride], 1)
    send_index = (
        gather_index.reshape(experts, 3, 2, half_slots)
        .transpose(0, 2, 1, 3)
        .reshape(devices, 3, half_slots)
    )
    outgoing = row_table[send_index]
    received = lax.all_to_all(outgoing, "expert", split_axis=0, concat_axis=0, tiled=True)
    partner = from_partner_2(received, "expert", 0)
    result = serve_rows(jnp.concatenate([received, partner], 2), up_half, down_half)
    piece_slots = received.shape[2]
    from_partner = from_partner_2(result[:, :, piece_slots:], "expert", 0)
    summed = (
        result[:, :, :piece_slots].astype(jnp.float32) + from_partner.astype(jnp.float32)
    ).astype(jnp.bfloat16)
    returned = lax.all_to_all(summed, "expert", split_axis=0, concat_axis=0, tiled=True)
    flat_back = returned.reshape(-1, model_width)

    def back_index(slot_of, member):
        expert_id = slot_of // capacity
        within = slot_of % capacity
        return (
            (2 * expert_id + within // half_slots) * 2 + member
        ) * half_slots + within % half_slots

    index_fwd = back_index(slot_fwd, 0)
    index_bwd = back_index(slot_bwd, 1)
    layer_out = combine(x_fwd[0], flat_back[index_fwd], affinity_fwd[0])
    input_grad = combine(grad_bwd[0], flat_back[index_bwd], affinity_bwd[0])
    fwd_next = shifted(layer_out[None], "section", 1)
    bwd_next = shifted(input_grad[None], "section", -1)
    return (fwd_next, bwd_next)


def line_kernel(
    sizes,
    routes_fwd,
    affinity_fwd,
    routes_bwd,
    affinity_bwd,
    x_fwd,
    x_bwd,
    grad_bwd,
    up,
    down,
    out_fwd,
    out_bwd,
    blocks,
    ups,
    downs,
    tables,
    total,
    slope,
    hidden_grad,
    hidden,
    pre_grad,
    returned,
    final,
    picked,
    expand,
    piece,
    local_sem,
    table_send,
    table_recv,
    own_send,
    across_send,
    outer_send,
    block_recv,
    up_send,
    up_recv,
    down_send,
    down_recv,
    back_send,
    back_recv,
    shift_send,
    shift_recv,
):
    sections, experts, tokens, capacity, pieces, cut = sizes
    half_rows = tokens // 2
    streams = (x_fwd, x_bwd, grad_bwd)
    section = lax.axis_index("section")
    device = lax.axis_index("expert")
    place, side = device // 2, device % 2
    last = experts - 1
    is_inner = (place > 0) & (place < last)
    is_end = (place == 0) | (place == last)
    across = jnp.where(place < experts // 2, 1, -1)

    def at_place(where):
        return {"expert": where * 2 + side}

    def remote(src, dst, send, recv, target):
        return pltpu.make_async_remote_copy(
            src_ref=src,
            dst_ref=dst,
            send_sem=send,
            recv_sem=recv,
            device_id=target,
            device_id_type=pl.DeviceIdType.MESH,
        )

    partner = {"expert": place * 2 + 1 - side}
    next_section = {"section": lax.rem(section + 1, sections)}
    previous_section = {"section": lax.rem(section + sections - 1, sections)}
    column = [at_place(lax.rem(place + ahead, experts)) for ahead in range(1, experts)]

    barrier = pltpu.get_barrier_semaphore()
    peers = column + [partner, next_section, previous_section]
    for peer in peers:
        pl.semaphore_signal(
            barrier, inc=1, device_id=peer, device_id_type=pl.DeviceIdType.MESH
        )

    row_id = lax.broadcasted_iota(jnp.int32, (tokens, tokens), 0)
    lane_id = lax.broadcasted_iota(jnp.int32, (tokens, tokens), 1)
    later = jnp.where(row_id < lane_id, 1.0, 0.0).astype(jnp.bfloat16)
    expert_id = row_id[:16]
    for member, (routes, affinity) in enumerate(
        ((routes_fwd, affinity_fwd), (routes_bwd, affinity_bwd))
    ):
        weights = affinity[...] / jnp.sum(affinity[...], 0, keepdims=True)
        share = jnp.zeros(expert_id.shape, jnp.float32)
        named = jnp.zeros(expert_id.shape, jnp.float32)
        for choice in range(routes.shape[0]):
            same = routes[choice : choice + 1, :] == expert_id
            share += jnp.where(same, weights[choice : choice + 1, :], 0.0)
            named += jnp.where(same, 1.0, 0.0)
        rank = jnp.dot(named.astype(jnp.bfloat16), later, preferred_element_type=jnp.float32)
        rank = jnp.where(named > 0.5, rank, -1.0)
        base = member * 2 * experts
        tables[place, base : base + experts, :] = share[:experts]
        tables[place, base + experts : base + 2 * experts, :] = rank[:experts]

    pl.semaphore_wait(barrier, len(peers))
    table_copies = [
        remote(
            tables.at[place],
            tables.at[place],
            table_send.at[ahead],
            table_recv.at[place],
            column[ahead],
        )
        for ahead in range(experts - 1)
    ]
    for copy in table_copies:
        copy.start()

    def rows_of(origin):
        return pl.ds(pl.multiple_of(origin * tokens, tokens), tokens)

    def half_of(origin, half):
        return pl.ds(pl.multiple_of(origin * tokens + half * half_rows, half_rows), half_rows)

    def columns_of(index):
        return pl.ds(pl.multiple_of(index * cut, cut), cut)

    def own_copy(stream, half):
        return remote(
            streams[stream].at[pl.ds(half * half_rows, half_rows)],
            blocks.at[stream, half_of(place, half)],
            own_send.at[stream, half],
            block_recv.at[stream, place, half],
            at_place(place + across),
        )

    def send_own(stream):
        for half in range(2):
            own_copy(stream, half).start()

    def wait_half(stream, origin, half):
        block = blocks.at[stream, half_of(origin, half)]
        remote(
            block, block, own_send.at[stream, half], block_recv.at[stream, origin, half], partner
        ).wait_recv()

    def across_copy(stream, half):
        origin = place - across
        block = blocks.at[stream, half_of(origin, half)]
        return remote(
            block,
            block,
            across_send.at[stream, half],
            block_recv.at[stream, origin, half],
            at_place(place + across),
        )

    def send_across(stream, half):
        @pl.when(is_inner)
        def _():
            wait_half(stream, place - across, half)
            across_copy(stream, half).start()

    def outer_copy(stream, steps):
        origin = place + across * steps
        return remote(
            picked.at[stream, steps],
            blocks.at[stream, pl.ds(pl.multiple_of(origin * tokens, tokens), capacity)],
            outer_send.at[stream, steps],
            block_recv.at[stream, origin, 0],
            at_place(place - across),
        )

    def table_row(member, kind, origin, expert):
        return tables[origin, pl.ds((member * 2 + kind) * experts + expert, 1), :]

    def send_outer(stream, steps):
        @pl.when(is_inner)
        def _():
            origin = place + across * steps
            if steps:
                for half in range(2):
                    wait_half(stream, origin, half)
            ranks = table_row(min(stream, 1), 1, origin, place - across)
            slots = lax.broadcasted_iota(jnp.int32, (capacity, tokens), 0).astype(jnp.float32)
            pick = jnp.where(slots == ranks, 1.0, 0.0).astype(jnp.bfloat16)

            @pl.loop(0, pieces)
            def _(index):
                picked[stream, steps, :, columns_of(index)] = jnp.dot(
                    pick,
                    blocks[stream, rows_of(origin), columns_of(index)],
                    preferred_element_type=jnp.float32,
                ).astype(jnp.bfloat16)

            outer_copy(stream, steps).start()

    def wait_at_end(stream):
        @pl.when(is_end)
        def _():
            for steps in range(1, experts):
                origin = place + across * steps
                landed = blocks.at[
                    stream, pl.ds(pl.multiple_of(origin * tokens, tokens), capacity)
                ]
                remote(
                    landed,
                    landed,
                    own_send.at[stream, 0],
                    block_recv.at[stream, origin, 0],
                    partner,
                ).wait_recv()

    def up_copy(index):
        rows = columns_of(index)
        return remote(
            up.at[rows], ups.at[1, rows], up_send.at[index], up_recv.at[index], partner
        )

    def down_copy(index):
        rows = columns_of(index)
        return remote(
            down.at[:, rows],
            downs.at[1, :, rows],
            down_send.at[index],
            down_recv.at[index],
            partner,
        )

    send_own(0)

    @pl.loop(0, pieces)
    def _(index):
        up_copy(index).start()

    @pl.loop(0, pieces)
    def _(index):
        down_copy(index).start()

    local = [
        pltpu.make_async_copy(
            streams[stream], blocks.at[stream, rows_of(place)], local_sem.at[stream]
        )
        for stream in range(3)
    ]
    local.append(pltpu.make_async_copy(up, ups.at[0], local_sem.at[3]))
    local.append(pltpu.make_async_copy(down, downs.at[0], local_sem.at[4]))
    for copy in local:
        copy.start()

    @pl.when(is_end)
    def _():
        for stream in range(3):
            for steps in range(1, experts):
                start = pl.multiple_of((place + across * steps) * tokens + capacity, 16)
                blocks[stream, pl.ds(start, tokens - capacity), :] = jnp.zeros(
                    (tokens - capacity, blocks.shape[2]), jnp.bfloat16
                )

    def wait_tables():
        for ahead in range(1, experts):
            origin = lax.rem(place + ahead, experts)
            remote(
                tables.at[origin],
                tables.at[origin],
                table_send.at[0],
                table_recv.at[origin],
                partner,
            ).wait_recv()

    def make_expand():
        @pl.when(is_inner)
        def _():
            @pl.loop(0, 2 * experts)
            def _(index):
                member = index // experts
                origin = index - member * experts
                ranks = table_row(member, 1, origin, place - across)
                rank = jnp.sum(jnp.where(row_id == lane_id, ranks, 0.0), 1, keepdims=True)
                expand[member, origin] = jnp.where(
                    lane_id.astype(jnp.float32) == rank, 1.0, 0.0
                ).astype(jnp.bfloat16)

    def weight_of(member, origin):
        packed = is_end & (origin != place)
        slots = row_id.astype(jnp.float32)
        lanes = lane_id[:1].astype(jnp.float32)
        ranks = jnp.where(packed, table_row(member, 1, origin, place), lanes)
        share = table_row(member, 0, origin, place)
        return jnp.sum(jnp.where(slots == ranks, share, 0.0), 1, keepdims=True)

    def project(stream, half):
        total[...] = jnp.zeros(total.shape, jnp.float32)

        @pl.loop(0, pieces)
        def _(index):
            total[...] += jnp.dot(
                blocks[stream, :, columns_of(index)],
                ups[half, columns_of(index), :],
                preferred_element_type=jnp.float32,
            )

    def make_hidden():
        @pl.loop(0, 2)
        def _(half):
            project(0, half)

            @pl.loop(0, experts)
            def _(origin):
                act = total[rows_of(origin), :]
                hidden[half, rows_of(origin), :] = (
                    act / (1.0 + jnp.exp(-act)) * weight_of(0, origin)
                ).astype(jnp.bfloat16)

    def make_slope():
        @pl.loop(0, 2)
        def _(half):
            project(1, half)

            @pl.loop(0, experts)
            def _(origin):
                weight = weight_of(1, origin)
                act = total[rows_of(origin), :]
                sigma = 1.0 / (1.0 + jnp.exp(-act))
                slope[half, rows_of(origin), :] = (
                    sigma * (1.0 + act * (1.0 - sigma))
                ) * weight

    def add_hidden_grad(half, index):
        hidden_grad[half] += lax.dot_general(
            blocks[2, :, columns_of(index)],
            downs[half, :, columns_of(index)],
            AGAINST_ROWS,
            preferred_element_type=jnp.float32,
        )

    def start_hidden_grad():
        hidden_grad[...] = jnp.zeros(hidden_grad.shape, jnp.float32)

        @pl.loop(0, 2 * pieces - 1)
        def _(index):
            half = index // pieces
            add_hidden_grad(half, index - half * pieces)

    def make_pre_grad():
        add_hidden_grad(1, pieces - 1)

        @pl.loop(0, 2 * experts)
        def _(index):
            half = index // experts
            origin = index - half * experts
            rows = rows_of(origin)
            pre_grad[half, rows, :] = (
                hidden_grad[half, rows, :] * slope[half, rows, :]
            ).astype(jnp.bfloat16)

    def back_copy(member, target, index, count):
        way = jnp.where(target > place, 1, -1)
        there = place + way
        slot = jnp.where((way < 0) & (target == there), experts, target)
        return remote(
            returned.at[member, target, index, pl.ds(0, count)],
            returned.at[member, slot, index, pl.ds(0, count)],
            back_send.at[member, target, index],
            back_recv.at[member, slot, index],
            at_place(there),
        )

    def add_back(member, slot, index):
        landed = returned.at[member, slot, index]
        remote(
            landed,
            landed,
            back_send.at[member, 0, index],
            back_recv.at[member, slot, index],
            partner,
        ).wait_recv()
        piece[...] += returned[member, slot, index].astype(jnp.float32)

    def add_packed_back(member, slot, index, origin):
        landed = returned.at[member, slot, index, pl.ds(0, capacity)]
        remote(
            landed,
            landed,
            back_send.at[member, 0, index],
            back_recv.at[member, slot, index],
            partner,
        ).wait_recv()
        piece[...] += jnp.dot(
            expand[member, origin, :, :capacity],
            returned[member, slot, index, :capacity],
            preferred_element_type=jnp.float32,
        )

    def shift_copy(member, index):
        return remote(
            final.at[member, index],
            (out_fwd, out_bwd)[member].at[:, columns_of(index)],
            shift_send.at[member, index],
            shift_recv.at[member, index],
            (next_section, previous_section)[member],
        )

    def serve(target, member, index):
        rows = rows_of(target)

        @pl.when(member == 0)
        def _():
            piece[...] = jnp.dot(
                hidden[0, rows, :],
                downs[0, :, columns_of(index)],
                preferred_element_type=jnp.float32,
            ) + jnp.dot(
                hidden[1, rows, :],
                downs[1, :, columns_of(index)],
                preferred_element_type=jnp.float32,
            )

        @pl.when(member == 1)
        def _():
            piece[...] = lax.dot_general(
                pre_grad[0, rows, :],
                ups[0, columns_of(index), :],
                AGAINST_ROWS,
                preferred_element_type=jnp.float32,
            ) + lax.dot_general(
                pre_grad[1, rows, :],
                ups[1, columns_of(index), :],
                AGAINST_ROWS,
                preferred_element_type=jnp.float32,
            )

        @pl.when(target != place)
        def _():
            @pl.when(is_end)
            def _():
                returned[member, target, index] = piece[...].astype(jnp.bfloat16)
                back_copy(member, target, index, capacity).start()

            @pl.when(is_inner)
            def _():
                beyond = (target - place) * across > 0

                @pl.when(beyond)
                def _():
                    add_packed_back(member, target, index, target)

                @pl.when(jnp.logical_not(beyond))
                def _():
                    add_back(member, target, index)

                returned[member, target, index] = piece[...].astype(jnp.bfloat16)
                back_copy(member, target, index, tokens).start()

        @pl.when(target == place)
        def _():
            @pl.when(is_inner)
            def _():
                add_packed_back(
                    member, jnp.where(across > 0, place, experts), index, place
                )

            add_back(member, jnp.where(across > 0, experts, place), index)

            for each in range(2):

                @pl.when(member == each)
                def _(each=each):
                    final[each, index] = (
                        piece[...]
                        + blocks[2 * each, rows, columns_of(index)].astype(jnp.float32)
                    ).astype(jnp.bfloat16)
                    shift_copy(each, index).start()

    local[0].wait()
    send_outer(0, 0)
    send_across(0, 0)
    send_across(0, 1)
    send_own(1)
    wait_tables()
    send_outer(0, 1)
    local[1].wait()
    send_outer(1, 0)
    send_across(1, 0)
    send_outer(0, 2)
    send_across(1, 1)
    send_own(2)
    send_outer(1, 1)
    local[2].wait()
    send_outer(2, 0)
    send_across(2, 0)
    send_across(2, 1)
    make_expand()
    send_outer(1, 2)
    local[3].wait()
    local[4].wait()
    wait_at_end(0)

    @pl.loop(0, pieces)
    def _(index):
        up_copy(index).wait_recv()

    make_hidden()

    @pl.loop(0, 2 * pieces + last + 3)
    def _(turn):
        @pl.when(turn < pieces)
        def _():
            down_copy(turn).wait_recv()

        @pl.when(turn == 1)
        def _():
            send_outer(2, 1)

        @pl.when(turn == 3)
        def _():
            send_outer(2, 2)

        @pl.when(turn == pieces)
        def _():
            make_pre_grad()

        @pl.loop(0, experts)
        def _(order):
            target = jnp.where(
                order < last - place,
                last - order,
                jnp.where(order < last, order - (last - place), place),
            )
            late = jnp.where(
                target > place,
                place,
                jnp.where(target < place, last - place, last + 3),
            )
            step = turn - late

            @pl.when((step >= 0) & (step < 2 * pieces))
            def _():
                member = jnp.where(step >= pieces, 1, 0)
                serve(target, member, step - member * pieces)

        @pl.when(turn == 2)
        def _():
            wait_at_end(1)
            make_slope()

        @pl.when(turn == pieces - 2)
        def _():
            wait_at_end(2)
            start_hidden_grad()

    for stream in range(3):
        for half in range(2):
            own_copy(stream, half).wait_send()

    @pl.when(is_inner)
    def _():
        for stream in range(3):
            for half in range(2):
                across_copy(stream, half).wait_send()
            for steps in range(experts - 1):
                outer_copy(stream, steps).wait_send()

    for copy in table_copies:
        copy.wait_send()

    @pl.loop(0, pieces)
    def _(index):
        up_copy(index).wait_send()
        down_copy(index).wait_send()
        for member in range(2):

            @pl.loop(1, experts)
            def _(ahead):
                target = lax.rem(place + ahead, experts)

                @pl.when(is_end)
                def _():
                    back_copy(member, target, index, capacity).wait_send()

                @pl.when(is_inner)
                def _():
                    back_copy(member, target, index, tokens).wait_send()

            shift_copy(member, index).wait()


def line_path(
    x_fwd,
    routes_fwd,
    affinity_fwd,
    x_bwd,
    grad_bwd,
    routes_bwd,
    affinity_bwd,
    up_weight,
    down_weight,
):
    devices = lax.axis_size("expert")
    sections = lax.axis_size("section")
    experts = devices // 2
    tokens, width = x_fwd.shape[1:]
    top_count = routes_fwd.shape[2]
    units = up_weight.shape[2]
    capacity = 3 * tokens * top_count // devices
    cut = piece_width(width)
    pieces = width // cut
    rows = experts * tokens
    bf16, f32 = jnp.bfloat16, jnp.float32
    dma = pltpu.SemaphoreType.DMA
    in_vmem = pl.BlockSpec(memory_space=pltpu.VMEM)
    anywhere = pl.BlockSpec(memory_space=pl.ANY)
    outs = pl.pallas_call(
        functools.partial(line_kernel, (sections, experts, tokens, capacity, pieces, cut)),
        name="expert_line",
        out_shape=[jax.ShapeDtypeStruct((tokens, width), bf16)] * 2,
        in_specs=[in_vmem] * 4 + [anywhere] * 5,
        out_specs=[anywhere] * 2,
        scratch_shapes=[
            pltpu.VMEM((3, rows, width), bf16),
            pltpu.VMEM((2, width, units), bf16),
            pltpu.VMEM((2, units, width), bf16),
            pltpu.VMEM((experts, 4 * experts, tokens), f32),
            pltpu.VMEM((rows, units), f32),
            pltpu.VMEM((2, rows, units), f32),
            pltpu.VMEM((2, rows, units), f32),
            pltpu.VMEM((2, rows, units), bf16),
            pltpu.VMEM((2, rows, units), bf16),
            pltpu.VMEM((2, experts + 1, pieces, tokens, cut), bf16),
            pltpu.VMEM((2, pieces, tokens, cut), bf16),
            pltpu.VMEM((3, experts - 1, capacity, width), bf16),
            pltpu.VMEM((2, experts, tokens, tokens), bf16),
            pltpu.VMEM((tokens, cut), f32),
            dma((5,)),
            dma((experts - 1,)),
            dma((experts,)),
            dma((3, 2)),
            dma((3, 2)),
            dma((3, experts - 1)),
            dma((3, experts, 2)),
            dma((pieces,)),
            dma((pieces,)),
            dma((pieces,)),
            dma((pieces,)),
            dma((2, experts, pieces)),
            dma((2, experts + 1, pieces)),
            dma((2, pieces)),
            dma((2, pieces)),
        ],
        compiler_params=pltpu.CompilerParams(
            collective_id=0, has_side_effects=True, vmem_limit_bytes=60 << 20
        ),
    )(
        routes_fwd[0].T,
        affinity_fwd[0].T,
        routes_bwd[0].T,
        affinity_bwd[0].T,
        x_fwd[0],
        x_bwd[0],
        grad_bwd[0],
        up_weight[0],
        down_weight[0],
    )
    return tuple(out[None] for out in outs)


def piece_width(width):
    for cut in (512, 256, 128):
        if width % cut == 0:
            return cut
    return 0


def per_device(*args):
    experts = lax.axis_size("expert") // 2
    tokens, width = args[0].shape[1:]
    if experts == 4 and tokens == 128 and piece_width(width):
        return line_path(*args)
    return general_path(*args)


def solution(mesh):
    in_specs = (
        P("section", "expert", None),
        P("section", "expert", None),
        P("section", "expert", None),
        P("section", "expert", None),
        P("section", "expert", None),
        P("section", "expert", None),
        P("section", "expert", None),
        P("section", None, "expert"),
        P("section", "expert", None),
    )
    out_specs = (P("section", "expert", None), P("section", "expert", None))
    return jax.shard_map(
        per_device, mesh=mesh, in_specs=in_specs, out_specs=out_specs, check_vma=False
    )
```

```python
import functools

import jax
import jax.numpy as jnp
from jax import lax
from jax.experimental import pallas as pl
from jax.experimental.pallas import tpu as pltpu
from jax.sharding import PartitionSpec as P

AGAINST_ROWS = (((1,), (1,)), ((), ()))


def from_partner_2(block, axis, apart):
    count = lax.axis_size(axis)
    route = []
    for low in range(count):
        high = low | 1 << apart
        if high != low and high < count:
            route += [(low, high), (high, low)]
    return lax.ppermute(block, axis, route)


def shifted(shard, axis, by):
    size = lax.axis_size(axis)
    return lax.ppermute(shard, axis, [(i, (i + by) % size) for i in range(size)])


def silu_grad(values):
    sigma = jax.nn.sigmoid(values)
    return sigma * (1.0 + values * (1.0 - sigma))


def slot_table(routes, experts, capacity):
    flat_routes = routes.reshape(-1)
    entries = flat_routes.shape[0]
    onehot = (flat_routes[:, None] == jnp.arange(experts, dtype=jnp.int32)[None, :]).astype(
        jnp.int32
    )
    before = jnp.cumsum(onehot, 0) - onehot
    position = jnp.sum(before * onehot, 1)
    slot_of = flat_routes * capacity + position
    source = (
        jnp.full((experts * capacity,), entries, jnp.int32)
        .at[slot_of]
        .set(jnp.arange(entries, dtype=jnp.int32))
    )
    return (slot_of, source)


def serve_rows(received, up_half, down_half):
    sources = received.shape[0]
    slots = received.shape[2]
    model_width = received.shape[3]
    row_count = sources * slots
    rows_fwd = received[:, 0].reshape(row_count, model_width)
    rows_saved = received[:, 1].reshape(row_count, model_width)
    rows_grad = received[:, 2].reshape(row_count, model_width)
    against_rows = (((1,), (1,)), ((), ()))
    hidden = jax.nn.silu(jnp.dot(rows_fwd, up_half, preferred_element_type=jnp.float32)).astype(
        jnp.bfloat16
    )
    part_fwd = jnp.dot(hidden, down_half, preferred_element_type=jnp.float32).astype(jnp.bfloat16)
    pre_act = jnp.dot(rows_saved, up_half, preferred_element_type=jnp.float32)
    hidden_grad = lax.dot_general(
        rows_grad, down_half, against_rows, preferred_element_type=jnp.float32
    )
    pre_grad = (hidden_grad * silu_grad(pre_act)).astype(jnp.bfloat16)
    part_bwd = lax.dot_general(
        pre_grad, up_half, against_rows, preferred_element_type=jnp.float32
    ).astype(jnp.bfloat16)
    return jnp.stack(
        [
            part_fwd.reshape(sources, slots, model_width),
            part_bwd.reshape(sources, slots, model_width),
        ],
        1,
    )


def combine(inputs, routed_rows, affinity):
    tokens = inputs.shape[0]
    top_count = affinity.shape[1]
    weights = affinity / jnp.sum(affinity, -1, keepdims=True)
    routed = routed_rows.reshape(tokens, top_count, inputs.shape[1]).astype(jnp.float32)
    return (inputs.astype(jnp.float32) + jnp.sum(weights[..., None] * routed, 1)).astype(
        jnp.bfloat16
    )


def general_path(
    x_fwd,
    routes_fwd,
    affinity_fwd,
    x_bwd,
    grad_bwd,
    routes_bwd,
    affinity_bwd,
    up_weight,
    down_weight,
):
    devices = lax.axis_size("expert")
    experts = devices // 2
    tokens = x_fwd.shape[1]
    model_width = x_fwd.shape[2]
    top_count = routes_fwd.shape[2]
    capacity = 3 * tokens * top_count // devices
    half_slots = capacity // 2
    up_half = up_weight[0]
    down_half = down_weight[0]
    slot_fwd, source_fwd = slot_table(routes_fwd[0], experts, capacity)
    slot_bwd, source_bwd = slot_table(routes_bwd[0], experts, capacity)
    zero_row = jnp.zeros((1, model_width), jnp.bfloat16)
    row_table = jnp.concatenate([x_fwd[0], zero_row, x_bwd[0], zero_row, grad_bwd[0], zero_row], 0)
    stride = tokens + 1
    token_fwd = (source_fwd // top_count).reshape(experts, capacity)
    token_bwd = (source_bwd // top_count).reshape(experts, capacity)
    gather_index = jnp.stack([token_fwd, token_bwd + stride, token_bwd + 2 * stride], 1)
    send_index = (
        gather_index.reshape(experts, 3, 2, half_slots)
        .transpose(0, 2, 1, 3)
        .reshape(devices, 3, half_slots)
    )
    outgoing = row_table[send_index]
    received = lax.all_to_all(outgoing, "expert", split_axis=0, concat_axis=0, tiled=True)
    partner = from_partner_2(received, "expert", 0)
    result = serve_rows(jnp.concatenate([received, partner], 2), up_half, down_half)
    piece_slots = received.shape[2]
    from_partner = from_partner_2(result[:, :, piece_slots:], "expert", 0)
    summed = (
        result[:, :, :piece_slots].astype(jnp.float32) + from_partner.astype(jnp.float32)
    ).astype(jnp.bfloat16)
    returned = lax.all_to_all(summed, "expert", split_axis=0, concat_axis=0, tiled=True)
    flat_back = returned.reshape(-1, model_width)

    def back_index(slot_of, member):
        expert_id = slot_of // capacity
        within = slot_of % capacity
        return (
            (2 * expert_id + within // half_slots) * 2 + member
        ) * half_slots + within % half_slots

    index_fwd = back_index(slot_fwd, 0)
    index_bwd = back_index(slot_bwd, 1)
    layer_out = combine(x_fwd[0], flat_back[index_fwd], affinity_fwd[0])
    input_grad = combine(grad_bwd[0], flat_back[index_bwd], affinity_bwd[0])
    fwd_next = shifted(layer_out[None], "section", 1)
    bwd_next = shifted(input_grad[None], "section", -1)
    return (fwd_next, bwd_next)


def line_kernel(
    sizes,
    routes_fwd,
    affinity_fwd,
    routes_bwd,
    affinity_bwd,
    x_fwd,
    x_bwd,
    grad_bwd,
    up,
    down,
    out_fwd,
    out_bwd,
    blocks,
    ups,
    downs,
    tables,
    total,
    slope,
    hidden_grad,
    hidden,
    pre_grad,
    returned,
    final,
    picked,
    expand,
    piece,
    local_sem,
    table_send,
    table_recv,
    own_send,
    across_send,
    outer_send,
    block_recv,
    up_send,
    up_recv,
    down_send,
    down_recv,
    back_send,
    back_recv,
    shift_send,
    shift_recv,
):
    sections, experts, tokens, capacity, pieces, cut, wide = sizes
    spans = pieces * cut // wide
    half_rows = tokens // 2
    streams = (x_fwd, x_bwd, grad_bwd)
    section = lax.axis_index("section")
    device = lax.axis_index("expert")
    place, side = device // 2, device % 2
    last = experts - 1
    is_inner = (place > 0) & (place < last)
    is_end = (place == 0) | (place == last)
    across = jnp.where(place < experts // 2, 1, -1)

    def at_place(where):
        return {"expert": where * 2 + side}

    def remote(src, dst, send, recv, target):
        return pltpu.make_async_remote_copy(
            src_ref=src,
            dst_ref=dst,
            send_sem=send,
            recv_sem=recv,
            device_id=target,
            device_id_type=pl.DeviceIdType.MESH,
        )

    partner = {"expert": place * 2 + 1 - side}
    next_section = {"section": lax.rem(section + 1, sections)}
    previous_section = {"section": lax.rem(section + sections - 1, sections)}
    column = [at_place(lax.rem(place + ahead, experts)) for ahead in range(1, experts)]

    barrier = pltpu.get_barrier_semaphore()
    peers = column + [partner, next_section, previous_section]
    for peer in peers:
        pl.semaphore_signal(
            barrier, inc=1, device_id=peer, device_id_type=pl.DeviceIdType.MESH
        )

    row_id = lax.broadcasted_iota(jnp.int32, (tokens, tokens), 0)
    lane_id = lax.broadcasted_iota(jnp.int32, (tokens, tokens), 1)
    later = jnp.where(row_id < lane_id, 1.0, 0.0).astype(jnp.bfloat16)
    expert_id = row_id[:16]
    for member, (routes, affinity) in enumerate(
        ((routes_fwd, affinity_fwd), (routes_bwd, affinity_bwd))
    ):
        weights = affinity[...] / jnp.sum(affinity[...], 0, keepdims=True)
        share = jnp.zeros(expert_id.shape, jnp.float32)
        named = jnp.zeros(expert_id.shape, jnp.float32)
        for choice in range(routes.shape[0]):
            same = routes[choice : choice + 1, :] == expert_id
            share += jnp.where(same, weights[choice : choice + 1, :], 0.0)
            named += jnp.where(same, 1.0, 0.0)
        rank = jnp.dot(named.astype(jnp.bfloat16), later, preferred_element_type=jnp.float32)
        rank = jnp.where(named > 0.5, rank, -1.0)
        base = member * 2 * experts
        tables[place, base : base + experts, :] = share[:experts]
        tables[place, base + experts : base + 2 * experts, :] = rank[:experts]

    pl.semaphore_wait(barrier, len(peers))
    table_copies = [
        remote(
            tables.at[place],
            tables.at[place],
            table_send.at[ahead],
            table_recv.at[place],
            column[ahead],
        )
        for ahead in range(experts - 1)
    ]
    for copy in table_copies:
        copy.start()

    def rows_of(origin):
        return pl.ds(pl.multiple_of(origin * tokens, tokens), tokens)

    def half_of(origin, half):
        return pl.ds(pl.multiple_of(origin * tokens + half * half_rows, half_rows), half_rows)

    def columns_of(index):
        return pl.ds(pl.multiple_of(index * cut, cut), cut)

    def span_of(index):
        return pl.ds(pl.multiple_of(index * wide, wide), wide)

    def own_copy(stream, half):
        return remote(
            streams[stream].at[pl.ds(half * half_rows, half_rows)],
            blocks.at[stream, half_of(place, half)],
            own_send.at[stream, half],
            block_recv.at[stream, place, half],
            at_place(place + across),
        )

    def send_own(stream):
        for half in range(2):
            own_copy(stream, half).start()

    def wait_half(stream, origin, half):
        block = blocks.at[stream, half_of(origin, half)]
        remote(
            block, block, own_send.at[stream, half], block_recv.at[stream, origin, half], partner
        ).wait_recv()

    def across_copy(stream, half):
        origin = place - across
        block = blocks.at[stream, half_of(origin, half)]
        return remote(
            block,
            block,
            across_send.at[stream, half],
            block_recv.at[stream, origin, half],
            at_place(place + across),
        )

    def send_across(stream, half):
        @pl.when(is_inner)
        def _():
            wait_half(stream, place - across, half)
            across_copy(stream, half).start()

    def outer_copy(stream, steps):
        origin = place + across * steps
        return remote(
            picked.at[stream, steps],
            blocks.at[stream, pl.ds(pl.multiple_of(origin * tokens, tokens), capacity)],
            outer_send.at[stream, steps],
            block_recv.at[stream, origin, 0],
            at_place(place - across),
        )

    def table_row(member, kind, origin, expert):
        return tables[origin, pl.ds((member * 2 + kind) * experts + expert, 1), :]

    def send_outer(stream, steps):
        @pl.when(is_inner)
        def _():
            origin = place + across * steps
            if steps:
                for half in range(2):
                    wait_half(stream, origin, half)
            ranks = table_row(min(stream, 1), 1, origin, place - across)
            slots = lax.broadcasted_iota(jnp.int32, (capacity, tokens), 0).astype(jnp.float32)
            pick = jnp.where(slots == ranks, 1.0, 0.0).astype(jnp.bfloat16)

            @pl.loop(0, spans)
            def _(index):
                picked[stream, steps, :, span_of(index)] = jnp.dot(
                    pick,
                    blocks[stream, rows_of(origin), span_of(index)],
                    preferred_element_type=jnp.float32,
                ).astype(jnp.bfloat16)

            outer_copy(stream, steps).start()

    def wait_at_end(stream):
        @pl.when(is_end)
        def _():
            for steps in range(1, experts):
                origin = place + across * steps
                landed = blocks.at[
                    stream, pl.ds(pl.multiple_of(origin * tokens, tokens), capacity)
                ]
                remote(
                    landed,
                    landed,
                    own_send.at[stream, 0],
                    block_recv.at[stream, origin, 0],
                    partner,
                ).wait_recv()

    def up_copy(index):
        rows = span_of(index)
        return remote(
            up.at[rows], ups.at[1, rows], up_send.at[index], up_recv.at[index], partner
        )

    def down_copy(index):
        rows = columns_of(index)
        return remote(
            down.at[:, rows],
            downs.at[1, :, rows],
            down_send.at[index],
            down_recv.at[index],
            partner,
        )

    send_own(0)

    @pl.loop(0, spans)
    def _(index):
        up_copy(index).start()

    @pl.loop(0, pieces)
    def _(index):
        down_copy(index).start()

    local = [
        pltpu.make_async_copy(
            streams[stream], blocks.at[stream, rows_of(place)], local_sem.at[stream]
        )
        for stream in range(3)
    ]
    local.append(pltpu.make_async_copy(up, ups.at[0], local_sem.at[3]))
    local.append(pltpu.make_async_copy(down, downs.at[0], local_sem.at[4]))
    for copy in local[:3]:
        copy.start()

    @pl.when(is_end)
    def _():
        for stream in range(3):
            for steps in range(1, experts):
                start = pl.multiple_of((place + across * steps) * tokens + capacity, 16)
                blocks[stream, pl.ds(start, tokens - capacity), :] = jnp.zeros(
                    (tokens - capacity, blocks.shape[2]), jnp.bfloat16
                )

    def wait_tables():
        for ahead in range(1, experts):
            origin = lax.rem(place + ahead, experts)
            remote(
                tables.at[origin],
                tables.at[origin],
                table_send.at[0],
                table_recv.at[origin],
                partner,
            ).wait_recv()

    def make_expand():
        @pl.when(is_inner)
        def _():
            @pl.loop(0, 2 * experts)
            def _(index):
                member = index // experts
                origin = index - member * experts
                ranks = table_row(member, 1, origin, place - across)
                rank = jnp.sum(jnp.where(row_id == lane_id, ranks, 0.0), 1, keepdims=True)
                expand[member, origin] = jnp.where(
                    lane_id.astype(jnp.float32) == rank, 1.0, 0.0
                ).astype(jnp.bfloat16)

    def weight_of(member, origin):
        packed = is_end & (origin != place)
        slots = row_id.astype(jnp.float32)
        lanes = lane_id[:1].astype(jnp.float32)
        ranks = jnp.where(packed, table_row(member, 1, origin, place), lanes)
        share = table_row(member, 0, origin, place)
        return jnp.sum(jnp.where(slots == ranks, share, 0.0), 1, keepdims=True)

    def project(stream, half):
        total[...] = jnp.zeros(total.shape, jnp.float32)

        @pl.loop(0, spans)
        def _(index):
            total[...] += jnp.dot(
                blocks[stream, :, span_of(index)],
                ups[half, span_of(index), :],
                preferred_element_type=jnp.float32,
            )

    def make_hidden():
        @pl.loop(0, 2)
        def _(half):
            project(0, half)

            @pl.loop(0, experts)
            def _(origin):
                act = total[rows_of(origin), :]
                hidden[half, rows_of(origin), :] = (
                    act / (1.0 + jnp.exp(-act)) * weight_of(0, origin)
                ).astype(jnp.bfloat16)

    def make_slope():
        @pl.loop(0, 2)
        def _(half):
            project(1, half)

            @pl.loop(0, experts)
            def _(origin):
                weight = weight_of(1, origin)
                act = total[rows_of(origin), :]
                sigma = 1.0 / (1.0 + jnp.exp(-act))
                slope[half, rows_of(origin), :] = (
                    sigma * (1.0 + act * (1.0 - sigma))
                ) * weight

    def add_hidden_grad(half, index):
        hidden_grad[half] += lax.dot_general(
            blocks[2, :, span_of(index)],
            downs[half, :, span_of(index)],
            AGAINST_ROWS,
            preferred_element_type=jnp.float32,
        )

    def start_hidden_grad():
        hidden_grad[...] = jnp.zeros(hidden_grad.shape, jnp.float32)

        @pl.loop(0, 2 * spans - 1)
        def _(index):
            half = index // spans
            add_hidden_grad(half, index - half * spans)

    def make_pre_grad():
        add_hidden_grad(1, spans - 1)

        @pl.loop(0, 2 * experts)
        def _(index):
            half = index // experts
            origin = index - half * experts
            rows = rows_of(origin)
            pre_grad[half, rows, :] = (
                hidden_grad[half, rows, :] * slope[half, rows, :]
            ).astype(jnp.bfloat16)

    def back_copy(member, target, index, count):
        way = jnp.where(target > place, 1, -1)
        there = place + way
        slot = jnp.where((way < 0) & (target == there), experts, target)
        return remote(
            returned.at[member, target, index, pl.ds(0, count)],
            returned.at[member, slot, index, pl.ds(0, count)],
            back_send.at[member, target, index],
            back_recv.at[member, slot, index],
            at_place(there),
        )

    def add_back(member, slot, index):
        landed = returned.at[member, slot, index]
        remote(
            landed,
            landed,
            back_send.at[member, 0, index],
            back_recv.at[member, slot, index],
            partner,
        ).wait_recv()
        piece[...] += returned[member, slot, index].astype(jnp.float32)

    def add_packed_back(member, slot, index, origin):
        landed = returned.at[member, slot, index, pl.ds(0, capacity)]
        remote(
            landed,
            landed,
            back_send.at[member, 0, index],
            back_recv.at[member, slot, index],
            partner,
        ).wait_recv()
        piece[...] += jnp.dot(
            expand[member, origin, :, :capacity],
            returned[member, slot, index, :capacity],
            preferred_element_type=jnp.float32,
        )

    def shift_copy(member, index):
        return remote(
            final.at[member, index],
            (out_fwd, out_bwd)[member].at[:, columns_of(index)],
            shift_send.at[member, index],
            shift_recv.at[member, index],
            (next_section, previous_section)[member],
        )

    def serve(target, member, index):
        rows = rows_of(target)

        @pl.when(member == 0)
        def _():
            piece[...] = jnp.dot(
                hidden[0, rows, :],
                downs[0, :, columns_of(index)],
                preferred_element_type=jnp.float32,
            ) + jnp.dot(
                hidden[1, rows, :],
                downs[1, :, columns_of(index)],
                preferred_element_type=jnp.float32,
            )

        @pl.when(member == 1)
        def _():
            piece[...] = lax.dot_general(
                pre_grad[0, rows, :],
                ups[0, columns_of(index), :],
                AGAINST_ROWS,
                preferred_element_type=jnp.float32,
            ) + lax.dot_general(
                pre_grad[1, rows, :],
                ups[1, columns_of(index), :],
                AGAINST_ROWS,
                preferred_element_type=jnp.float32,
            )

        @pl.when(target != place)
        def _():
            @pl.when(is_end)
            def _():
                returned[member, target, index] = piece[...].astype(jnp.bfloat16)
                back_copy(member, target, index, capacity).start()

            @pl.when(is_inner)
            def _():
                beyond = (target - place) * across > 0

                @pl.when(beyond)
                def _():
                    add_packed_back(member, target, index, target)

                @pl.when(jnp.logical_not(beyond))
                def _():
                    add_back(member, target, index)

                returned[member, target, index] = piece[...].astype(jnp.bfloat16)
                back_copy(member, target, index, tokens).start()

        @pl.when(target == place)
        def _():
            @pl.when(is_inner)
            def _():
                add_packed_back(
                    member, jnp.where(across > 0, place, experts), index, place
                )

            add_back(member, jnp.where(across > 0, experts, place), index)

            for each in range(2):

                @pl.when(member == each)
                def _(each=each):
                    final[each, index] = (
                        piece[...]
                        + blocks[2 * each, rows, columns_of(index)].astype(jnp.float32)
                    ).astype(jnp.bfloat16)
                    shift_copy(each, index).start()

    local[0].wait()
    send_outer(0, 0)
    send_across(0, 0)
    send_across(0, 1)
    send_own(1)
    for copy in local[3:]:
        copy.start()
    wait_tables()
    send_outer(0, 1)
    local[1].wait()
    send_outer(1, 0)
    send_across(1, 0)
    send_outer(0, 2)
    send_across(1, 1)
    send_own(2)
    send_outer(1, 1)
    local[2].wait()
    send_outer(2, 0)
    send_across(2, 0)
    send_across(2, 1)
    make_expand()
    send_outer(1, 2)
    local[3].wait()
    local[4].wait()
    wait_at_end(0)

    @pl.loop(0, spans)
    def _(index):
        up_copy(index).wait_recv()

    make_hidden()

    forward_lag = jnp.where(is_end, 9, 8)
    backward_lag = jnp.where(is_end, 9, 4)

    @pl.loop(0, 2 * pieces + 9)
    def _(turn):
        @pl.when(turn < pieces)
        def _():
            down_copy(turn).wait_recv()

        @pl.when(turn == pieces // 7)
        def _():
            send_outer(2, 1)

        @pl.when(turn == 3 * pieces // 7)
        def _():
            send_outer(2, 2)

        @pl.when(turn == pieces)
        def _():
            make_pre_grad()

        @pl.loop(0, experts + 1)
        def _(order):
            target = jnp.where(
                order < last - place,
                last - order,
                jnp.where(order < last, order - (last - place), place),
            )
            late = jnp.where(
                order < last,
                jnp.where(target > place, place, last - place),
                jnp.where(order == last, forward_lag, backward_lag),
            )
            step = turn - late
            low = jnp.where(order > last, pieces, 0)
            high = jnp.where(order == last, pieces, 2 * pieces)

            @pl.when((step >= low) & (step < high))
            def _():
                member = jnp.where(step >= pieces, 1, 0)
                serve(target, member, step - member * pieces)

        @pl.when(turn == 2 * pieces // 7)
        def _():
            wait_at_end(1)
            make_slope()

        @pl.when(turn == pieces - 1 - wide // cut)
        def _():
            wait_at_end(2)
            start_hidden_grad()

    for stream in range(3):
        for half in range(2):
            own_copy(stream, half).wait_send()

    @pl.when(is_inner)
    def _():
        for stream in range(3):
            for half in range(2):
                across_copy(stream, half).wait_send()
            for steps in range(experts - 1):
                outer_copy(stream, steps).wait_send()

    for copy in table_copies:
        copy.wait_send()

    @pl.loop(0, spans)
    def _(index):
        up_copy(index).wait_send()

    @pl.loop(0, pieces)
    def _(index):
        down_copy(index).wait_send()
        for member in range(2):

            @pl.loop(1, experts)
            def _(ahead):
                target = lax.rem(place + ahead, experts)

                @pl.when(is_end)
                def _():
                    back_copy(member, target, index, capacity).wait_send()

                @pl.when(is_inner)
                def _():
                    back_copy(member, target, index, tokens).wait_send()

            shift_copy(member, index).wait()


def line_path(
    x_fwd,
    routes_fwd,
    affinity_fwd,
    x_bwd,
    grad_bwd,
    routes_bwd,
    affinity_bwd,
    up_weight,
    down_weight,
):
    devices = lax.axis_size("expert")
    sections = lax.axis_size("section")
    experts = devices // 2
    tokens, width = x_fwd.shape[1:]
    top_count = routes_fwd.shape[2]
    units = up_weight.shape[2]
    capacity = 3 * tokens * top_count // devices
    wide = piece_width(width)
    cut = wide // 2
    pieces = width // cut
    spans = width // wide
    rows = experts * tokens
    bf16, f32 = jnp.bfloat16, jnp.float32
    dma = pltpu.SemaphoreType.DMA
    in_vmem = pl.BlockSpec(memory_space=pltpu.VMEM)
    anywhere = pl.BlockSpec(memory_space=pl.ANY)
    outs = pl.pallas_call(
        functools.partial(line_kernel, (sections, experts, tokens, capacity, pieces, cut, wide)),
        name="expert_line",
        out_shape=[pltpu.VMEM((tokens, width), bf16)] * 2,
        in_specs=[in_vmem] * 4 + [anywhere] * 5,
        out_specs=[in_vmem] * 2,
        scratch_shapes=[
            pltpu.VMEM((3, rows, width), bf16),
            pltpu.VMEM((2, width, units), bf16),
            pltpu.VMEM((2, units, width), bf16),
            pltpu.VMEM((experts, 4 * experts, tokens), f32),
            pltpu.VMEM((rows, units), f32),
            pltpu.VMEM((2, rows, units), f32),
            pltpu.VMEM((2, rows, units), f32),
            pltpu.VMEM((2, rows, units), bf16),
            pltpu.VMEM((2, rows, units), bf16),
            pltpu.VMEM((2, experts + 1, pieces, tokens, cut), bf16),
            pltpu.VMEM((2, pieces, tokens, cut), bf16),
            pltpu.VMEM((3, experts - 1, capacity, width), bf16),
            pltpu.VMEM((2, experts, tokens, tokens), bf16),
            pltpu.VMEM((tokens, cut), f32),
            dma((5,)),
            dma((experts - 1,)),
            dma((experts,)),
            dma((3, 2)),
            dma((3, 2)),
            dma((3, experts - 1)),
            dma((3, experts, 2)),
            dma((spans,)),
            dma((spans,)),
            dma((pieces,)),
            dma((pieces,)),
            dma((2, experts, pieces)),
            dma((2, experts + 1, pieces)),
            dma((2, pieces)),
            dma((2, pieces)),
        ],
        compiler_params=pltpu.CompilerParams(
            collective_id=0, has_side_effects=True, vmem_limit_bytes=56 << 20
        ),
    )(
        routes_fwd[0].T,
        affinity_fwd[0].T,
        routes_bwd[0].T,
        affinity_bwd[0].T,
        x_fwd[0],
        x_bwd[0],
        grad_bwd[0],
        up_weight[0],
        down_weight[0],
    )
    return tuple(out[None] for out in outs)


def piece_width(width):
    for wide in (512, 256):
        if width % wide == 0:
            return wide
    return 0


def per_device(*args):
    experts = lax.axis_size("expert") // 2
    tokens, width = args[0].shape[1:]
    if experts == 4 and tokens == 128 and piece_width(width):
        return line_path(*args)
    return general_path(*args)


def solution(mesh):
    in_specs = (
        P("section", "expert", None),
        P("section", "expert", None),
        P("section", "expert", None),
        P("section", "expert", None),
        P("section", "expert", None),
        P("section", "expert", None),
        P("section", "expert", None),
        P("section", None, "expert"),
        P("section", "expert", None),
    )
    out_specs = (P("section", "expert", None), P("section", "expert", None))
    return jax.shard_map(
        per_device, mesh=mesh, in_specs=in_specs, out_specs=out_specs, check_vma=False
    )
```

```python
import functools

import jax
import jax.numpy as jnp
from jax import lax
from jax.experimental import pallas as pl
from jax.experimental.pallas import tpu as pltpu
from jax.sharding import PartitionSpec as P

AGAINST_ROWS = (((1,), (1,)), ((), ()))


def from_partner_2(block, axis, apart):
    count = lax.axis_size(axis)
    route = []
    for low in range(count):
        high = low | 1 << apart
        if high != low and high < count:
            route += [(low, high), (high, low)]
    return lax.ppermute(block, axis, route)


def shifted(shard, axis, by):
    size = lax.axis_size(axis)
    return lax.ppermute(shard, axis, [(i, (i + by) % size) for i in range(size)])


def silu_grad(values):
    sigma = jax.nn.sigmoid(values)
    return sigma * (1.0 + values * (1.0 - sigma))


def slot_table(routes, experts, capacity):
    flat_routes = routes.reshape(-1)
    entries = flat_routes.shape[0]
    onehot = (flat_routes[:, None] == jnp.arange(experts, dtype=jnp.int32)[None, :]).astype(
        jnp.int32
    )
    before = jnp.cumsum(onehot, 0) - onehot
    position = jnp.sum(before * onehot, 1)
    slot_of = flat_routes * capacity + position
    source = (
        jnp.full((experts * capacity,), entries, jnp.int32)
        .at[slot_of]
        .set(jnp.arange(entries, dtype=jnp.int32))
    )
    return (slot_of, source)


def serve_rows(received, up_half, down_half):
    sources = received.shape[0]
    slots = received.shape[2]
    model_width = received.shape[3]
    row_count = sources * slots
    rows_fwd = received[:, 0].reshape(row_count, model_width)
    rows_saved = received[:, 1].reshape(row_count, model_width)
    rows_grad = received[:, 2].reshape(row_count, model_width)
    against_rows = (((1,), (1,)), ((), ()))
    hidden = jax.nn.silu(jnp.dot(rows_fwd, up_half, preferred_element_type=jnp.float32)).astype(
        jnp.bfloat16
    )
    part_fwd = jnp.dot(hidden, down_half, preferred_element_type=jnp.float32).astype(jnp.bfloat16)
    pre_act = jnp.dot(rows_saved, up_half, preferred_element_type=jnp.float32)
    hidden_grad = lax.dot_general(
        rows_grad, down_half, against_rows, preferred_element_type=jnp.float32
    )
    pre_grad = (hidden_grad * silu_grad(pre_act)).astype(jnp.bfloat16)
    part_bwd = lax.dot_general(
        pre_grad, up_half, against_rows, preferred_element_type=jnp.float32
    ).astype(jnp.bfloat16)
    return jnp.stack(
        [
            part_fwd.reshape(sources, slots, model_width),
            part_bwd.reshape(sources, slots, model_width),
        ],
        1,
    )


def combine(inputs, routed_rows, affinity):
    tokens = inputs.shape[0]
    top_count = affinity.shape[1]
    weights = affinity / jnp.sum(affinity, -1, keepdims=True)
    routed = routed_rows.reshape(tokens, top_count, inputs.shape[1]).astype(jnp.float32)
    return (inputs.astype(jnp.float32) + jnp.sum(weights[..., None] * routed, 1)).astype(
        jnp.bfloat16
    )


def general_path(
    x_fwd,
    routes_fwd,
    affinity_fwd,
    x_bwd,
    grad_bwd,
    routes_bwd,
    affinity_bwd,
    up_weight,
    down_weight,
):
    devices = lax.axis_size("expert")
    experts = devices // 2
    tokens = x_fwd.shape[1]
    model_width = x_fwd.shape[2]
    top_count = routes_fwd.shape[2]
    capacity = 3 * tokens * top_count // devices
    half_slots = capacity // 2
    up_half = up_weight[0]
    down_half = down_weight[0]
    slot_fwd, source_fwd = slot_table(routes_fwd[0], experts, capacity)
    slot_bwd, source_bwd = slot_table(routes_bwd[0], experts, capacity)
    zero_row = jnp.zeros((1, model_width), jnp.bfloat16)
    row_table = jnp.concatenate([x_fwd[0], zero_row, x_bwd[0], zero_row, grad_bwd[0], zero_row], 0)
    stride = tokens + 1
    token_fwd = (source_fwd // top_count).reshape(experts, capacity)
    token_bwd = (source_bwd // top_count).reshape(experts, capacity)
    gather_index = jnp.stack([token_fwd, token_bwd + stride, token_bwd + 2 * stride], 1)
    send_index = (
        gather_index.reshape(experts, 3, 2, half_slots)
        .transpose(0, 2, 1, 3)
        .reshape(devices, 3, half_slots)
    )
    outgoing = row_table[send_index]
    received = lax.all_to_all(outgoing, "expert", split_axis=0, concat_axis=0, tiled=True)
    partner = from_partner_2(received, "expert", 0)
    result = serve_rows(jnp.concatenate([received, partner], 2), up_half, down_half)
    piece_slots = received.shape[2]
    from_partner = from_partner_2(result[:, :, piece_slots:], "expert", 0)
    summed = (
        result[:, :, :piece_slots].astype(jnp.float32) + from_partner.astype(jnp.float32)
    ).astype(jnp.bfloat16)
    returned = lax.all_to_all(summed, "expert", split_axis=0, concat_axis=0, tiled=True)
    flat_back = returned.reshape(-1, model_width)

    def back_index(slot_of, member):
        expert_id = slot_of // capacity
        within = slot_of % capacity
        return (
            (2 * expert_id + within // half_slots) * 2 + member
        ) * half_slots + within % half_slots

    index_fwd = back_index(slot_fwd, 0)
    index_bwd = back_index(slot_bwd, 1)
    layer_out = combine(x_fwd[0], flat_back[index_fwd], affinity_fwd[0])
    input_grad = combine(grad_bwd[0], flat_back[index_bwd], affinity_bwd[0])
    fwd_next = shifted(layer_out[None], "section", 1)
    bwd_next = shifted(input_grad[None], "section", -1)
    return (fwd_next, bwd_next)


def line_kernel(
    sizes,
    routes_fwd,
    affinity_fwd,
    routes_bwd,
    affinity_bwd,
    x_fwd,
    x_bwd,
    grad_bwd,
    up,
    down,
    out_fwd,
    out_bwd,
    blocks,
    ups,
    downs,
    tables,
    total,
    slope,
    hidden_grad,
    hidden,
    pre_grad,
    returned,
    final,
    picked,
    expand,
    piece,
    local_sem,
    table_send,
    table_recv,
    own_send,
    across_send,
    outer_send,
    block_recv,
    up_send,
    up_recv,
    down_send,
    down_recv,
    back_send,
    back_recv,
    shift_send,
    shift_recv,
):
    sections, experts, tokens, capacity, pieces, cut, wide = sizes
    spans = pieces * cut // wide
    half_rows = tokens // 2
    streams = (x_fwd, x_bwd, grad_bwd)
    section = lax.axis_index("section")
    device = lax.axis_index("expert")
    place, side = device // 2, device % 2
    last = experts - 1
    is_inner = (place > 0) & (place < last)
    is_end = (place == 0) | (place == last)
    across = jnp.where(place < experts // 2, 1, -1)

    def at_place(where):
        return {"expert": where * 2 + side}

    def remote(src, dst, send, recv, target):
        return pltpu.make_async_remote_copy(
            src_ref=src,
            dst_ref=dst,
            send_sem=send,
            recv_sem=recv,
            device_id=target,
            device_id_type=pl.DeviceIdType.MESH,
        )

    partner = {"expert": place * 2 + 1 - side}
    next_section = {"section": lax.rem(section + 1, sections)}
    previous_section = {"section": lax.rem(section + sections - 1, sections)}
    column = [at_place(lax.rem(place + ahead, experts)) for ahead in range(1, experts)]

    barrier = pltpu.get_barrier_semaphore()
    peers = column + [partner, next_section, previous_section]
    for peer in peers:
        pl.semaphore_signal(
            barrier, inc=1, device_id=peer, device_id_type=pl.DeviceIdType.MESH
        )

    row_id = lax.broadcasted_iota(jnp.int32, (tokens, tokens), 0)
    lane_id = lax.broadcasted_iota(jnp.int32, (tokens, tokens), 1)
    later = jnp.where(row_id < lane_id, 1.0, 0.0).astype(jnp.bfloat16)
    expert_id = row_id[:16]
    for member, (routes, affinity) in enumerate(
        ((routes_fwd, affinity_fwd), (routes_bwd, affinity_bwd))
    ):
        weights = affinity[...] / jnp.sum(affinity[...], 0, keepdims=True)
        share = jnp.zeros(expert_id.shape, jnp.float32)
        named = jnp.zeros(expert_id.shape, jnp.float32)
        for choice in range(routes.shape[0]):
            same = routes[choice : choice + 1, :] == expert_id
            share += jnp.where(same, weights[choice : choice + 1, :], 0.0)
            named += jnp.where(same, 1.0, 0.0)
        rank = jnp.dot(named.astype(jnp.bfloat16), later, preferred_element_type=jnp.float32)
        rank = jnp.where(named > 0.5, rank, -1.0)
        base = member * 2 * experts
        tables[place, base : base + experts, :] = share[:experts]
        tables[place, base + experts : base + 2 * experts, :] = rank[:experts]

    pl.semaphore_wait(barrier, len(peers))
    table_copies = [
        remote(
            tables.at[place],
            tables.at[place],
            table_send.at[ahead],
            table_recv.at[place],
            column[ahead],
        )
        for ahead in range(experts - 1)
    ]
    for copy in table_copies:
        copy.start()

    def rows_of(origin):
        return pl.ds(pl.multiple_of(origin * tokens, tokens), tokens)

    def half_of(origin, half):
        return pl.ds(pl.multiple_of(origin * tokens + half * half_rows, half_rows), half_rows)

    def columns_of(index):
        return pl.ds(pl.multiple_of(index * cut, cut), cut)

    def span_of(index):
        return pl.ds(pl.multiple_of(index * wide, wide), wide)

    def own_copy(stream, half):
        return remote(
            streams[stream].at[pl.ds(half * half_rows, half_rows)],
            blocks.at[stream, half_of(place, half)],
            own_send.at[stream, half],
            block_recv.at[stream, place, half],
            at_place(place + across),
        )

    def send_own(stream):
        for half in range(2):
            own_copy(stream, half).start()

    def wait_half(stream, origin, half):
        block = blocks.at[stream, half_of(origin, half)]
        remote(
            block, block, own_send.at[stream, half], block_recv.at[stream, origin, half], partner
        ).wait_recv()

    def across_copy(stream, half):
        origin = place - across
        block = blocks.at[stream, half_of(origin, half)]
        return remote(
            block,
            block,
            across_send.at[stream, half],
            block_recv.at[stream, origin, half],
            at_place(place + across),
        )

    def send_across(stream, half):
        @pl.when(is_inner)
        def _():
            wait_half(stream, place - across, half)
            across_copy(stream, half).start()

    def outer_copy(stream, steps):
        origin = place + across * steps
        return remote(
            picked.at[stream, steps],
            blocks.at[stream, pl.ds(pl.multiple_of(origin * tokens, tokens), capacity)],
            outer_send.at[stream, steps],
            block_recv.at[stream, origin, 0],
            at_place(place - across),
        )

    def table_row(member, kind, origin, expert):
        return tables[origin, pl.ds((member * 2 + kind) * experts + expert, 1), :]

    def send_outer(stream, steps):
        @pl.when(is_inner)
        def _():
            origin = place + across * steps
            if steps:
                for half in range(2):
                    wait_half(stream, origin, half)
            ranks = table_row(min(stream, 1), 1, origin, place - across)
            slots = lax.broadcasted_iota(jnp.int32, (capacity, tokens), 0).astype(jnp.float32)
            pick = jnp.where(slots == ranks, 1.0, 0.0).astype(jnp.bfloat16)

            @pl.loop(0, spans)
            def _(index):
                picked[stream, steps, :, span_of(index)] = jnp.dot(
                    pick,
                    blocks[stream, rows_of(origin), span_of(index)],
                    preferred_element_type=jnp.float32,
                ).astype(jnp.bfloat16)

            outer_copy(stream, steps).start()

    def wait_at_end(stream):
        @pl.when(is_end)
        def _():
            for steps in range(1, experts):
                origin = place + across * steps
                landed = blocks.at[
                    stream, pl.ds(pl.multiple_of(origin * tokens, tokens), capacity)
                ]
                remote(
                    landed,
                    landed,
                    own_send.at[stream, 0],
                    block_recv.at[stream, origin, 0],
                    partner,
                ).wait_recv()

    def up_copy(index):
        rows = span_of(index)
        return remote(
            up.at[rows], ups.at[1, rows], up_send.at[index], up_recv.at[index], partner
        )

    def down_copy(index):
        rows = columns_of(index)
        return remote(
            down.at[:, rows],
            downs.at[1, :, rows],
            down_send.at[index],
            down_recv.at[index],
            partner,
        )

    send_own(0)

    @pl.loop(0, spans)
    def _(index):
        up_copy(index).start()

    @pl.loop(0, pieces)
    def _(index):
        down_copy(index).start()

    local = [
        pltpu.make_async_copy(
            streams[stream], blocks.at[stream, rows_of(place)], local_sem.at[stream]
        )
        for stream in range(3)
    ]
    local.append(pltpu.make_async_copy(up, ups.at[0], local_sem.at[3]))
    local.append(pltpu.make_async_copy(down, downs.at[0], local_sem.at[4]))
    for copy in local[:3]:
        copy.start()

    @pl.when(is_end)
    def _():
        for stream in range(3):
            for steps in range(1, experts):
                start = pl.multiple_of((place + across * steps) * tokens + capacity, 16)
                blocks[stream, pl.ds(start, tokens - capacity), :] = jnp.zeros(
                    (tokens - capacity, blocks.shape[2]), jnp.bfloat16
                )

    def wait_tables():
        for ahead in range(1, experts):
            origin = lax.rem(place + ahead, experts)
            remote(
                tables.at[origin],
                tables.at[origin],
                table_send.at[0],
                table_recv.at[origin],
                partner,
            ).wait_recv()

    def make_expand():
        @pl.when(is_inner)
        def _():
            @pl.loop(0, 2 * experts)
            def _(index):
                member = index // experts
                origin = index - member * experts
                ranks = table_row(member, 1, origin, place - across)
                rank = jnp.sum(jnp.where(row_id == lane_id, ranks, 0.0), 1, keepdims=True)
                expand[member, origin] = jnp.where(
                    lane_id.astype(jnp.float32) == rank, 1.0, 0.0
                ).astype(jnp.bfloat16)

    def weight_of(member, origin):
        packed = is_end & (origin != place)
        slots = row_id.astype(jnp.float32)
        lanes = lane_id[:1].astype(jnp.float32)
        ranks = jnp.where(packed, table_row(member, 1, origin, place), lanes)
        share = table_row(member, 0, origin, place)
        return jnp.sum(jnp.where(slots == ranks, share, 0.0), 1, keepdims=True)

    def project(stream, half):
        total[...] = jnp.zeros(total.shape, jnp.float32)

        @pl.loop(0, spans)
        def _(index):
            total[...] += jnp.dot(
                blocks[stream, :, span_of(index)],
                ups[half, span_of(index), :],
                preferred_element_type=jnp.float32,
            )

    def make_hidden():
        @pl.loop(0, 2)
        def _(half):
            project(0, half)

            @pl.loop(0, experts)
            def _(origin):
                act = total[rows_of(origin), :]
                hidden[half, rows_of(origin), :] = (
                    act / (1.0 + jnp.exp(-act)) * weight_of(0, origin)
                ).astype(jnp.bfloat16)

    def make_slope():
        @pl.loop(0, 2)
        def _(half):
            project(1, half)

            @pl.loop(0, experts)
            def _(origin):
                weight = weight_of(1, origin)
                act = total[rows_of(origin), :]
                sigma = 1.0 / (1.0 + jnp.exp(-act))
                slope[half, rows_of(origin), :] = (
                    sigma * (1.0 + act * (1.0 - sigma))
                ) * weight

    def add_hidden_grad(half, index):
        hidden_grad[half] += lax.dot_general(
            blocks[2, :, span_of(index)],
            downs[half, :, span_of(index)],
            AGAINST_ROWS,
            preferred_element_type=jnp.float32,
        )

    def start_hidden_grad():
        hidden_grad[...] = jnp.zeros(hidden_grad.shape, jnp.float32)

        @pl.loop(0, 2 * spans - 1)
        def _(index):
            half = index // spans
            add_hidden_grad(half, index - half * spans)

    def make_pre_grad():
        add_hidden_grad(1, spans - 1)

        @pl.loop(0, 2 * experts)
        def _(index):
            half = index // experts
            origin = index - half * experts
            rows = rows_of(origin)
            pre_grad[half, rows, :] = (
                hidden_grad[half, rows, :] * slope[half, rows, :]
            ).astype(jnp.bfloat16)

    def back_copy(member, target, index, count):
        way = jnp.where(target > place, 1, -1)
        there = place + way
        slot = jnp.where((way < 0) & (target == there), experts, target)
        return remote(
            returned.at[member, target, index, pl.ds(0, count)],
            returned.at[member, slot, index, pl.ds(0, count)],
            back_send.at[member, target, index],
            back_recv.at[member, slot, index],
            at_place(there),
        )

    def add_back(member, slot, index):
        landed = returned.at[member, slot, index]
        remote(
            landed,
            landed,
            back_send.at[member, 0, index],
            back_recv.at[member, slot, index],
            partner,
        ).wait_recv()
        piece[...] += returned[member, slot, index].astype(jnp.float32)

    def add_packed_back(member, slot, index, origin):
        landed = returned.at[member, slot, index, pl.ds(0, capacity)]
        remote(
            landed,
            landed,
            back_send.at[member, 0, index],
            back_recv.at[member, slot, index],
            partner,
        ).wait_recv()
        piece[...] += jnp.dot(
            expand[member, origin, :, :capacity],
            returned[member, slot, index, :capacity],
            preferred_element_type=jnp.float32,
        )

    def shift_copy(member, index):
        return remote(
            final.at[member, index],
            (out_fwd, out_bwd)[member].at[:, columns_of(index)],
            shift_send.at[member, index],
            shift_recv.at[member, index],
            (next_section, previous_section)[member],
        )

    def serve(target, member, index):
        rows = rows_of(target)

        @pl.when(member == 0)
        def _():
            piece[...] = jnp.dot(
                hidden[0, rows, :],
                downs[0, :, columns_of(index)],
                preferred_element_type=jnp.float32,
            ) + jnp.dot(
                hidden[1, rows, :],
                downs[1, :, columns_of(index)],
                preferred_element_type=jnp.float32,
            )

        @pl.when(member == 1)
        def _():
            piece[...] = lax.dot_general(
                pre_grad[0, rows, :],
                ups[0, columns_of(index), :],
                AGAINST_ROWS,
                preferred_element_type=jnp.float32,
            ) + lax.dot_general(
                pre_grad[1, rows, :],
                ups[1, columns_of(index), :],
                AGAINST_ROWS,
                preferred_element_type=jnp.float32,
            )

        @pl.when(target != place)
        def _():
            @pl.when(is_end)
            def _():
                returned[member, target, index] = piece[...].astype(jnp.bfloat16)
                back_copy(member, target, index, capacity).start()

            @pl.when(is_inner)
            def _():
                beyond = (target - place) * across > 0

                @pl.when(beyond)
                def _():
                    add_packed_back(member, target, index, target)

                @pl.when(jnp.logical_not(beyond))
                def _():
                    add_back(member, target, index)

                returned[member, target, index] = piece[...].astype(jnp.bfloat16)
                back_copy(member, target, index, tokens).start()

        @pl.when(target == place)
        def _():
            @pl.when(is_inner)
            def _():
                add_packed_back(
                    member, jnp.where(across > 0, place, experts), index, place
                )

            add_back(member, jnp.where(across > 0, experts, place), index)

            for each in range(2):

                @pl.when(member == each)
                def _(each=each):
                    final[each, index] = (
                        piece[...]
                        + blocks[2 * each, rows, columns_of(index)].astype(jnp.float32)
                    ).astype(jnp.bfloat16)
                    shift_copy(each, index).start()

    local[0].wait()
    send_outer(0, 0)
    send_across(0, 0)
    send_across(0, 1)
    send_own(1)
    for copy in local[3:]:
        copy.start()
    wait_tables()
    send_outer(0, 1)
    local[1].wait()
    send_outer(1, 0)
    send_across(1, 0)
    send_outer(0, 2)
    send_across(1, 1)
    send_own(2)
    send_outer(1, 1)
    local[2].wait()
    send_outer(2, 0)
    send_across(2, 0)
    send_across(2, 1)
    make_expand()
    send_outer(1, 2)
    local[3].wait()
    local[4].wait()
    wait_at_end(0)

    @pl.loop(0, spans)
    def _(index):
        up_copy(index).wait_recv()

    make_hidden()

    reach = jnp.where(is_end, last, last - 1)
    gate = pieces // 2

    def arrived(tick):
        steady = jnp.where(tick < pieces, tick - 2, jnp.maximum(pieces - 3, tick - 6))
        return jnp.clip(jnp.minimum(2 * (tick - gate), steady), 0, pieces)

    def own_arrived(tick):
        early = arrived(jnp.minimum(tick, pieces - 1) - 2)
        at_end = jnp.where(tick < (1 + last) * pieces, early, pieces)
        return jnp.where(is_end, at_end, arrived(tick))

    @pl.loop(0, (2 + last) * pieces)
    def _(tick):
        @pl.when(tick < pieces)
        def _():
            down_copy(tick).wait_recv()

        @pl.when(tick == pieces // 7)
        def _():
            send_outer(2, 1)

        @pl.when(tick == 3 * pieces // 7)
        def _():
            send_outer(2, 2)

        @pl.when(tick == pieces)
        def _():
            make_pre_grad()

        ready = jnp.where(is_end, tick, tick - 1)

        @pl.when((ready >= 0) & (ready < pieces))
        def _():
            @pl.loop(0, reach)
            def _(nearer):
                serve(place + across * (reach - nearer), 0, ready)

        later_step = tick - pieces - jnp.where(is_end, 0, 2)

        @pl.when((later_step >= 0) & (later_step < (reach + 1) * pieces))
        def _():
            nearer = later_step // pieces
            serve(place + across * (reach - nearer), 1, later_step - nearer * pieces)

        @pl.when(is_inner)
        def _():
            @pl.loop(arrived(tick - 1), arrived(tick))
            def _(index):
                serve(place - across, 0, index)

            outer_step = later_step - 3

            @pl.when((outer_step >= 0) & (outer_step < pieces))
            def _():
                serve(place - across, 1, outer_step)

        @pl.loop(own_arrived(tick - 1), own_arrived(tick))
        def _(index):
            serve(place, 0, index)

        @pl.when(tick == 2 * pieces // 7)
        def _():
            wait_at_end(1)
            make_slope()

        @pl.when(tick == pieces - 1 - wide // cut)
        def _():
            wait_at_end(2)
            start_hidden_grad()

    for stream in range(3):
        for half in range(2):
            own_copy(stream, half).wait_send()

    @pl.when(is_inner)
    def _():
        for stream in range(3):
            for half in range(2):
                across_copy(stream, half).wait_send()
            for steps in range(experts - 1):
                outer_copy(stream, steps).wait_send()

    for copy in table_copies:
        copy.wait_send()

    @pl.loop(0, spans)
    def _(index):
        up_copy(index).wait_send()

    @pl.loop(0, pieces)
    def _(index):
        down_copy(index).wait_send()
        for member in range(2):

            @pl.loop(1, experts)
            def _(ahead):
                target = lax.rem(place + ahead, experts)

                @pl.when(is_end)
                def _():
                    back_copy(member, target, index, capacity).wait_send()

                @pl.when(is_inner)
                def _():
                    back_copy(member, target, index, tokens).wait_send()

            shift_copy(member, index).wait()


def line_path(
    x_fwd,
    routes_fwd,
    affinity_fwd,
    x_bwd,
    grad_bwd,
    routes_bwd,
    affinity_bwd,
    up_weight,
    down_weight,
):
    devices = lax.axis_size("expert")
    sections = lax.axis_size("section")
    experts = devices // 2
    tokens, width = x_fwd.shape[1:]
    top_count = routes_fwd.shape[2]
    units = up_weight.shape[2]
    capacity = 3 * tokens * top_count // devices
    wide = piece_width(width)
    cut = wide // 2
    pieces = width // cut
    spans = width // wide
    rows = experts * tokens
    bf16, f32 = jnp.bfloat16, jnp.float32
    dma = pltpu.SemaphoreType.DMA
    in_vmem = pl.BlockSpec(memory_space=pltpu.VMEM)
    anywhere = pl.BlockSpec(memory_space=pl.ANY)
    outs = pl.pallas_call(
        functools.partial(line_kernel, (sections, experts, tokens, capacity, pieces, cut, wide)),
        name="expert_line",
        out_shape=[pltpu.VMEM((tokens, width), bf16)] * 2,
        in_specs=[in_vmem] * 4 + [anywhere] * 5,
        out_specs=[in_vmem] * 2,
        scratch_shapes=[
            pltpu.VMEM((3, rows, width), bf16),
            pltpu.VMEM((2, width, units), bf16),
            pltpu.VMEM((2, units, width), bf16),
            pltpu.VMEM((experts, 4 * experts, tokens), f32),
            pltpu.VMEM((rows, units), f32),
            pltpu.VMEM((2, rows, units), f32),
            pltpu.VMEM((2, rows, units), f32),
            pltpu.VMEM((2, rows, units), bf16),
            pltpu.VMEM((2, rows, units), bf16),
            pltpu.VMEM((2, experts + 1, pieces, tokens, cut), bf16),
            pltpu.VMEM((2, pieces, tokens, cut), bf16),
            pltpu.VMEM((3, experts - 1, capacity, width), bf16),
            pltpu.VMEM((2, experts, tokens, tokens), bf16),
            pltpu.VMEM((tokens, cut), f32),
            dma((5,)),
            dma((experts - 1,)),
            dma((experts,)),
            dma((3, 2)),
            dma((3, 2)),
            dma((3, experts - 1)),
            dma((3, experts, 2)),
            dma((spans,)),
            dma((spans,)),
            dma((pieces,)),
            dma((pieces,)),
            dma((2, experts, pieces)),
            dma((2, experts + 1, pieces)),
            dma((2, pieces)),
            dma((2, pieces)),
        ],
        compiler_params=pltpu.CompilerParams(
            collective_id=0, has_side_effects=True, vmem_limit_bytes=56 << 20
        ),
    )(
        routes_fwd[0].T,
        affinity_fwd[0].T,
        routes_bwd[0].T,
        affinity_bwd[0].T,
        x_fwd[0],
        x_bwd[0],
        grad_bwd[0],
        up_weight[0],
        down_weight[0],
    )
    return tuple(out[None] for out in outs)


def piece_width(width):
    for wide in (512, 256):
        if width % wide == 0:
            return wide
    return 0


def per_device(*args):
    experts = lax.axis_size("expert") // 2
    tokens, width = args[0].shape[1:]
    if experts == 4 and tokens == 128 and piece_width(width):
        return line_path(*args)
    return general_path(*args)


def solution(mesh):
    in_specs = (
        P("section", "expert", None),
        P("section", "expert", None),
        P("section", "expert", None),
        P("section", "expert", None),
        P("section", "expert", None),
        P("section", "expert", None),
        P("section", "expert", None),
        P("section", None, "expert"),
        P("section", "expert", None),
    )
    out_specs = (P("section", "expert", None), P("section", "expert", None))
    return jax.shard_map(
        per_device, mesh=mesh, in_specs=in_specs, out_specs=out_specs, check_vma=False
    )
```

```python
import functools

import jax
import jax.numpy as jnp
from jax import lax
from jax.experimental import pallas as pl
from jax.experimental.pallas import tpu as pltpu
from jax.sharding import PartitionSpec as P

AGAINST_ROWS = (((1,), (1,)), ((), ()))


def from_partner_2(block, axis, apart):
    count = lax.axis_size(axis)
    route = []
    for low in range(count):
        high = low | 1 << apart
        if high != low and high < count:
            route += [(low, high), (high, low)]
    return lax.ppermute(block, axis, route)


def shifted(shard, axis, by):
    size = lax.axis_size(axis)
    return lax.ppermute(shard, axis, [(i, (i + by) % size) for i in range(size)])


def silu_grad(values):
    sigma = jax.nn.sigmoid(values)
    return sigma * (1.0 + values * (1.0 - sigma))


def slot_table(routes, experts, capacity):
    flat_routes = routes.reshape(-1)
    entries = flat_routes.shape[0]
    onehot = (flat_routes[:, None] == jnp.arange(experts, dtype=jnp.int32)[None, :]).astype(
        jnp.int32
    )
    before = jnp.cumsum(onehot, 0) - onehot
    position = jnp.sum(before * onehot, 1)
    slot_of = flat_routes * capacity + position
    source = (
        jnp.full((experts * capacity,), entries, jnp.int32)
        .at[slot_of]
        .set(jnp.arange(entries, dtype=jnp.int32))
    )
    return (slot_of, source)


def serve_rows(received, up_half, down_half):
    sources = received.shape[0]
    slots = received.shape[2]
    model_width = received.shape[3]
    row_count = sources * slots
    rows_fwd = received[:, 0].reshape(row_count, model_width)
    rows_saved = received[:, 1].reshape(row_count, model_width)
    rows_grad = received[:, 2].reshape(row_count, model_width)
    against_rows = (((1,), (1,)), ((), ()))
    hidden = jax.nn.silu(jnp.dot(rows_fwd, up_half, preferred_element_type=jnp.float32)).astype(
        jnp.bfloat16
    )
    part_fwd = jnp.dot(hidden, down_half, preferred_element_type=jnp.float32).astype(jnp.bfloat16)
    pre_act = jnp.dot(rows_saved, up_half, preferred_element_type=jnp.float32)
    hidden_grad = lax.dot_general(
        rows_grad, down_half, against_rows, preferred_element_type=jnp.float32
    )
    pre_grad = (hidden_grad * silu_grad(pre_act)).astype(jnp.bfloat16)
    part_bwd = lax.dot_general(
        pre_grad, up_half, against_rows, preferred_element_type=jnp.float32
    ).astype(jnp.bfloat16)
    return jnp.stack(
        [
            part_fwd.reshape(sources, slots, model_width),
            part_bwd.reshape(sources, slots, model_width),
        ],
        1,
    )


def combine(inputs, routed_rows, affinity):
    tokens = inputs.shape[0]
    top_count = affinity.shape[1]
    weights = affinity / jnp.sum(affinity, -1, keepdims=True)
    routed = routed_rows.reshape(tokens, top_count, inputs.shape[1]).astype(jnp.float32)
    return (inputs.astype(jnp.float32) + jnp.sum(weights[..., None] * routed, 1)).astype(
        jnp.bfloat16
    )


def general_path(
    x_fwd,
    routes_fwd,
    affinity_fwd,
    x_bwd,
    grad_bwd,
    routes_bwd,
    affinity_bwd,
    up_weight,
    down_weight,
):
    devices = lax.axis_size("expert")
    experts = devices // 2
    tokens = x_fwd.shape[1]
    model_width = x_fwd.shape[2]
    top_count = routes_fwd.shape[2]
    capacity = 3 * tokens * top_count // devices
    half_slots = capacity // 2
    up_half = up_weight[0]
    down_half = down_weight[0]
    slot_fwd, source_fwd = slot_table(routes_fwd[0], experts, capacity)
    slot_bwd, source_bwd = slot_table(routes_bwd[0], experts, capacity)
    zero_row = jnp.zeros((1, model_width), jnp.bfloat16)
    row_table = jnp.concatenate([x_fwd[0], zero_row, x_bwd[0], zero_row, grad_bwd[0], zero_row], 0)
    stride = tokens + 1
    token_fwd = (source_fwd // top_count).reshape(experts, capacity)
    token_bwd = (source_bwd // top_count).reshape(experts, capacity)
    gather_index = jnp.stack([token_fwd, token_bwd + stride, token_bwd + 2 * stride], 1)
    send_index = (
        gather_index.reshape(experts, 3, 2, half_slots)
        .transpose(0, 2, 1, 3)
        .reshape(devices, 3, half_slots)
    )
    outgoing = row_table[send_index]
    received = lax.all_to_all(outgoing, "expert", split_axis=0, concat_axis=0, tiled=True)
    partner = from_partner_2(received, "expert", 0)
    result = serve_rows(jnp.concatenate([received, partner], 2), up_half, down_half)
    piece_slots = received.shape[2]
    from_partner = from_partner_2(result[:, :, piece_slots:], "expert", 0)
    summed = (
        result[:, :, :piece_slots].astype(jnp.float32) + from_partner.astype(jnp.float32)
    ).astype(jnp.bfloat16)
    returned = lax.all_to_all(summed, "expert", split_axis=0, concat_axis=0, tiled=True)
    flat_back = returned.reshape(-1, model_width)

    def back_index(slot_of, member):
        expert_id = slot_of // capacity
        within = slot_of % capacity
        return (
            (2 * expert_id + within // half_slots) * 2 + member
        ) * half_slots + within % half_slots

    index_fwd = back_index(slot_fwd, 0)
    index_bwd = back_index(slot_bwd, 1)
    layer_out = combine(x_fwd[0], flat_back[index_fwd], affinity_fwd[0])
    input_grad = combine(grad_bwd[0], flat_back[index_bwd], affinity_bwd[0])
    fwd_next = shifted(layer_out[None], "section", 1)
    bwd_next = shifted(input_grad[None], "section", -1)
    return (fwd_next, bwd_next)


def line_kernel(
    sizes,
    routes_fwd,
    affinity_fwd,
    routes_bwd,
    affinity_bwd,
    x_fwd,
    x_bwd,
    grad_bwd,
    up,
    down,
    out_fwd,
    out_bwd,
    routes,
    affinities,
    blocks,
    ups,
    downs,
    tables,
    total,
    slope,
    hidden_grad,
    hidden,
    pre_grad,
    returned,
    final,
    picked,
    expand,
    piece,
    local_sem,
    table_send,
    table_recv,
    own_send,
    across_send,
    outer_send,
    block_recv,
    up_send,
    up_recv,
    down_send,
    down_recv,
    back_send,
    back_recv,
    shift_send,
    shift_recv,
):
    sections, experts, tokens, capacity, pieces, cut, wide = sizes
    spans = pieces * cut // wide
    half_rows = tokens // 2
    streams = (x_fwd, x_bwd, grad_bwd)
    section = lax.axis_index("section")
    device = lax.axis_index("expert")
    place, side = device // 2, device % 2
    last = experts - 1
    is_inner = (place > 0) & (place < last)
    is_end = (place == 0) | (place == last)
    across = jnp.where(place < experts // 2, 1, -1)

    def at_place(where):
        return {"expert": where * 2 + side}

    def remote(src, dst, send, recv, target):
        return pltpu.make_async_remote_copy(
            src_ref=src,
            dst_ref=dst,
            send_sem=send,
            recv_sem=recv,
            device_id=target,
            device_id_type=pl.DeviceIdType.MESH,
        )

    partner = {"expert": place * 2 + 1 - side}
    next_section = {"section": lax.rem(section + 1, sections)}
    previous_section = {"section": lax.rem(section + sections - 1, sections)}
    column = [at_place(lax.rem(place + ahead, experts)) for ahead in range(1, experts)]

    barrier = pltpu.get_barrier_semaphore()
    peers = column + [partner, next_section, previous_section]
    for peer in peers:
        pl.semaphore_signal(
            barrier, inc=1, device_id=peer, device_id_type=pl.DeviceIdType.MESH
        )

    small = [
        pltpu.make_async_copy(source, target, local_sem.at[5 + index])
        for index, (source, target) in enumerate(
            (
                (routes_fwd, routes.at[0]),
                (affinity_fwd, affinities.at[0]),
                (routes_bwd, routes.at[1]),
                (affinity_bwd, affinities.at[1]),
            )
        )
    ]
    for copy in small:
        copy.start()
    row_id = lax.broadcasted_iota(jnp.int32, (tokens, tokens), 0)
    lane_id = lax.broadcasted_iota(jnp.int32, (tokens, tokens), 1)
    later = jnp.where(row_id < lane_id, 1.0, 0.0).astype(jnp.bfloat16)
    expert_id = row_id[:16]
    for copy in small:
        copy.wait()
    for member in range(2):
        weights = affinities[member] / jnp.sum(affinities[member], 0, keepdims=True)
        share = jnp.zeros(expert_id.shape, jnp.float32)
        named = jnp.zeros(expert_id.shape, jnp.float32)
        for choice in range(routes.shape[1]):
            same = routes[member, choice : choice + 1, :] == expert_id
            share += jnp.where(same, weights[choice : choice + 1, :], 0.0)
            named += jnp.where(same, 1.0, 0.0)
        rank = jnp.dot(named.astype(jnp.bfloat16), later, preferred_element_type=jnp.float32)
        rank = jnp.where(named > 0.5, rank, -1.0)
        base = member * 2 * experts
        tables[place, base : base + experts, :] = share[:experts]
        tables[place, base + experts : base + 2 * experts, :] = rank[:experts]

    pl.semaphore_wait(barrier, len(peers))
    table_copies = [
        remote(
            tables.at[place],
            tables.at[place],
            table_send.at[ahead],
            table_recv.at[place],
            column[ahead],
        )
        for ahead in range(experts - 1)
    ]
    for copy in table_copies:
        copy.start()

    def rows_of(origin):
        return pl.ds(pl.multiple_of(origin * tokens, tokens), tokens)

    def half_of(origin, half):
        return pl.ds(pl.multiple_of(origin * tokens + half * half_rows, half_rows), half_rows)

    def columns_of(index):
        return pl.ds(pl.multiple_of(index * cut, cut), cut)

    def span_of(index):
        return pl.ds(pl.multiple_of(index * wide, wide), wide)

    def own_copy(stream, half):
        return remote(
            streams[stream].at[pl.ds(half * half_rows, half_rows)],
            blocks.at[stream, half_of(place, half)],
            own_send.at[stream, half],
            block_recv.at[stream, place, half],
            at_place(place + across),
        )

    def send_own(stream):
        for half in range(2):
            own_copy(stream, half).start()

    def wait_half(stream, origin, half):
        block = blocks.at[stream, half_of(origin, half)]
        remote(
            block, block, own_send.at[stream, half], block_recv.at[stream, origin, half], partner
        ).wait_recv()

    def across_copy(stream, half):
        origin = place - across
        block = blocks.at[stream, half_of(origin, half)]
        return remote(
            block,
            block,
            across_send.at[stream, half],
            block_recv.at[stream, origin, half],
            at_place(place + across),
        )

    def send_across(stream, half):
        @pl.when(is_inner)
        def _():
            wait_half(stream, place - across, half)
            across_copy(stream, half).start()

    def outer_copy(stream, steps):
        origin = place + across * steps
        return remote(
            picked.at[stream, steps],
            blocks.at[stream, pl.ds(pl.multiple_of(origin * tokens, tokens), capacity)],
            outer_send.at[stream, steps],
            block_recv.at[stream, origin, 0],
            at_place(place - across),
        )

    def table_row(member, kind, origin, expert):
        return tables[origin, pl.ds((member * 2 + kind) * experts + expert, 1), :]

    def send_outer(stream, steps):
        @pl.when(is_inner)
        def _():
            origin = place + across * steps
            if steps:
                for half in range(2):
                    wait_half(stream, origin, half)
            ranks = table_row(min(stream, 1), 1, origin, place - across)
            slots = lax.broadcasted_iota(jnp.int32, (capacity, tokens), 0).astype(jnp.float32)
            pick = jnp.where(slots == ranks, 1.0, 0.0).astype(jnp.bfloat16)

            @pl.loop(0, spans)
            def _(index):
                picked[stream, steps, :, span_of(index)] = jnp.dot(
                    pick,
                    blocks[stream, rows_of(origin), span_of(index)],
                    preferred_element_type=jnp.float32,
                ).astype(jnp.bfloat16)

            outer_copy(stream, steps).start()

    def wait_at_end(stream):
        @pl.when(is_end)
        def _():
            for steps in range(1, experts):
                origin = place + across * steps
                landed = blocks.at[
                    stream, pl.ds(pl.multiple_of(origin * tokens, tokens), capacity)
                ]
                remote(
                    landed,
                    landed,
                    own_send.at[stream, 0],
                    block_recv.at[stream, origin, 0],
                    partner,
                ).wait_recv()

    def up_copy(index):
        rows = span_of(index)
        return remote(
            up.at[rows], ups.at[1, rows], up_send.at[0], up_recv.at[0], partner
        )

    def down_copy(index):
        rows = columns_of(index)
        return remote(
            down.at[:, rows],
            downs.at[1, :, rows],
            down_send.at[0],
            down_recv.at[index],
            partner,
        )

    whole_up = remote(up, ups.at[1], up_send.at[0], up_recv.at[0], partner)
    whole_down = remote(down, downs.at[1], down_send.at[0], down_recv.at[0], partner)
    send_own(0)

    @pl.loop(0, spans)
    def _(index):
        up_copy(index).start()

    @pl.loop(0, pieces)
    def _(index):
        down_copy(index).start()

    local = [
        pltpu.make_async_copy(
            streams[stream], blocks.at[stream, rows_of(place)], local_sem.at[stream]
        )
        for stream in range(3)
    ]
    local.append(pltpu.make_async_copy(up, ups.at[0], local_sem.at[3]))
    local.append(pltpu.make_async_copy(down, downs.at[0], local_sem.at[4]))
    for copy in local[:3]:
        copy.start()

    @pl.when(is_end)
    def _():
        for stream in range(3):
            for steps in range(1, experts):
                start = pl.multiple_of((place + across * steps) * tokens + capacity, 16)
                blocks[stream, pl.ds(start, tokens - capacity), :] = jnp.zeros(
                    (tokens - capacity, blocks.shape[2]), jnp.bfloat16
                )

    def wait_tables():
        for ahead in range(1, experts):
            origin = lax.rem(place + ahead, experts)
            remote(
                tables.at[origin],
                tables.at[origin],
                table_send.at[0],
                table_recv.at[origin],
                partner,
            ).wait_recv()

    def make_expand():
        @pl.when(is_inner)
        def _():
            @pl.loop(0, 2 * experts)
            def _(index):
                member = index // experts
                origin = index - member * experts
                ranks = table_row(member, 1, origin, place - across)
                rank = jnp.sum(jnp.where(row_id == lane_id, ranks, 0.0), 1, keepdims=True)
                expand[member, origin] = jnp.where(
                    lane_id.astype(jnp.float32) == rank, 1.0, 0.0
                ).astype(jnp.bfloat16)

    def weight_of(member, origin):
        packed = is_end & (origin != place)
        slots = row_id.astype(jnp.float32)
        lanes = lane_id[:1].astype(jnp.float32)
        ranks = jnp.where(packed, table_row(member, 1, origin, place), lanes)
        share = table_row(member, 0, origin, place)
        return jnp.sum(jnp.where(slots == ranks, share, 0.0), 1, keepdims=True)

    def project(stream, half):
        total[...] = jnp.zeros(total.shape, jnp.float32)

        @pl.loop(0, spans)
        def _(index):
            total[...] += jnp.dot(
                blocks[stream, :, span_of(index)],
                ups[half, span_of(index), :],
                preferred_element_type=jnp.float32,
            )

    def make_hidden():
        @pl.loop(0, 2)
        def _(half):
            project(0, half)

            @pl.loop(0, experts)
            def _(origin):
                act = total[rows_of(origin), :]
                hidden[half, rows_of(origin), :] = (
                    act / (1.0 + jnp.exp(-act)) * weight_of(0, origin)
                ).astype(jnp.bfloat16)

    def make_slope():
        @pl.loop(0, 2)
        def _(half):
            project(1, half)

            @pl.loop(0, experts)
            def _(origin):
                weight = weight_of(1, origin)
                act = total[rows_of(origin), :]
                sigma = 1.0 / (1.0 + jnp.exp(-act))
                slope[half, rows_of(origin), :] = (
                    sigma * (1.0 + act * (1.0 - sigma))
                ) * weight

    def add_hidden_grad(half, index):
        hidden_grad[half] += lax.dot_general(
            blocks[2, :, span_of(index)],
            downs[half, :, span_of(index)],
            AGAINST_ROWS,
            preferred_element_type=jnp.float32,
        )

    def start_hidden_grad():
        hidden_grad[...] = jnp.zeros(hidden_grad.shape, jnp.float32)

        @pl.loop(0, 2 * spans - 1)
        def _(index):
            half = index // spans
            add_hidden_grad(half, index - half * spans)

    def make_pre_grad():
        add_hidden_grad(1, spans - 1)

        @pl.loop(0, 2 * experts)
        def _(index):
            half = index // experts
            origin = index - half * experts
            rows = rows_of(origin)
            pre_grad[half, rows, :] = (
                hidden_grad[half, rows, :] * slope[half, rows, :]
            ).astype(jnp.bfloat16)

    def back_copy(member, target, index, count):
        way = jnp.where(target > place, 1, -1)
        there = place + way
        slot = jnp.where((way < 0) & (target == there), experts, target)
        return remote(
            returned.at[member, target, index, pl.ds(0, count)],
            returned.at[member, slot, index, pl.ds(0, count)],
            back_send.at[member, target],
            back_recv.at[member, slot, index],
            at_place(there),
        )

    def add_back(member, slot, index):
        landed = returned.at[member, slot, index]
        remote(
            landed,
            landed,
            back_send.at[member, 0],
            back_recv.at[member, slot, index],
            partner,
        ).wait_recv()
        piece[...] += returned[member, slot, index].astype(jnp.float32)

    def add_packed_back(member, slot, index, origin):
        landed = returned.at[member, slot, index, pl.ds(0, capacity)]
        remote(
            landed,
            landed,
            back_send.at[member, 0],
            back_recv.at[member, slot, index],
            partner,
        ).wait_recv()
        piece[...] += jnp.dot(
            expand[member, origin, :, :capacity],
            returned[member, slot, index, :capacity],
            preferred_element_type=jnp.float32,
        )

    def shift_copy(member, index):
        return remote(
            final.at[member, index],
            (out_fwd, out_bwd)[member].at[:, columns_of(index)],
            shift_send.at[member],
            shift_recv.at[member],
            (next_section, previous_section)[member],
        )

    def serve(target, member, index):
        rows = rows_of(target)

        @pl.when(member == 0)
        def _():
            piece[...] = jnp.dot(
                hidden[0, rows, :],
                downs[0, :, columns_of(index)],
                preferred_element_type=jnp.float32,
            ) + jnp.dot(
                hidden[1, rows, :],
                downs[1, :, columns_of(index)],
                preferred_element_type=jnp.float32,
            )

        @pl.when(member == 1)
        def _():
            piece[...] = lax.dot_general(
                pre_grad[0, rows, :],
                ups[0, columns_of(index), :],
                AGAINST_ROWS,
                preferred_element_type=jnp.float32,
            ) + lax.dot_general(
                pre_grad[1, rows, :],
                ups[1, columns_of(index), :],
                AGAINST_ROWS,
                preferred_element_type=jnp.float32,
            )

        @pl.when(target != place)
        def _():
            @pl.when(is_end)
            def _():
                returned[member, target, index] = piece[...].astype(jnp.bfloat16)
                back_copy(member, target, index, capacity).start()

            @pl.when(is_inner)
            def _():
                beyond = (target - place) * across > 0

                @pl.when(beyond)
                def _():
                    add_packed_back(member, target, index, target)

                @pl.when(jnp.logical_not(beyond))
                def _():
                    add_back(member, target, index)

                returned[member, target, index] = piece[...].astype(jnp.bfloat16)
                back_copy(member, target, index, tokens).start()

        @pl.when(target == place)
        def _():
            @pl.when(is_inner)
            def _():
                add_packed_back(
                    member, jnp.where(across > 0, place, experts), index, place
                )

            add_back(member, jnp.where(across > 0, experts, place), index)

            for each in range(2):

                @pl.when(member == each)
                def _(each=each):
                    final[each, index] = (
                        piece[...]
                        + blocks[2 * each, rows, columns_of(index)].astype(jnp.float32)
                    ).astype(jnp.bfloat16)
                    shift_copy(each, index).start()

    local[0].wait()
    send_outer(0, 0)
    send_across(0, 0)
    send_across(0, 1)
    send_own(1)
    for copy in local[3:]:
        copy.start()
    wait_tables()
    send_outer(0, 1)
    local[1].wait()
    send_outer(1, 0)
    send_across(1, 0)
    send_outer(0, 2)
    send_across(1, 1)
    send_own(2)
    send_outer(1, 1)
    local[2].wait()
    send_outer(2, 0)
    send_across(2, 0)
    send_across(2, 1)
    make_expand()
    send_outer(1, 2)
    local[3].wait()
    local[4].wait()
    wait_at_end(0)

    whole_up.wait_recv()

    make_hidden()

    reach = jnp.where(is_end, last, last - 1)
    gate = pieces // 2

    def arrived(tick):
        steady = jnp.where(tick < pieces, tick - 2, jnp.maximum(pieces - 3, tick - 6))
        return jnp.clip(jnp.minimum(2 * (tick - gate), steady), 0, pieces)

    def own_arrived(tick):
        early = arrived(jnp.minimum(tick, pieces - 1) - 2)
        at_end = jnp.where(tick < (1 + last) * pieces, early, pieces)
        return jnp.where(is_end, at_end, arrived(tick))

    @pl.loop(0, (2 + last) * pieces)
    def _(tick):
        @pl.when(tick < pieces)
        def _():
            down_copy(tick).wait_recv()

        @pl.when(tick == pieces // 7)
        def _():
            send_outer(2, 1)

        @pl.when(tick == 3 * pieces // 7)
        def _():
            send_outer(2, 2)

        @pl.when(tick == pieces)
        def _():
            make_pre_grad()

        ready = jnp.where(is_end, tick, tick - 1)

        @pl.when((ready >= 0) & (ready < pieces))
        def _():
            @pl.loop(0, reach)
            def _(nearer):
                serve(place + across * (reach - nearer), 0, ready)

        later_step = tick - pieces - jnp.where(is_end, 0, 2)

        @pl.when((later_step >= 0) & (later_step < (reach + 1) * pieces))
        def _():
            nearer = later_step // pieces
            serve(place + across * (reach - nearer), 1, later_step - nearer * pieces)

        @pl.when(is_inner)
        def _():
            @pl.loop(arrived(tick - 1), arrived(tick))
            def _(index):
                serve(place - across, 0, index)

            outer_step = later_step - 3

            @pl.when((outer_step >= 0) & (outer_step < pieces))
            def _():
                serve(place - across, 1, outer_step)

        @pl.loop(own_arrived(tick - 1), own_arrived(tick))
        def _(index):
            serve(place, 0, index)

        @pl.when(tick == 2 * pieces // 7)
        def _():
            wait_at_end(1)
            make_slope()

        @pl.when(tick == pieces - 1 - wide // cut)
        def _():
            wait_at_end(2)
            start_hidden_grad()

    for stream in range(3):
        for half in range(2):
            own_copy(stream, half).wait_send()

    @pl.when(is_inner)
    def _():
        for stream in range(3):
            for half in range(2):
                across_copy(stream, half).wait_send()
            for steps in range(experts - 1):
                outer_copy(stream, steps).wait_send()

    for copy in table_copies:
        copy.wait_send()

    whole_up.wait_send()
    whole_down.wait_send()

    @pl.loop(1, experts)
    def _(ahead):
        target = lax.rem(place + ahead, experts)
        for member in range(2):

            @pl.when(is_end)
            def _(member=member):
                sent = returned.at[member, target, :, pl.ds(0, capacity)]
                remote(
                    sent, sent, back_send.at[member, target], back_recv.at[0, 0, 0], partner
                ).wait_send()

            @pl.when(is_inner)
            def _(member=member):
                sent = returned.at[member, target]
                remote(
                    sent, sent, back_send.at[member, target], back_recv.at[0, 0, 0], partner
                ).wait_send()

    for member, out in enumerate((out_fwd, out_bwd)):
        remote(
            final.at[member],
            final.at[member],
            shift_send.at[member],
            shift_recv.at[member],
            partner,
        ).wait_send()
        remote(
            out, out, shift_send.at[member], shift_recv.at[member], partner
        ).wait_recv()


def store_kernel(fwd, bwd, out_fwd, out_bwd, sems):
    parts = sems.shape[1]
    rows = fwd.shape[0] // parts
    copies = []
    for member, (source, target) in enumerate(((fwd, out_fwd), (bwd, out_bwd))):
        for part in range(parts):
            here = pl.ds(part * rows, rows)
            copies.append(
                pltpu.make_async_copy(
                    source.at[here], target.at[here], sems.at[member, part]
                )
            )
    for copy in copies:
        copy.start()
    for copy in copies:
        copy.wait()


def line_path(
    x_fwd,
    routes_fwd,
    affinity_fwd,
    x_bwd,
    grad_bwd,
    routes_bwd,
    affinity_bwd,
    up_weight,
    down_weight,
):
    devices = lax.axis_size("expert")
    sections = lax.axis_size("section")
    experts = devices // 2
    tokens, width = x_fwd.shape[1:]
    top_count = routes_fwd.shape[2]
    units = up_weight.shape[2]
    capacity = 3 * tokens * top_count // devices
    wide = piece_width(width)
    cut = wide // 2
    pieces = width // cut
    spans = width // wide
    rows = experts * tokens
    bf16, f32 = jnp.bfloat16, jnp.float32
    dma = pltpu.SemaphoreType.DMA
    in_vmem = pl.BlockSpec(memory_space=pltpu.VMEM)
    anywhere = pl.BlockSpec(memory_space=pl.ANY)
    outs = pl.pallas_call(
        functools.partial(line_kernel, (sections, experts, tokens, capacity, pieces, cut, wide)),
        name="expert_line",
        out_shape=[pltpu.VMEM((tokens, width), bf16)] * 2,
        in_specs=[anywhere] * 9,
        out_specs=[in_vmem] * 2,
        scratch_shapes=[
            pltpu.VMEM((2, top_count, tokens), jnp.int32),
            pltpu.VMEM((2, top_count, tokens), f32),
            pltpu.VMEM((3, rows, width), bf16),
            pltpu.VMEM((2, width, units), bf16),
            pltpu.VMEM((2, units, width), bf16),
            pltpu.VMEM((experts, 4 * experts, tokens), f32),
            pltpu.VMEM((rows, units), f32),
            pltpu.VMEM((2, rows, units), f32),
            pltpu.VMEM((2, rows, units), f32),
            pltpu.VMEM((2, rows, units), bf16),
            pltpu.VMEM((2, rows, units), bf16),
            pltpu.VMEM((2, experts + 1, pieces, tokens, cut), bf16),
            pltpu.VMEM((2, pieces, tokens, cut), bf16),
            pltpu.VMEM((3, experts - 1, capacity, width), bf16),
            pltpu.VMEM((2, experts, tokens, tokens), bf16),
            pltpu.VMEM((tokens, cut), f32),
            dma((9,)),
            dma((experts - 1,)),
            dma((experts,)),
            dma((3, 2)),
            dma((3, 2)),
            dma((3, experts - 1)),
            dma((3, experts, 2)),
            dma((1,)),
            dma((1,)),
            dma((1,)),
            dma((pieces,)),
            dma((2, experts)),
            dma((2, experts + 1, pieces)),
            dma((2,)),
            dma((2,)),
        ],
        compiler_params=pltpu.CompilerParams(
            collective_id=0, has_side_effects=True, vmem_limit_bytes=56 << 20
        ),
    )(
        routes_fwd[0].T,
        affinity_fwd[0].T,
        routes_bwd[0].T,
        affinity_bwd[0].T,
        x_fwd[0],
        x_bwd[0],
        grad_bwd[0],
        up_weight[0],
        down_weight[0],
    )
    stored = pl.pallas_call(
        store_kernel,
        name="store_outputs",
        out_shape=[jax.ShapeDtypeStruct((tokens, width), bf16)] * 2,
        in_specs=[in_vmem] * 2,
        out_specs=[anywhere] * 2,
        scratch_shapes=[dma((2, 4))],
    )(*[pltpu.with_memory_space_constraint(out, pltpu.VMEM) for out in outs])
    return tuple(out[None] for out in stored)


def piece_width(width):
    for wide in (512, 256):
        if width % wide == 0:
            return wide
    return 0


def per_device(*args):
    experts = lax.axis_size("expert") // 2
    tokens, width = args[0].shape[1:]
    if experts == 4 and tokens == 128 and piece_width(width):
        return line_path(*args)
    return general_path(*args)


def solution(mesh):
    in_specs = (
        P("section", "expert", None),
        P("section", "expert", None),
        P("section", "expert", None),
        P("section", "expert", None),
        P("section", "expert", None),
        P("section", "expert", None),
        P("section", "expert", None),
        P("section", None, "expert"),
        P("section", "expert", None),
    )
    out_specs = (P("section", "expert", None), P("section", "expert", None))
    return jax.shard_map(
        per_device, mesh=mesh, in_specs=in_specs, out_specs=out_specs, check_vma=False
    )
```

```python
import functools

import jax
import jax.numpy as jnp
from jax import lax
from jax.experimental import pallas as pl
from jax.experimental.pallas import tpu as pltpu
from jax.sharding import PartitionSpec as P

AGAINST_ROWS = (((1,), (1,)), ((), ()))


def from_partner_2(block, axis, apart):
    count = lax.axis_size(axis)
    route = []
    for low in range(count):
        high = low | 1 << apart
        if high != low and high < count:
            route += [(low, high), (high, low)]
    return lax.ppermute(block, axis, route)


def shifted(shard, axis, by):
    size = lax.axis_size(axis)
    return lax.ppermute(shard, axis, [(i, (i + by) % size) for i in range(size)])


def silu_grad(values):
    sigma = jax.nn.sigmoid(values)
    return sigma * (1.0 + values * (1.0 - sigma))


def slot_table(routes, experts, capacity):
    flat_routes = routes.reshape(-1)
    entries = flat_routes.shape[0]
    onehot = (flat_routes[:, None] == jnp.arange(experts, dtype=jnp.int32)[None, :]).astype(
        jnp.int32
    )
    before = jnp.cumsum(onehot, 0) - onehot
    position = jnp.sum(before * onehot, 1)
    slot_of = flat_routes * capacity + position
    source = (
        jnp.full((experts * capacity,), entries, jnp.int32)
        .at[slot_of]
        .set(jnp.arange(entries, dtype=jnp.int32))
    )
    return (slot_of, source)


def serve_rows(received, up_half, down_half):
    sources = received.shape[0]
    slots = received.shape[2]
    model_width = received.shape[3]
    row_count = sources * slots
    rows_fwd = received[:, 0].reshape(row_count, model_width)
    rows_saved = received[:, 1].reshape(row_count, model_width)
    rows_grad = received[:, 2].reshape(row_count, model_width)
    against_rows = (((1,), (1,)), ((), ()))
    hidden = jax.nn.silu(jnp.dot(rows_fwd, up_half, preferred_element_type=jnp.float32)).astype(
        jnp.bfloat16
    )
    part_fwd = jnp.dot(hidden, down_half, preferred_element_type=jnp.float32).astype(jnp.bfloat16)
    pre_act = jnp.dot(rows_saved, up_half, preferred_element_type=jnp.float32)
    hidden_grad = lax.dot_general(
        rows_grad, down_half, against_rows, preferred_element_type=jnp.float32
    )
    pre_grad = (hidden_grad * silu_grad(pre_act)).astype(jnp.bfloat16)
    part_bwd = lax.dot_general(
        pre_grad, up_half, against_rows, preferred_element_type=jnp.float32
    ).astype(jnp.bfloat16)
    return jnp.stack(
        [
            part_fwd.reshape(sources, slots, model_width),
            part_bwd.reshape(sources, slots, model_width),
        ],
        1,
    )


def combine(inputs, routed_rows, affinity):
    tokens = inputs.shape[0]
    top_count = affinity.shape[1]
    weights = affinity / jnp.sum(affinity, -1, keepdims=True)
    routed = routed_rows.reshape(tokens, top_count, inputs.shape[1]).astype(jnp.float32)
    return (inputs.astype(jnp.float32) + jnp.sum(weights[..., None] * routed, 1)).astype(
        jnp.bfloat16
    )


def general_path(
    x_fwd,
    routes_fwd,
    affinity_fwd,
    x_bwd,
    grad_bwd,
    routes_bwd,
    affinity_bwd,
    up_weight,
    down_weight,
):
    devices = lax.axis_size("expert")
    experts = devices // 2
    tokens = x_fwd.shape[1]
    model_width = x_fwd.shape[2]
    top_count = routes_fwd.shape[2]
    capacity = 3 * tokens * top_count // devices
    half_slots = capacity // 2
    up_half = up_weight[0]
    down_half = down_weight[0]
    slot_fwd, source_fwd = slot_table(routes_fwd[0], experts, capacity)
    slot_bwd, source_bwd = slot_table(routes_bwd[0], experts, capacity)
    zero_row = jnp.zeros((1, model_width), jnp.bfloat16)
    row_table = jnp.concatenate([x_fwd[0], zero_row, x_bwd[0], zero_row, grad_bwd[0], zero_row], 0)
    stride = tokens + 1
    token_fwd = (source_fwd // top_count).reshape(experts, capacity)
    token_bwd = (source_bwd // top_count).reshape(experts, capacity)
    gather_index = jnp.stack([token_fwd, token_bwd + stride, token_bwd + 2 * stride], 1)
    send_index = (
        gather_index.reshape(experts, 3, 2, half_slots)
        .transpose(0, 2, 1, 3)
        .reshape(devices, 3, half_slots)
    )
    outgoing = row_table[send_index]
    received = lax.all_to_all(outgoing, "expert", split_axis=0, concat_axis=0, tiled=True)
    partner = from_partner_2(received, "expert", 0)
    result = serve_rows(jnp.concatenate([received, partner], 2), up_half, down_half)
    piece_slots = received.shape[2]
    from_partner = from_partner_2(result[:, :, piece_slots:], "expert", 0)
    summed = (
        result[:, :, :piece_slots].astype(jnp.float32) + from_partner.astype(jnp.float32)
    ).astype(jnp.bfloat16)
    returned = lax.all_to_all(summed, "expert", split_axis=0, concat_axis=0, tiled=True)
    flat_back = returned.reshape(-1, model_width)

    def back_index(slot_of, member):
        expert_id = slot_of // capacity
        within = slot_of % capacity
        return (
            (2 * expert_id + within // half_slots) * 2 + member
        ) * half_slots + within % half_slots

    index_fwd = back_index(slot_fwd, 0)
    index_bwd = back_index(slot_bwd, 1)
    layer_out = combine(x_fwd[0], flat_back[index_fwd], affinity_fwd[0])
    input_grad = combine(grad_bwd[0], flat_back[index_bwd], affinity_bwd[0])
    fwd_next = shifted(layer_out[None], "section", 1)
    bwd_next = shifted(input_grad[None], "section", -1)
    return (fwd_next, bwd_next)


def line_kernel(
    sizes,
    routes_fwd,
    affinity_fwd,
    routes_bwd,
    affinity_bwd,
    x_fwd,
    x_bwd,
    grad_bwd,
    up,
    down,
    out_fwd,
    out_bwd,
    routes,
    affinities,
    blocks,
    ups,
    downs,
    tables,
    total,
    slope,
    hidden_grad,
    hidden,
    pre_grad,
    returned,
    final,
    picked,
    expand,
    piece,
    local_sem,
    small_sem,
    table_send,
    table_recv,
    own_send,
    across_send,
    outer_send,
    block_recv,
    up_send,
    up_recv,
    down_send,
    down_recv,
    back_send,
    back_recv,
    shift_send,
    shift_recv,
):
    sections, experts, tokens, capacity, pieces, cut, wide = sizes
    spans = pieces * cut // wide
    half_rows = tokens // 2
    section = lax.axis_index("section")
    device = lax.axis_index("expert")
    place, side = device // 2, device % 2
    last = experts - 1
    is_inner = (place > 0) & (place < last)
    is_end = (place == 0) | (place == last)
    across = jnp.where(place < experts // 2, 1, -1)

    def at_place(where):
        return {"expert": where * 2 + side}

    def remote(src, dst, send, recv, target):
        return pltpu.make_async_remote_copy(
            src_ref=src,
            dst_ref=dst,
            send_sem=send,
            recv_sem=recv,
            device_id=target,
            device_id_type=pl.DeviceIdType.MESH,
        )

    partner = {"expert": place * 2 + 1 - side}
    next_section = {"section": lax.rem(section + 1, sections)}
    previous_section = {"section": lax.rem(section + sections - 1, sections)}
    column = [at_place(lax.rem(place + ahead, experts)) for ahead in range(1, experts)]

    barrier = pltpu.get_barrier_semaphore()
    peers = column + [partner, next_section, previous_section]
    for peer in peers:
        pl.semaphore_signal(
            barrier, inc=1, device_id=peer, device_id_type=pl.DeviceIdType.MESH
        )

    def rows_of(origin):
        return pl.ds(pl.multiple_of(origin * tokens, tokens), tokens)

    def half_of(origin, half):
        return pl.ds(pl.multiple_of(origin * tokens + half * half_rows, half_rows), half_rows)

    def columns_of(index):
        return pl.ds(pl.multiple_of(index * cut, cut), cut)

    def span_of(index):
        return pl.ds(pl.multiple_of(index * wide, wide), wide)

    small = [
        pltpu.make_async_copy(source, target, small_sem.at[index])
        for index, (source, target) in enumerate(
            (
                (routes_fwd, routes.at[0]),
                (affinity_fwd, affinities.at[0]),
                (routes_bwd, routes.at[1]),
                (affinity_bwd, affinities.at[1]),
            )
        )
    ]
    for copy in small:
        copy.start()
    first_rows, other_rows = pl.ds(0, wide), pl.ds(wide, up.shape[0] - wide)
    local = [
        pltpu.make_async_copy(source, target, local_sem.at[index])
        for index, (source, target) in enumerate(
            (
                (x_fwd, blocks.at[0, rows_of(place)]),
                (up.at[first_rows], ups.at[0, first_rows]),
                (x_bwd, blocks.at[1, rows_of(place)]),
                (grad_bwd, blocks.at[2, rows_of(place)]),
                (up.at[other_rows], ups.at[0, other_rows]),
                (down, downs.at[0]),
            )
        )
    ]
    local[0].start()
    local[1].start()
    row_id = lax.broadcasted_iota(jnp.int32, (tokens, tokens), 0)
    lane_id = lax.broadcasted_iota(jnp.int32, (tokens, tokens), 1)
    later = jnp.where(row_id < lane_id, 1.0, 0.0).astype(jnp.bfloat16)
    expert_id = row_id[:16]
    for copy in small:
        copy.wait()
    for member in range(2):
        weights = affinities[member] / jnp.sum(affinities[member], 0, keepdims=True)
        share = jnp.zeros(expert_id.shape, jnp.float32)
        named = jnp.zeros(expert_id.shape, jnp.float32)
        for choice in range(routes.shape[1]):
            same = routes[member, choice : choice + 1, :] == expert_id
            share += jnp.where(same, weights[choice : choice + 1, :], 0.0)
            named += jnp.where(same, 1.0, 0.0)
        rank = jnp.dot(named.astype(jnp.bfloat16), later, preferred_element_type=jnp.float32)
        rank = jnp.where(named > 0.5, rank, -1.0)
        base = member * 2 * experts
        tables[place, base : base + experts, :] = share[:experts]
        tables[place, base + experts : base + 2 * experts, :] = rank[:experts]

    pl.semaphore_wait(barrier, len(peers))
    table_copies = [
        remote(
            tables.at[place],
            tables.at[place],
            table_send.at[ahead],
            table_recv.at[place],
            column[ahead],
        )
        for ahead in range(experts - 1)
    ]
    for copy in table_copies:
        copy.start()

    def own_copy(stream, half):
        return remote(
            blocks.at[stream, half_of(place, half)],
            blocks.at[stream, half_of(place, half)],
            own_send.at[0],
            block_recv.at[stream, place, half],
            at_place(place + across),
        )

    def send_own(stream):
        for half in range(2):
            own_copy(stream, half).start()

    def wait_half(stream, origin, half):
        block = blocks.at[stream, half_of(origin, half)]
        remote(
            block, block, own_send.at[0], block_recv.at[stream, origin, half], partner
        ).wait_recv()

    def across_copy(stream, half):
        origin = place - across
        block = blocks.at[stream, half_of(origin, half)]
        return remote(
            block,
            block,
            across_send.at[0],
            block_recv.at[stream, origin, half],
            at_place(place + across),
        )

    def send_across(stream, half):
        @pl.when(is_inner)
        def _():
            wait_half(stream, place - across, half)
            across_copy(stream, half).start()

    def outer_copy(stream, steps):
        origin = place + across * steps
        return remote(
            picked.at[stream, steps],
            blocks.at[stream, pl.ds(pl.multiple_of(origin * tokens, tokens), capacity)],
            outer_send.at[0],
            block_recv.at[stream, origin, 0],
            at_place(place - across),
        )

    def table_row(member, kind, origin, expert):
        return tables[origin, pl.ds((member * 2 + kind) * experts + expert, 1), :]

    def send_outer(stream, steps):
        @pl.when(is_inner)
        def _():
            origin = place + across * steps
            if steps:
                for half in range(2):
                    wait_half(stream, origin, half)
            ranks = table_row(min(stream, 1), 1, origin, place - across)
            slots = lax.broadcasted_iota(jnp.int32, (capacity, tokens), 0).astype(jnp.float32)
            pick = jnp.where(slots == ranks, 1.0, 0.0).astype(jnp.bfloat16)

            @pl.loop(0, spans)
            def _(index):
                picked[stream, steps, :, span_of(index)] = jnp.dot(
                    pick,
                    blocks[stream, rows_of(origin), span_of(index)],
                    preferred_element_type=jnp.float32,
                ).astype(jnp.bfloat16)

            outer_copy(stream, steps).start()

    def wait_at_end(stream):
        @pl.when(is_end)
        def _():
            for steps in range(1, experts):
                origin = place + across * steps
                landed = blocks.at[
                    stream, pl.ds(pl.multiple_of(origin * tokens, tokens), capacity)
                ]
                remote(
                    landed,
                    landed,
                    own_send.at[0],
                    block_recv.at[stream, origin, 0],
                    partner,
                ).wait_recv()

    def up_copy(index):
        rows = span_of(index)
        return remote(
            up.at[rows], ups.at[1, rows], up_send.at[0], up_recv.at[0], partner
        )

    def split_piece(index, part):
        if part is None:
            return cut, pl.ds(0, cut), columns_of(index), index
        width = cut // 2
        start = pl.multiple_of(part * width, width)
        columns = pl.ds(pl.multiple_of(index * cut + part * width, width), width)
        return width, pl.ds(start, width), columns, index + part

    def down_copy(index, part=None):
        _, _, columns, order = split_piece(index, part)
        return remote(
            down.at[:, columns],
            downs.at[1, :, columns],
            down_send.at[0],
            down_recv.at[order],
            partner,
        )

    first_up = remote(
        ups.at[0, first_rows], ups.at[1, first_rows], up_send.at[0], up_recv.at[0], partner
    )
    whole_up = remote(up, ups.at[1], up_send.at[0], up_recv.at[0], partner)
    whole_down = remote(down, downs.at[1], down_send.at[0], down_recv.at[0], partner)
    local[0].wait()
    send_own(0)
    local[1].wait()
    first_up.start()

    @pl.loop(1, spans)
    def _(index):
        up_copy(index).start()

    @pl.loop(0, pieces - 1)
    def _(index):
        down_copy(index).start()

    for part in range(2):
        down_copy(pieces - 1, part).start()

    local[2].start()
    local[3].start()

    @pl.when(is_end)
    def _():
        for stream in range(3):
            for steps in range(1, experts):
                start = pl.multiple_of((place + across * steps) * tokens + capacity, 16)
                blocks[stream, pl.ds(start, tokens - capacity), :] = jnp.zeros(
                    (tokens - capacity, blocks.shape[2]), jnp.bfloat16
                )

    def wait_tables():
        for ahead in range(1, experts):
            origin = lax.rem(place + ahead, experts)
            remote(
                tables.at[origin],
                tables.at[origin],
                table_send.at[0],
                table_recv.at[origin],
                partner,
            ).wait_recv()

    def make_expand():
        @pl.when(is_inner)
        def _():
            @pl.loop(0, 2 * experts)
            def _(index):
                member = index // experts
                origin = index - member * experts
                ranks = table_row(member, 1, origin, place - across)
                rank = jnp.sum(jnp.where(row_id == lane_id, ranks, 0.0), 1, keepdims=True)
                expand[member, origin] = jnp.where(
                    lane_id.astype(jnp.float32) == rank, 1.0, 0.0
                ).astype(jnp.bfloat16)

    def weight_of(member, origin):
        packed = is_end & (origin != place)
        slots = row_id.astype(jnp.float32)
        lanes = lane_id[:1].astype(jnp.float32)
        ranks = jnp.where(packed, table_row(member, 1, origin, place), lanes)
        share = table_row(member, 0, origin, place)
        return jnp.sum(jnp.where(slots == ranks, share, 0.0), 1, keepdims=True)

    def project(stream, half):
        total[...] = jnp.zeros(total.shape, jnp.float32)

        @pl.loop(0, spans)
        def _(index):
            total[...] += jnp.dot(
                blocks[stream, :, span_of(index)],
                ups[half, span_of(index), :],
                preferred_element_type=jnp.float32,
            )

    def make_hidden():
        @pl.loop(0, 2)
        def _(half):
            project(0, half)

            @pl.loop(0, experts)
            def _(origin):
                act = total[rows_of(origin), :]
                hidden[half, rows_of(origin), :] = (
                    act / (1.0 + jnp.exp(-act)) * weight_of(0, origin)
                ).astype(jnp.bfloat16)

    def make_slope():
        @pl.loop(0, 2)
        def _(half):
            project(1, half)

            @pl.loop(0, experts)
            def _(origin):
                weight = weight_of(1, origin)
                act = total[rows_of(origin), :]
                sigma = 1.0 / (1.0 + jnp.exp(-act))
                slope[half, rows_of(origin), :] = (
                    sigma * (1.0 + act * (1.0 - sigma))
                ) * weight

    def add_hidden_grad(half, index):
        hidden_grad[half] += lax.dot_general(
            blocks[2, :, span_of(index)],
            downs[half, :, span_of(index)],
            AGAINST_ROWS,
            preferred_element_type=jnp.float32,
        )

    def start_hidden_grad():
        hidden_grad[...] = jnp.zeros(hidden_grad.shape, jnp.float32)

        @pl.loop(0, 2 * spans - 2)
        def _(index):
            half = index // spans
            add_hidden_grad(half, index - half * spans)

    def make_pre_grad():
        add_hidden_grad(1, spans - 1)

        @pl.loop(0, 2 * experts)
        def _(index):
            half = index // experts
            origin = index - half * experts
            rows = rows_of(origin)
            pre_grad[half, rows, :] = (
                hidden_grad[half, rows, :] * slope[half, rows, :]
            ).astype(jnp.bfloat16)

    def serve(target, member, index, part=None):
        width, lanes, columns, order = split_piece(index, part)
        rows = rows_of(target)
        sum_ref = piece.at[:, pl.ds(0, width)]

        def back_copy(count):
            way = jnp.where(target > place, 1, -1)
            there = place + way
            slot = jnp.where((way < 0) & (target == there), experts, target)
            return remote(
                returned.at[member, target, index, pl.ds(0, count), lanes],
                returned.at[member, slot, index, pl.ds(0, count), lanes],
                back_send.at[member, target],
                back_recv.at[member, slot, order],
                at_place(there),
            )

        def wait_back(slot, count):
            landed = returned.at[member, slot, index, pl.ds(0, count), lanes]
            remote(
                landed,
                landed,
                back_send.at[member, 0],
                back_recv.at[member, slot, order],
                partner,
            ).wait_recv()
            return returned[member, slot, index, pl.ds(0, count), lanes]

        def add_back(slot):
            sum_ref[...] += wait_back(slot, tokens).astype(jnp.float32)

        def add_packed_back(slot):
            packed = wait_back(slot, capacity)
            sum_ref[...] += jnp.dot(
                expand[member, target, :, :capacity],
                packed,
                preferred_element_type=jnp.float32,
            )

        def forward_product(half):
            return jnp.dot(
                hidden[half, rows, :],
                downs[half, :, columns],
                preferred_element_type=jnp.float32,
            )

        def backward_product(half):
            return lax.dot_general(
                pre_grad[half, rows, :],
                ups[half, columns, :],
                AGAINST_ROWS,
                preferred_element_type=jnp.float32,
            )

        if member == 0:
            sum_ref[...] = forward_product(0) + forward_product(1)
        else:
            sum_ref[...] = backward_product(0) + backward_product(1)

        @pl.when(target != place)
        def _():
            @pl.when(is_end)
            def _():
                returned[member, target, index, :, lanes] = sum_ref[...].astype(jnp.bfloat16)
                back_copy(capacity).start()

            @pl.when(is_inner)
            def _():
                beyond = (target - place) * across > 0

                @pl.when(beyond)
                def _():
                    add_packed_back(target)

                @pl.when(jnp.logical_not(beyond))
                def _():
                    add_back(target)

                returned[member, target, index, :, lanes] = sum_ref[...].astype(jnp.bfloat16)
                back_copy(tokens).start()

        @pl.when(target == place)
        def _():
            @pl.when(is_inner)
            def _():
                add_packed_back(jnp.where(across > 0, place, experts))

            add_back(jnp.where(across > 0, experts, place))
            final[member, index, :, lanes] = (
                sum_ref[...] + blocks[2 * member, rows, columns].astype(jnp.float32)
            ).astype(jnp.bfloat16)
            remote(
                final.at[member, index, :, lanes],
                (out_fwd, out_bwd)[member].at[:, columns],
                shift_send.at[member],
                shift_recv.at[member],
                (next_section, previous_section)[member],
            ).start()

    def serve_last(target):
        @pl.loop(0, 2)
        def _(part):
            serve(target, 0, pieces - 1, part)

    def serve_forward(target, index):
        @pl.when(index < pieces - 1)
        def _():
            serve(target, 0, index)

        @pl.when(index == pieces - 1)
        def _():
            serve_last(target)

    send_outer(0, 0)
    send_across(0, 0)
    send_across(0, 1)
    local[2].wait()
    send_own(1)
    local[4].start()
    local[5].start()
    wait_tables()
    send_outer(0, 1)
    send_outer(1, 0)
    send_across(1, 0)
    send_outer(0, 2)
    send_across(1, 1)
    local[3].wait()
    send_own(2)
    send_outer(1, 1)
    send_outer(2, 0)
    send_across(2, 0)
    send_across(2, 1)
    make_expand()
    send_outer(1, 2)
    local[4].wait()
    local[5].wait()
    wait_at_end(0)
    whole_up.wait_recv()

    make_hidden()

    reach = jnp.where(is_end, last, last - 1)
    gate = pieces // 2

    def arrived(tick):
        steady = jnp.where(tick < pieces, tick - 2, jnp.maximum(pieces - 3, tick - 6))
        return jnp.clip(jnp.minimum(2 * (tick - gate), steady), 0, pieces)

    def own_arrived(tick):
        early = arrived(jnp.minimum(tick, pieces - 1) - 2)
        at_end = jnp.where(tick < (1 + last) * pieces, early, pieces)
        return jnp.where(is_end, at_end, arrived(tick))

    @pl.loop(0, (2 + last) * pieces)
    def _(tick):
        @pl.when(tick < pieces - 1)
        def _():
            down_copy(tick).wait_recv()

        @pl.when(tick == pieces // 7)
        def _():
            send_outer(2, 1)

        @pl.when(tick == 3 * pieces // 7)
        def _():
            send_outer(2, 2)

        @pl.when(tick == pieces)
        def _():
            make_pre_grad()

        ready = jnp.where(is_end, tick, tick - 1)

        @pl.when((ready >= 0) & (ready < pieces - 1))
        def _():
            @pl.loop(0, reach)
            def _(nearer):
                serve(place + across * (reach - nearer), 0, ready)

        @pl.when((tick == pieces - 1) | (tick == pieces))
        def _():
            @pl.loop(0, 2)
            def _(part):
                @pl.when(tick == pieces - 1)
                def _():
                    down_copy(pieces - 1, part).wait_recv()

                @pl.when(ready == pieces - 1)
                def _():
                    @pl.loop(0, reach)
                    def _(nearer):
                        serve(place + across * (reach - nearer), 0, pieces - 1, part)

        later_step = tick - pieces - jnp.where(is_end, 0, 2)

        @pl.when((later_step >= 0) & (later_step < (reach + 1) * pieces))
        def _():
            nearer = later_step // pieces
            serve(place + across * (reach - nearer), 1, later_step - nearer * pieces)

        @pl.when(is_inner)
        def _():
            @pl.loop(arrived(tick - 1), arrived(tick))
            def _(index):
                serve_forward(place - across, index)

            outer_step = later_step - 3

            @pl.when((outer_step >= 0) & (outer_step < pieces))
            def _():
                serve(place - across, 1, outer_step)

        @pl.loop(own_arrived(tick - 1), own_arrived(tick))
        def _(index):
            serve_forward(place, index)

        @pl.when(tick == 2 * pieces // 7)
        def _():
            wait_at_end(1)
            make_slope()

        @pl.when(tick == pieces - 2 - wide // cut)
        def _():
            wait_at_end(2)
            start_hidden_grad()

        @pl.when(tick == pieces - 1 - wide // cut)
        def _():
            add_hidden_grad(1, spans - 2)

    def wait_sent(sent, semaphore):
        remote(sent, sent, semaphore, back_recv.at[0, 0, 0], partner).wait_send()

    wait_sent(blocks.at[:, rows_of(place)], own_send.at[0])

    @pl.when(is_inner)
    def _():
        wait_sent(blocks.at[:, rows_of(place)], across_send.at[0])
        wait_sent(picked, outer_send.at[0])

    for copy in table_copies:
        copy.wait_send()

    whole_up.wait_send()
    whole_down.wait_send()

    @pl.loop(1, experts)
    def _(ahead):
        target = lax.rem(place + ahead, experts)
        for member in range(2):

            @pl.when(is_end)
            def _(member=member):
                sent = returned.at[member, target, :, pl.ds(0, capacity)]
                wait_sent(sent, back_send.at[member, target])

            @pl.when(is_inner)
            def _(member=member):
                wait_sent(returned.at[member, target], back_send.at[member, target])

    for member, out in enumerate((out_fwd, out_bwd)):
        remote(
            final.at[member],
            final.at[member],
            shift_send.at[member],
            shift_recv.at[member],
            partner,
        ).wait_send()
        remote(
            out, out, shift_send.at[member], shift_recv.at[member], partner
        ).wait_recv()


def store_kernel(fwd, bwd, out_fwd, out_bwd, sems):
    parts = sems.shape[1]
    rows = fwd.shape[0] // parts
    copies = []
    for member, (source, target) in enumerate(((fwd, out_fwd), (bwd, out_bwd))):
        for part in range(parts):
            here = pl.ds(part * rows, rows)
            copies.append(
                pltpu.make_async_copy(
                    source.at[here], target.at[here], sems.at[member, part]
                )
            )
    for copy in copies:
        copy.start()
    for copy in copies:
        copy.wait()


def line_path(
    x_fwd,
    routes_fwd,
    affinity_fwd,
    x_bwd,
    grad_bwd,
    routes_bwd,
    affinity_bwd,
    up_weight,
    down_weight,
):
    devices = lax.axis_size("expert")
    sections = lax.axis_size("section")
    experts = devices // 2
    tokens, width = x_fwd.shape[1:]
    top_count = routes_fwd.shape[2]
    units = up_weight.shape[2]
    capacity = 3 * tokens * top_count // devices
    wide = piece_width(width)
    cut = wide // 2
    pieces = width // cut
    spans = width // wide
    rows = experts * tokens
    bf16, f32 = jnp.bfloat16, jnp.float32
    dma = pltpu.SemaphoreType.DMA
    in_vmem = pl.BlockSpec(memory_space=pltpu.VMEM)
    anywhere = pl.BlockSpec(memory_space=pl.ANY)
    outs = pl.pallas_call(
        functools.partial(line_kernel, (sections, experts, tokens, capacity, pieces, cut, wide)),
        name="expert_line",
        out_shape=[pltpu.VMEM((tokens, width), bf16)] * 2,
        in_specs=[anywhere] * 9,
        out_specs=[in_vmem] * 2,
        scratch_shapes=[
            pltpu.VMEM((2, top_count, tokens), jnp.int32),
            pltpu.VMEM((2, top_count, tokens), f32),
            pltpu.VMEM((3, rows, width), bf16),
            pltpu.VMEM((2, width, units), bf16),
            pltpu.VMEM((2, units, width), bf16),
            pltpu.VMEM((experts, 4 * experts, tokens), f32),
            pltpu.VMEM((rows, units), f32),
            pltpu.VMEM((2, rows, units), f32),
            pltpu.VMEM((2, rows, units), f32),
            pltpu.VMEM((2, rows, units), bf16),
            pltpu.VMEM((2, rows, units), bf16),
            pltpu.VMEM((2, experts + 1, pieces, tokens, cut), bf16),
            pltpu.VMEM((2, pieces, tokens, cut), bf16),
            pltpu.VMEM((3, experts - 1, capacity, width), bf16),
            pltpu.VMEM((2, experts, tokens, tokens), bf16),
            pltpu.VMEM((tokens, cut), f32),
            dma((6,)),
            dma((4,)),
            dma((experts - 1,)),
            dma((experts,)),
            dma((1,)),
            dma((1,)),
            dma((1,)),
            dma((3, experts, 2)),
            dma((1,)),
            dma((1,)),
            dma((1,)),
            dma((pieces + 1,)),
            dma((2, experts)),
            dma((2, experts + 1, pieces + 1)),
            dma((2,)),
            dma((2,)),
        ],
        compiler_params=pltpu.CompilerParams(
            collective_id=0, has_side_effects=True, vmem_limit_bytes=56 << 20
        ),
    )(
        routes_fwd[0].T,
        affinity_fwd[0].T,
        routes_bwd[0].T,
        affinity_bwd[0].T,
        x_fwd[0],
        x_bwd[0],
        grad_bwd[0],
        up_weight[0],
        down_weight[0],
    )
    stored = pl.pallas_call(
        store_kernel,
        name="store_outputs",
        out_shape=[jax.ShapeDtypeStruct((tokens, width), bf16)] * 2,
        in_specs=[in_vmem] * 2,
        out_specs=[anywhere] * 2,
        scratch_shapes=[dma((2, 4))],
    )(*[pltpu.with_memory_space_constraint(out, pltpu.VMEM) for out in outs])
    return tuple(out[None] for out in stored)


def piece_width(width):
    for wide in (512, 256):
        if width % wide == 0:
            return wide
    return 0


def per_device(*args):
    experts = lax.axis_size("expert") // 2
    tokens, width = args[0].shape[1:]
    if experts == 4 and tokens == 128 and piece_width(width):
        return line_path(*args)
    return general_path(*args)


def solution(mesh):
    in_specs = (
        P("section", "expert", None),
        P("section", "expert", None),
        P("section", "expert", None),
        P("section", "expert", None),
        P("section", "expert", None),
        P("section", "expert", None),
        P("section", "expert", None),
        P("section", None, "expert"),
        P("section", "expert", None),
    )
    out_specs = (P("section", "expert", None), P("section", "expert", None))
    return jax.shard_map(
        per_device, mesh=mesh, in_specs=in_specs, out_specs=out_specs, check_vma=False
    )
```

```python
import functools

import jax
import jax.numpy as jnp
from jax import lax
from jax.experimental import pallas as pl
from jax.experimental.pallas import tpu as pltpu
from jax.sharding import PartitionSpec as P

AGAINST_ROWS = (((1,), (1,)), ((), ()))


def from_partner_2(block, axis, apart):
    count = lax.axis_size(axis)
    route = []
    for low in range(count):
        high = low | 1 << apart
        if high != low and high < count:
            route += [(low, high), (high, low)]
    return lax.ppermute(block, axis, route)


def shifted(shard, axis, by):
    size = lax.axis_size(axis)
    return lax.ppermute(shard, axis, [(i, (i + by) % size) for i in range(size)])


def silu_grad(values):
    sigma = jax.nn.sigmoid(values)
    return sigma * (1.0 + values * (1.0 - sigma))


def slot_table(routes, experts, capacity):
    flat_routes = routes.reshape(-1)
    entries = flat_routes.shape[0]
    onehot = (flat_routes[:, None] == jnp.arange(experts, dtype=jnp.int32)[None, :]).astype(
        jnp.int32
    )
    before = jnp.cumsum(onehot, 0) - onehot
    position = jnp.sum(before * onehot, 1)
    slot_of = flat_routes * capacity + position
    source = (
        jnp.full((experts * capacity,), entries, jnp.int32)
        .at[slot_of]
        .set(jnp.arange(entries, dtype=jnp.int32))
    )
    return (slot_of, source)


def serve_rows(received, up_half, down_half):
    sources = received.shape[0]
    slots = received.shape[2]
    model_width = received.shape[3]
    row_count = sources * slots
    rows_fwd = received[:, 0].reshape(row_count, model_width)
    rows_saved = received[:, 1].reshape(row_count, model_width)
    rows_grad = received[:, 2].reshape(row_count, model_width)
    against_rows = (((1,), (1,)), ((), ()))
    hidden = jax.nn.silu(jnp.dot(rows_fwd, up_half, preferred_element_type=jnp.float32)).astype(
        jnp.bfloat16
    )
    part_fwd = jnp.dot(hidden, down_half, preferred_element_type=jnp.float32).astype(jnp.bfloat16)
    pre_act = jnp.dot(rows_saved, up_half, preferred_element_type=jnp.float32)
    hidden_grad = lax.dot_general(
        rows_grad, down_half, against_rows, preferred_element_type=jnp.float32
    )
    pre_grad = (hidden_grad * silu_grad(pre_act)).astype(jnp.bfloat16)
    part_bwd = lax.dot_general(
        pre_grad, up_half, against_rows, preferred_element_type=jnp.float32
    ).astype(jnp.bfloat16)
    return jnp.stack(
        [
            part_fwd.reshape(sources, slots, model_width),
            part_bwd.reshape(sources, slots, model_width),
        ],
        1,
    )


def combine(inputs, routed_rows, affinity):
    tokens = inputs.shape[0]
    top_count = affinity.shape[1]
    weights = affinity / jnp.sum(affinity, -1, keepdims=True)
    routed = routed_rows.reshape(tokens, top_count, inputs.shape[1]).astype(jnp.float32)
    return (inputs.astype(jnp.float32) + jnp.sum(weights[..., None] * routed, 1)).astype(
        jnp.bfloat16
    )


def general_path(
    x_fwd,
    routes_fwd,
    affinity_fwd,
    x_bwd,
    grad_bwd,
    routes_bwd,
    affinity_bwd,
    up_weight,
    down_weight,
):
    devices = lax.axis_size("expert")
    experts = devices // 2
    tokens = x_fwd.shape[1]
    model_width = x_fwd.shape[2]
    top_count = routes_fwd.shape[2]
    capacity = 3 * tokens * top_count // devices
    half_slots = capacity // 2
    up_half = up_weight[0]
    down_half = down_weight[0]
    slot_fwd, source_fwd = slot_table(routes_fwd[0], experts, capacity)
    slot_bwd, source_bwd = slot_table(routes_bwd[0], experts, capacity)
    zero_row = jnp.zeros((1, model_width), jnp.bfloat16)
    row_table = jnp.concatenate([x_fwd[0], zero_row, x_bwd[0], zero_row, grad_bwd[0], zero_row], 0)
    stride = tokens + 1
    token_fwd = (source_fwd // top_count).reshape(experts, capacity)
    token_bwd = (source_bwd // top_count).reshape(experts, capacity)
    gather_index = jnp.stack([token_fwd, token_bwd + stride, token_bwd + 2 * stride], 1)
    send_index = (
        gather_index.reshape(experts, 3, 2, half_slots)
        .transpose(0, 2, 1, 3)
        .reshape(devices, 3, half_slots)
    )
    outgoing = row_table[send_index]
    received = lax.all_to_all(outgoing, "expert", split_axis=0, concat_axis=0, tiled=True)
    partner = from_partner_2(received, "expert", 0)
    result = serve_rows(jnp.concatenate([received, partner], 2), up_half, down_half)
    piece_slots = received.shape[2]
    from_partner = from_partner_2(result[:, :, piece_slots:], "expert", 0)
    summed = (
        result[:, :, :piece_slots].astype(jnp.float32) + from_partner.astype(jnp.float32)
    ).astype(jnp.bfloat16)
    returned = lax.all_to_all(summed, "expert", split_axis=0, concat_axis=0, tiled=True)
    flat_back = returned.reshape(-1, model_width)

    def back_index(slot_of, member):
        expert_id = slot_of // capacity
        within = slot_of % capacity
        return (
            (2 * expert_id + within // half_slots) * 2 + member
        ) * half_slots + within % half_slots

    index_fwd = back_index(slot_fwd, 0)
    index_bwd = back_index(slot_bwd, 1)
    layer_out = combine(x_fwd[0], flat_back[index_fwd], affinity_fwd[0])
    input_grad = combine(grad_bwd[0], flat_back[index_bwd], affinity_bwd[0])
    fwd_next = shifted(layer_out[None], "section", 1)
    bwd_next = shifted(input_grad[None], "section", -1)
    return (fwd_next, bwd_next)


def line_kernel(
    sizes,
    routes_fwd,
    affinity_fwd,
    routes_bwd,
    affinity_bwd,
    x_fwd,
    x_bwd,
    grad_bwd,
    up,
    down,
    out_fwd,
    out_bwd,
    routes,
    affinities,
    blocks,
    ups,
    downs,
    tables,
    total,
    slope,
    hidden_grad,
    hidden,
    pre_grad,
    returned,
    final,
    picked,
    expand,
    piece,
    local_sem,
    small_sem,
    table_send,
    table_recv,
    own_send,
    across_send,
    outer_send,
    block_recv,
    up_send,
    up_recv,
    down_send,
    down_recv,
    back_send,
    back_recv,
    forward_recv,
    shift_send,
    shift_recv,
):
    sections, experts, tokens, capacity, pieces, cut, wide = sizes
    spans = pieces * cut // wide
    half_rows = tokens // 2
    section = lax.axis_index("section")
    device = lax.axis_index("expert")
    place, side = device // 2, device % 2
    last = experts - 1
    is_inner = (place > 0) & (place < last)
    is_end = (place == 0) | (place == last)
    across = jnp.where(place < experts // 2, 1, -1)
    reach = jnp.where(is_end, last, last - 1)

    def at_place(where):
        return {"expert": where * 2 + side}

    def remote(src, dst, send, recv, target):
        return pltpu.make_async_remote_copy(
            src_ref=src,
            dst_ref=dst,
            send_sem=send,
            recv_sem=recv,
            device_id=target,
            device_id_type=pl.DeviceIdType.MESH,
        )

    partner = {"expert": place * 2 + 1 - side}
    next_section = {"section": lax.rem(section + 1, sections)}
    previous_section = {"section": lax.rem(section + sections - 1, sections)}
    column = [at_place(lax.rem(place + ahead, experts)) for ahead in range(1, experts)]

    barrier = pltpu.get_barrier_semaphore()
    peers = column + [partner, next_section, previous_section]
    for peer in peers:
        pl.semaphore_signal(
            barrier, inc=1, device_id=peer, device_id_type=pl.DeviceIdType.MESH
        )

    def rows_of(origin):
        return pl.ds(pl.multiple_of(origin * tokens, tokens), tokens)

    def half_of(origin, half):
        return pl.ds(pl.multiple_of(origin * tokens + half * half_rows, half_rows), half_rows)

    def columns_of(index):
        return pl.ds(pl.multiple_of(index * cut, cut), cut)

    def span_of(index):
        return pl.ds(pl.multiple_of(index * wide, wide), wide)

    small = [
        pltpu.make_async_copy(source, target, small_sem.at[index])
        for index, (source, target) in enumerate(
            (
                (routes_fwd, routes.at[0]),
                (affinity_fwd, affinities.at[0]),
                (routes_bwd, routes.at[1]),
                (affinity_bwd, affinities.at[1]),
            )
        )
    ]
    for copy in small:
        copy.start()
    first_rows, other_rows = pl.ds(0, wide), pl.ds(wide, up.shape[0] - wide)
    local = [
        pltpu.make_async_copy(source, target, local_sem.at[index])
        for index, (source, target) in enumerate(
            (
                (x_fwd, blocks.at[0, rows_of(place)]),
                (up.at[first_rows], ups.at[0, first_rows]),
                (x_bwd, blocks.at[1, rows_of(place)]),
                (grad_bwd, blocks.at[2, rows_of(place)]),
                (up.at[other_rows], ups.at[0, other_rows]),
                (down, downs.at[0]),
            )
        )
    ]
    local[0].start()
    local[1].start()
    row_id = lax.broadcasted_iota(jnp.int32, (tokens, tokens), 0)
    lane_id = lax.broadcasted_iota(jnp.int32, (tokens, tokens), 1)
    later = jnp.where(row_id < lane_id, 1.0, 0.0).astype(jnp.bfloat16)
    expert_id = row_id[:16]
    for copy in small:
        copy.wait()
    for member in range(2):
        weights = affinities[member] / jnp.sum(affinities[member], 0, keepdims=True)
        share = jnp.zeros(expert_id.shape, jnp.float32)
        named = jnp.zeros(expert_id.shape, jnp.float32)
        for choice in range(routes.shape[1]):
            same = routes[member, choice : choice + 1, :] == expert_id
            share += jnp.where(same, weights[choice : choice + 1, :], 0.0)
            named += jnp.where(same, 1.0, 0.0)
        rank = jnp.dot(named.astype(jnp.bfloat16), later, preferred_element_type=jnp.float32)
        rank = jnp.where(named > 0.5, rank, -1.0)
        base = member * 2 * experts
        tables[place, base : base + experts, :] = share[:experts]
        tables[place, base + experts : base + 2 * experts, :] = rank[:experts]

    pl.semaphore_wait(barrier, len(peers))
    table_copies = [
        remote(
            tables.at[place],
            tables.at[place],
            table_send.at[ahead],
            table_recv.at[place],
            column[ahead],
        )
        for ahead in range(experts - 1)
    ]
    for copy in table_copies:
        copy.start()

    def own_copy(stream, half):
        return remote(
            blocks.at[stream, half_of(place, half)],
            blocks.at[stream, half_of(place, half)],
            own_send.at[0],
            block_recv.at[stream, place, half],
            at_place(place + across),
        )

    def send_own(stream):
        for half in range(2):
            own_copy(stream, half).start()

    def wait_half(stream, origin, half):
        block = blocks.at[stream, half_of(origin, half)]
        remote(
            block, block, own_send.at[0], block_recv.at[stream, origin, half], partner
        ).wait_recv()

    def across_copy(stream, half):
        origin = place - across
        block = blocks.at[stream, half_of(origin, half)]
        return remote(
            block,
            block,
            across_send.at[0],
            block_recv.at[stream, origin, half],
            at_place(place + across),
        )

    def send_across(stream, half):
        @pl.when(is_inner)
        def _():
            wait_half(stream, place - across, half)
            across_copy(stream, half).start()

    def outer_copy(stream, steps):
        origin = place + across * steps
        return remote(
            picked.at[stream, steps],
            blocks.at[stream, pl.ds(pl.multiple_of(origin * tokens, tokens), capacity)],
            outer_send.at[0],
            block_recv.at[stream, origin, 0],
            at_place(place - across),
        )

    def table_row(member, kind, origin, expert):
        return tables[origin, pl.ds((member * 2 + kind) * experts + expert, 1), :]

    def send_outer(stream, steps):
        @pl.when(is_inner)
        def _():
            origin = place + across * steps
            if steps:
                for half in range(2):
                    wait_half(stream, origin, half)
            ranks = table_row(min(stream, 1), 1, origin, place - across)
            slots = lax.broadcasted_iota(jnp.int32, (capacity, tokens), 0).astype(jnp.float32)
            pick = jnp.where(slots == ranks, 1.0, 0.0).astype(jnp.bfloat16)

            @pl.loop(0, spans)
            def _(index):
                picked[stream, steps, :, span_of(index)] = jnp.dot(
                    pick,
                    blocks[stream, rows_of(origin), span_of(index)],
                    preferred_element_type=jnp.float32,
                ).astype(jnp.bfloat16)

            outer_copy(stream, steps).start()

    def wait_at_end(stream):
        @pl.when(is_end)
        def _():
            for steps in range(1, experts):
                origin = place + across * steps
                landed = blocks.at[
                    stream, pl.ds(pl.multiple_of(origin * tokens, tokens), capacity)
                ]
                remote(
                    landed,
                    landed,
                    own_send.at[0],
                    block_recv.at[stream, origin, 0],
                    partner,
                ).wait_recv()

    def up_copy(index):
        rows = span_of(index)
        return remote(
            up.at[rows], ups.at[1, rows], up_send.at[0], up_recv.at[0], partner
        )

    def split_piece(index, part):
        if part is None:
            return cut, pl.ds(0, cut), columns_of(index), index
        width = cut // 2
        start = pl.multiple_of(part * width, width)
        columns = pl.ds(pl.multiple_of(index * cut + part * width, width), width)
        return width, pl.ds(start, width), columns, index + part

    def down_copy(index, part=None):
        _, _, columns, order = split_piece(index, part)
        return remote(
            down.at[:, columns],
            downs.at[1, :, columns],
            down_send.at[0],
            down_recv.at[order],
            partner,
        )

    first_up = remote(
        ups.at[0, first_rows], ups.at[1, first_rows], up_send.at[0], up_recv.at[0], partner
    )
    whole_up = remote(up, ups.at[1], up_send.at[0], up_recv.at[0], partner)
    whole_down = remote(down, downs.at[1], down_send.at[0], down_recv.at[0], partner)
    local[0].wait()
    send_own(0)
    local[1].wait()
    first_up.start()

    @pl.loop(1, spans)
    def _(index):
        up_copy(index).start()

    @pl.loop(0, pieces - 1)
    def _(index):
        down_copy(index).start()

    for part in range(2):
        down_copy(pieces - 1, part).start()

    local[2].start()
    local[3].start()

    @pl.when(is_end)
    def _():
        for stream in range(3):
            for steps in range(1, experts):
                start = pl.multiple_of((place + across * steps) * tokens + capacity, 16)
                blocks[stream, pl.ds(start, tokens - capacity), :] = jnp.zeros(
                    (tokens - capacity, blocks.shape[2]), jnp.bfloat16
                )

    def wait_tables():
        for ahead in range(1, experts):
            origin = lax.rem(place + ahead, experts)
            remote(
                tables.at[origin],
                tables.at[origin],
                table_send.at[0],
                table_recv.at[origin],
                partner,
            ).wait_recv()

    def make_expand():
        @pl.when(is_inner)
        def _():
            @pl.loop(0, 2 * experts)
            def _(index):
                member = index // experts
                origin = index - member * experts
                ranks = table_row(member, 1, origin, place - across)
                rank = jnp.sum(jnp.where(row_id == lane_id, ranks, 0.0), 1, keepdims=True)
                expand[member, origin] = jnp.where(
                    lane_id.astype(jnp.float32) == rank, 1.0, 0.0
                ).astype(jnp.bfloat16)

    def weight_of(member, origin):
        packed = is_end & (origin != place)
        slots = row_id.astype(jnp.float32)
        lanes = lane_id[:1].astype(jnp.float32)
        ranks = jnp.where(packed, table_row(member, 1, origin, place), lanes)
        share = table_row(member, 0, origin, place)
        return jnp.sum(jnp.where(slots == ranks, share, 0.0), 1, keepdims=True)

    def project(stream, half):
        total[...] = jnp.zeros(total.shape, jnp.float32)

        @pl.loop(0, spans)
        def _(index):
            total[...] += jnp.dot(
                blocks[stream, :, span_of(index)],
                ups[half, span_of(index), :],
                preferred_element_type=jnp.float32,
            )

    def make_hidden():
        @pl.loop(0, 2)
        def _(half):
            project(0, half)

            @pl.loop(0, experts)
            def _(origin):
                act = total[rows_of(origin), :]
                hidden[half, rows_of(origin), :] = (
                    act / (1.0 + jnp.exp(-act)) * weight_of(0, origin)
                ).astype(jnp.bfloat16)

    def make_slope():
        @pl.loop(0, 2)
        def _(half):
            project(1, half)

            @pl.loop(0, experts)
            def _(origin):
                weight = weight_of(1, origin)
                act = total[rows_of(origin), :]
                sigma = 1.0 / (1.0 + jnp.exp(-act))
                slope[half, rows_of(origin), :] = (
                    sigma * (1.0 + act * (1.0 - sigma))
                ) * weight

    def add_hidden_grad(half, index):
        hidden_grad[half] += lax.dot_general(
            blocks[2, :, span_of(index)],
            downs[half, :, span_of(index)],
            AGAINST_ROWS,
            preferred_element_type=jnp.float32,
        )

    def grow_hidden_grad(low, high):
        @pl.loop(low, high)
        def _(index):
            half = index // spans
            add_hidden_grad(half, index - half * spans)

    def make_pre_grad():
        add_hidden_grad(1, spans - 1)

        @pl.loop(0, 2 * experts)
        def _(index):
            half = index // experts
            origin = index - half * experts
            rows = rows_of(origin)
            pre_grad[half, rows, :] = (
                hidden_grad[half, rows, :] * slope[half, rows, :]
            ).astype(jnp.bfloat16)

    def serve(target, member, index, part=None):
        width, lanes, columns, order = split_piece(index, part)
        rows = rows_of(target)
        sum_ref = piece.at[:, pl.ds(0, width)]

        def arrival(slot, group):
            if member == 0:
                return forward_recv.at[group, order]
            return back_recv.at[slot, index]

        def back_copy(count):
            way = jnp.where(target > place, 1, -1)
            there = place + way
            slot = jnp.where((way < 0) & (target == there), experts, target)
            return remote(
                returned.at[member, target, index, pl.ds(0, count), lanes],
                returned.at[member, slot, index, pl.ds(0, count), lanes],
                back_send.at[member, target],
                arrival(slot, jnp.where(is_end, 0, 1)),
                at_place(there),
            )

        def wait_bytes(landed, semaphore):
            remote(landed, landed, back_send.at[member, 0], semaphore, partner).wait_recv()

        def wait_group(group, count, height):
            landed = returned.at[0, pl.ds(0, count), index, pl.ds(0, height), lanes]
            wait_bytes(landed, arrival(None, group))

        def wait_back(slot, height):
            landed = returned.at[member, slot, index, pl.ds(0, height), lanes]
            wait_bytes(landed, arrival(slot, None))

        def add_back(slot):
            if member == 0:

                @pl.when(is_end)
                def _():
                    wait_group(1, 1, tokens)

                @pl.when(is_inner & (target != place))
                def _():
                    wait_group(1, 2, tokens)

            else:
                wait_back(slot, tokens)
            sum_ref[...] += returned[member, slot, index, :, lanes].astype(jnp.float32)

        def add_packed_back(slot):
            if member == 0:

                @pl.when(target == place + across * reach)
                def _():
                    wait_group(0, last, capacity)

            else:
                wait_back(slot, capacity)
            sum_ref[...] += jnp.dot(
                expand[member, target, :, :capacity],
                returned[member, slot, index, pl.ds(0, capacity), lanes],
                preferred_element_type=jnp.float32,
            )

        def forward_product(half):
            return jnp.dot(
                hidden[half, rows, :],
                downs[half, :, columns],
                preferred_element_type=jnp.float32,
            )

        def backward_product(half):
            return lax.dot_general(
                pre_grad[half, rows, :],
                ups[half, columns, :],
                AGAINST_ROWS,
                preferred_element_type=jnp.float32,
            )

        if member == 0:
            sum_ref[...] = forward_product(0) + forward_product(1)
        else:
            sum_ref[...] = backward_product(0) + backward_product(1)

        @pl.when(target != place)
        def _():
            @pl.when(is_end)
            def _():
                returned[member, target, index, :, lanes] = sum_ref[...].astype(jnp.bfloat16)
                back_copy(capacity).start()

            @pl.when(is_inner)
            def _():
                beyond = (target - place) * across > 0

                @pl.when(beyond)
                def _():
                    add_packed_back(target)

                @pl.when(jnp.logical_not(beyond))
                def _():
                    add_back(target)

                returned[member, target, index, :, lanes] = sum_ref[...].astype(jnp.bfloat16)
                back_copy(tokens).start()

        @pl.when(target == place)
        def _():
            @pl.when(is_inner)
            def _():
                add_packed_back(jnp.where(across > 0, place, experts))

            add_back(jnp.where(across > 0, experts, place))
            final[member, index, :, lanes] = (
                sum_ref[...] + blocks[2 * member, rows, columns].astype(jnp.float32)
            ).astype(jnp.bfloat16)
            remote(
                final.at[member, index, :, lanes],
                (out_fwd, out_bwd)[member].at[:, columns],
                shift_send.at[member],
                shift_recv.at[member],
                (next_section, previous_section)[member],
            ).start()

    def serve_last(target):
        @pl.loop(0, 2)
        def _(part):
            serve(target, 0, pieces - 1, part)

    def serve_forward(target, index):
        @pl.when(index < pieces - 1)
        def _():
            serve(target, 0, index)

        @pl.when(index == pieces - 1)
        def _():
            serve_last(target)

    send_outer(0, 0)
    local[2].wait()
    send_outer(1, 0)
    send_across(0, 0)
    send_across(0, 1)
    send_own(1)
    local[4].start()
    local[5].start()
    wait_tables()
    send_outer(0, 1)
    send_across(1, 0)
    send_outer(0, 2)
    send_across(1, 1)
    local[3].wait()
    send_own(2)
    send_outer(2, 0)
    send_outer(1, 1)
    send_across(2, 0)
    send_across(2, 1)
    make_expand()
    send_outer(1, 2)
    local[4].wait()
    local[5].wait()
    wait_at_end(0)
    whole_up.wait_recv()

    make_hidden()

    gate = pieces // 2

    def arrived(tick):
        steady = jnp.where(tick < pieces, tick - 2, jnp.maximum(pieces - 3, tick - 6))
        return jnp.clip(jnp.minimum(2 * (tick - gate), steady), 0, pieces)

    def own_arrived(tick):
        early = arrived(jnp.minimum(tick, pieces - 3) - 2)
        at_end = jnp.where(tick < (1 + last) * pieces, early, pieces)
        return jnp.where(is_end, at_end, arrived(tick))

    @pl.loop(0, (2 + last) * pieces)
    def _(tick):
        @pl.when(tick < pieces - 1)
        def _():
            down_copy(tick).wait_recv()

        @pl.when(tick == pieces // 7)
        def _():
            send_outer(2, 1)

        @pl.when(tick == 3 * pieces // 7)
        def _():
            send_outer(2, 2)

        @pl.when(tick == pieces)
        def _():
            make_pre_grad()

        ready = jnp.where(is_end, tick, tick - 1)

        @pl.when((ready >= 0) & (ready < pieces - 1))
        def _():
            @pl.loop(0, reach)
            def _(nearer):
                serve(place + across * (reach - nearer), 0, ready)

        @pl.when((tick == pieces - 1) | (tick == pieces))
        def _():
            @pl.loop(0, 2)
            def _(part):
                @pl.when(tick == pieces - 1)
                def _():
                    down_copy(pieces - 1, part).wait_recv()

                @pl.when(ready == pieces - 1)
                def _():
                    @pl.loop(0, reach)
                    def _(nearer):
                        serve(place + across * (reach - nearer), 0, pieces - 1, part)

        later_step = tick - pieces - jnp.where(is_end, 0, 2)

        @pl.when((later_step >= 0) & (later_step < (reach + 1) * pieces))
        def _():
            nearer = later_step // pieces
            serve(place + across * (reach - nearer), 1, later_step - nearer * pieces)

        @pl.when(is_inner)
        def _():
            @pl.loop(arrived(tick - 1), arrived(tick))
            def _(index):
                serve_forward(place - across, index)

            outer_step = later_step - 3

            @pl.when((outer_step >= 0) & (outer_step < pieces))
            def _():
                serve(place - across, 1, outer_step)

        @pl.loop(own_arrived(tick - 1), own_arrived(tick))
        def _(index):
            serve_forward(place, index)

        @pl.when(tick == 2 * pieces // 7)
        def _():
            wait_at_end(1)
            make_slope()

        @pl.when(tick == pieces - 5)
        def _():
            wait_at_end(2)
            hidden_grad[...] = jnp.zeros(hidden_grad.shape, jnp.float32)

        @pl.when((tick >= pieces - 5) & (tick < pieces - 2))
        def _():
            third = tick - (pieces - 5)
            most = 2 * spans - 1
            grow_hidden_grad(third * most // 3, (third + 1) * most // 3)

    def wait_sent(sent, semaphore):
        remote(sent, sent, semaphore, back_recv.at[0, 0], partner).wait_send()

    wait_sent(blocks.at[:, rows_of(place)], own_send.at[0])

    @pl.when(is_inner)
    def _():
        wait_sent(blocks.at[:, rows_of(place)], across_send.at[0])
        wait_sent(picked, outer_send.at[0])

    for copy in table_copies:
        copy.wait_send()

    whole_up.wait_send()
    whole_down.wait_send()

    @pl.loop(1, experts)
    def _(ahead):
        target = lax.rem(place + ahead, experts)
        for member in range(2):

            @pl.when(is_end)
            def _(member=member):
                sent = returned.at[member, target, :, pl.ds(0, capacity)]
                wait_sent(sent, back_send.at[member, target])

            @pl.when(is_inner)
            def _(member=member):
                wait_sent(returned.at[member, target], back_send.at[member, target])

    for member, out in enumerate((out_fwd, out_bwd)):
        remote(
            final.at[member],
            final.at[member],
            shift_send.at[member],
            shift_recv.at[member],
            partner,
        ).wait_send()
        remote(
            out, out, shift_send.at[member], shift_recv.at[member], partner
        ).wait_recv()


def store_kernel(fwd, bwd, out_fwd, out_bwd, sems):
    parts = sems.shape[1]
    rows = fwd.shape[0] // parts
    copies = []
    for member, (source, target) in enumerate(((fwd, out_fwd), (bwd, out_bwd))):
        for part in range(parts):
            here = pl.ds(part * rows, rows)
            copies.append(
                pltpu.make_async_copy(
                    source.at[here], target.at[here], sems.at[member, part]
                )
            )
    for copy in copies:
        copy.start()
    for copy in copies:
        copy.wait()


def line_path(
    x_fwd,
    routes_fwd,
    affinity_fwd,
    x_bwd,
    grad_bwd,
    routes_bwd,
    affinity_bwd,
    up_weight,
    down_weight,
):
    devices = lax.axis_size("expert")
    sections = lax.axis_size("section")
    experts = devices // 2
    tokens, width = x_fwd.shape[1:]
    top_count = routes_fwd.shape[2]
    units = up_weight.shape[2]
    capacity = 3 * tokens * top_count // devices
    wide = piece_width(width)
    cut = wide // 2
    pieces = width // cut
    spans = width // wide
    rows = experts * tokens
    bf16, f32 = jnp.bfloat16, jnp.float32
    dma = pltpu.SemaphoreType.DMA
    in_vmem = pl.BlockSpec(memory_space=pltpu.VMEM)
    anywhere = pl.BlockSpec(memory_space=pl.ANY)
    outs = pl.pallas_call(
        functools.partial(line_kernel, (sections, experts, tokens, capacity, pieces, cut, wide)),
        name="expert_line",
        out_shape=[pltpu.VMEM((tokens, width), bf16)] * 2,
        in_specs=[anywhere] * 9,
        out_specs=[in_vmem] * 2,
        scratch_shapes=[
            pltpu.VMEM((2, top_count, tokens), jnp.int32),
            pltpu.VMEM((2, top_count, tokens), f32),
            pltpu.VMEM((3, rows, width), bf16),
            pltpu.VMEM((2, width, units), bf16),
            pltpu.VMEM((2, units, width), bf16),
            pltpu.VMEM((experts, 4 * experts, tokens), f32),
            pltpu.VMEM((rows, units), f32),
            pltpu.VMEM((2, rows, units), f32),
            pltpu.VMEM((2, rows, units), f32),
            pltpu.VMEM((2, rows, units), bf16),
            pltpu.VMEM((2, rows, units), bf16),
            pltpu.VMEM((2, experts + 1, pieces, tokens, cut), bf16),
            pltpu.VMEM((2, pieces, tokens, cut), bf16),
            pltpu.VMEM((3, experts - 1, capacity, width), bf16),
            pltpu.VMEM((2, experts, tokens, tokens), bf16),
            pltpu.VMEM((tokens, cut), f32),
            dma((6,)),
            dma((4,)),
            dma((experts - 1,)),
            dma((experts,)),
            dma((1,)),
            dma((1,)),
            dma((1,)),
            dma((3, experts, 2)),
            dma((1,)),
            dma((1,)),
            dma((1,)),
            dma((pieces + 1,)),
            dma((2, experts)),
            dma((experts + 1, pieces)),
            dma((2, pieces + 1)),
            dma((2,)),
            dma((2,)),
        ],
        compiler_params=pltpu.CompilerParams(
            collective_id=0, has_side_effects=True, vmem_limit_bytes=56 << 20
        ),
    )(
        routes_fwd[0].T,
        affinity_fwd[0].T,
        routes_bwd[0].T,
        affinity_bwd[0].T,
        x_fwd[0],
        x_bwd[0],
        grad_bwd[0],
        up_weight[0],
        down_weight[0],
    )
    stored = pl.pallas_call(
        store_kernel,
        name="store_outputs",
        out_shape=[jax.ShapeDtypeStruct((tokens, width), bf16)] * 2,
        in_specs=[in_vmem] * 2,
        out_specs=[anywhere] * 2,
        scratch_shapes=[dma((2, 4))],
    )(*[pltpu.with_memory_space_constraint(out, pltpu.VMEM) for out in outs])
    return tuple(out[None] for out in stored)


def piece_width(width):
    for wide in (512, 256):
        if width % wide == 0 and width >= 4 * wide:
            return wide
    return 0


def per_device(*args):
    experts = lax.axis_size("expert") // 2
    tokens, width = args[0].shape[1:]
    if experts == 4 and tokens == 128 and piece_width(width):
        return line_path(*args)
    return general_path(*args)


def solution(mesh):
    in_specs = (
        P("section", "expert", None),
        P("section", "expert", None),
        P("section", "expert", None),
        P("section", "expert", None),
        P("section", "expert", None),
        P("section", "expert", None),
        P("section", "expert", None),
        P("section", None, "expert"),
        P("section", "expert", None),
    )
    out_specs = (P("section", "expert", None), P("section", "expert", None))
    return jax.shard_map(
        per_device, mesh=mesh, in_specs=in_specs, out_specs=out_specs, check_vma=False
    )
```

```python
import functools

import jax
import jax.numpy as jnp
from jax import lax
from jax.experimental import pallas as pl
from jax.experimental.pallas import tpu as pltpu
from jax.sharding import PartitionSpec as P

AGAINST_ROWS = (((1,), (1,)), ((), ()))


def from_partner_2(block, axis, apart):
    count = lax.axis_size(axis)
    route = []
    for low in range(count):
        high = low | 1 << apart
        if high != low and high < count:
            route += [(low, high), (high, low)]
    return lax.ppermute(block, axis, route)


def shifted(shard, axis, by):
    size = lax.axis_size(axis)
    return lax.ppermute(shard, axis, [(i, (i + by) % size) for i in range(size)])


def silu_grad(values):
    sigma = jax.nn.sigmoid(values)
    return sigma * (1.0 + values * (1.0 - sigma))


def slot_table(routes, experts, capacity):
    flat_routes = routes.reshape(-1)
    entries = flat_routes.shape[0]
    onehot = (flat_routes[:, None] == jnp.arange(experts, dtype=jnp.int32)[None, :]).astype(
        jnp.int32
    )
    before = jnp.cumsum(onehot, 0) - onehot
    position = jnp.sum(before * onehot, 1)
    slot_of = flat_routes * capacity + position
    source = (
        jnp.full((experts * capacity,), entries, jnp.int32)
        .at[slot_of]
        .set(jnp.arange(entries, dtype=jnp.int32))
    )
    return (slot_of, source)


def serve_rows(received, up_half, down_half):
    sources = received.shape[0]
    slots = received.shape[2]
    model_width = received.shape[3]
    row_count = sources * slots
    rows_fwd = received[:, 0].reshape(row_count, model_width)
    rows_saved = received[:, 1].reshape(row_count, model_width)
    rows_grad = received[:, 2].reshape(row_count, model_width)
    against_rows = (((1,), (1,)), ((), ()))
    hidden = jax.nn.silu(jnp.dot(rows_fwd, up_half, preferred_element_type=jnp.float32)).astype(
        jnp.bfloat16
    )
    part_fwd = jnp.dot(hidden, down_half, preferred_element_type=jnp.float32).astype(jnp.bfloat16)
    pre_act = jnp.dot(rows_saved, up_half, preferred_element_type=jnp.float32)
    hidden_grad = lax.dot_general(
        rows_grad, down_half, against_rows, preferred_element_type=jnp.float32
    )
    pre_grad = (hidden_grad * silu_grad(pre_act)).astype(jnp.bfloat16)
    part_bwd = lax.dot_general(
        pre_grad, up_half, against_rows, preferred_element_type=jnp.float32
    ).astype(jnp.bfloat16)
    return jnp.stack(
        [
            part_fwd.reshape(sources, slots, model_width),
            part_bwd.reshape(sources, slots, model_width),
        ],
        1,
    )


def combine(inputs, routed_rows, affinity):
    tokens = inputs.shape[0]
    top_count = affinity.shape[1]
    weights = affinity / jnp.sum(affinity, -1, keepdims=True)
    routed = routed_rows.reshape(tokens, top_count, inputs.shape[1]).astype(jnp.float32)
    return (inputs.astype(jnp.float32) + jnp.sum(weights[..., None] * routed, 1)).astype(
        jnp.bfloat16
    )


def general_path(
    x_fwd,
    routes_fwd,
    affinity_fwd,
    x_bwd,
    grad_bwd,
    routes_bwd,
    affinity_bwd,
    up_weight,
    down_weight,
):
    devices = lax.axis_size("expert")
    experts = devices // 2
    tokens = x_fwd.shape[1]
    model_width = x_fwd.shape[2]
    top_count = routes_fwd.shape[2]
    capacity = 3 * tokens * top_count // devices
    half_slots = capacity // 2
    up_half = up_weight[0]
    down_half = down_weight[0]
    slot_fwd, source_fwd = slot_table(routes_fwd[0], experts, capacity)
    slot_bwd, source_bwd = slot_table(routes_bwd[0], experts, capacity)
    zero_row = jnp.zeros((1, model_width), jnp.bfloat16)
    row_table = jnp.concatenate([x_fwd[0], zero_row, x_bwd[0], zero_row, grad_bwd[0], zero_row], 0)
    stride = tokens + 1
    token_fwd = (source_fwd // top_count).reshape(experts, capacity)
    token_bwd = (source_bwd // top_count).reshape(experts, capacity)
    gather_index = jnp.stack([token_fwd, token_bwd + stride, token_bwd + 2 * stride], 1)
    send_index = (
        gather_index.reshape(experts, 3, 2, half_slots)
        .transpose(0, 2, 1, 3)
        .reshape(devices, 3, half_slots)
    )
    outgoing = row_table[send_index]
    received = lax.all_to_all(outgoing, "expert", split_axis=0, concat_axis=0, tiled=True)
    partner = from_partner_2(received, "expert", 0)
    result = serve_rows(jnp.concatenate([received, partner], 2), up_half, down_half)
    piece_slots = received.shape[2]
    from_partner = from_partner_2(result[:, :, piece_slots:], "expert", 0)
    summed = (
        result[:, :, :piece_slots].astype(jnp.float32) + from_partner.astype(jnp.float32)
    ).astype(jnp.bfloat16)
    returned = lax.all_to_all(summed, "expert", split_axis=0, concat_axis=0, tiled=True)
    flat_back = returned.reshape(-1, model_width)

    def back_index(slot_of, member):
        expert_id = slot_of // capacity
        within = slot_of % capacity
        return (
            (2 * expert_id + within // half_slots) * 2 + member
        ) * half_slots + within % half_slots

    index_fwd = back_index(slot_fwd, 0)
    index_bwd = back_index(slot_bwd, 1)
    layer_out = combine(x_fwd[0], flat_back[index_fwd], affinity_fwd[0])
    input_grad = combine(grad_bwd[0], flat_back[index_bwd], affinity_bwd[0])
    fwd_next = shifted(layer_out[None], "section", 1)
    bwd_next = shifted(input_grad[None], "section", -1)
    return (fwd_next, bwd_next)


def line_kernel(
    sizes,
    routes_fwd,
    affinity_fwd,
    routes_bwd,
    affinity_bwd,
    x_fwd,
    x_bwd,
    grad_bwd,
    up,
    down,
    out_fwd,
    out_bwd,
    routes,
    affinities,
    blocks,
    ups,
    downs,
    tables,
    total,
    slope,
    hidden_grad,
    hidden,
    pre_grad,
    returned,
    final,
    picked,
    expand,
    piece,
    local_sem,
    small_sem,
    table_send,
    table_recv,
    own_send,
    across_send,
    outer_send,
    block_recv,
    up_send,
    up_recv,
    down_send,
    down_recv,
    back_send,
    back_recv,
    forward_recv,
    shift_send,
    shift_recv,
):
    sections, experts, tokens, capacity, pieces, cut, wide = sizes
    spans = pieces * cut // wide
    half_rows = tokens // 2
    section = lax.axis_index("section")
    device = lax.axis_index("expert")
    place, side = device // 2, device % 2
    last = experts - 1
    is_inner = (place > 0) & (place < last)
    is_end = (place == 0) | (place == last)
    across = jnp.where(place < experts // 2, 1, -1)
    reach = jnp.where(is_end, last, last - 1)

    def at_place(where):
        return {"expert": where * 2 + side}

    def remote(src, dst, send, recv, target):
        return pltpu.make_async_remote_copy(
            src_ref=src,
            dst_ref=dst,
            send_sem=send,
            recv_sem=recv,
            device_id=target,
            device_id_type=pl.DeviceIdType.MESH,
        )

    partner = {"expert": place * 2 + 1 - side}
    next_section = {"section": lax.rem(section + 1, sections)}
    previous_section = {"section": lax.rem(section + sections - 1, sections)}

    barrier = pltpu.get_barrier_semaphore()

    def greet(peer):
        pl.semaphore_signal(
            barrier, inc=1, device_id=peer, device_id_type=pl.DeviceIdType.MESH
        )

    for peer in (partner, next_section, previous_section, at_place(place + across)):
        greet(peer)

    @pl.when(is_inner)
    def _():
        greet(at_place(place - across))


    def rows_of(origin):
        return pl.ds(pl.multiple_of(origin * tokens, tokens), tokens)

    def half_of(origin, half):
        return pl.ds(pl.multiple_of(origin * tokens + half * half_rows, half_rows), half_rows)

    def columns_of(index):
        return pl.ds(pl.multiple_of(index * cut, cut), cut)

    def span_of(index):
        return pl.ds(pl.multiple_of(index * wide, wide), wide)

    small = [
        pltpu.make_async_copy(source, target, small_sem.at[index])
        for index, (source, target) in enumerate(
            (
                (routes_fwd, routes.at[0]),
                (affinity_fwd, affinities.at[0]),
                (routes_bwd, routes.at[1]),
                (affinity_bwd, affinities.at[1]),
            )
        )
    ]
    for copy in small:
        copy.start()
    first_rows, other_rows = pl.ds(0, wide), pl.ds(wide, up.shape[0] - wide)
    local = [
        pltpu.make_async_copy(source, target, local_sem.at[index])
        for index, (source, target) in enumerate(
            (
                (x_fwd, blocks.at[0, rows_of(place)]),
                (up.at[first_rows], ups.at[0, first_rows]),
                (x_bwd, blocks.at[1, rows_of(place)]),
                (grad_bwd, blocks.at[2, rows_of(place)]),
                (up.at[other_rows], ups.at[0, other_rows]),
                (down, downs.at[0]),
            )
        )
    ]
    local[0].start()
    local[1].start()
    row_id = lax.broadcasted_iota(jnp.int32, (tokens, tokens), 0)
    lane_id = lax.broadcasted_iota(jnp.int32, (tokens, tokens), 1)
    later = jnp.where(row_id < lane_id, 1.0, 0.0).astype(jnp.bfloat16)
    expert_id = row_id[:16]
    for copy in small:
        copy.wait()
    for member in range(2):
        weights = affinities[member] / jnp.sum(affinities[member], 0, keepdims=True)
        share = jnp.zeros(expert_id.shape, jnp.float32)
        named = jnp.zeros(expert_id.shape, jnp.float32)
        for choice in range(routes.shape[1]):
            same = routes[member, choice : choice + 1, :] == expert_id
            share += jnp.where(same, weights[choice : choice + 1, :], 0.0)
            named += jnp.where(same, 1.0, 0.0)
        rank = jnp.dot(named.astype(jnp.bfloat16), later, preferred_element_type=jnp.float32)
        rank = jnp.where(named > 0.5, rank, -1.0)
        base = member * 2 * experts
        tables[place, base : base + experts, :] = share[:experts]
        tables[place, base + experts : base + 2 * experts, :] = rank[:experts]

    pl.semaphore_wait(barrier, jnp.where(is_end, 4, 5))
    def table_copy(origin, way, order):
        return remote(
            tables.at[origin],
            tables.at[origin],
            table_send.at[order],
            table_recv.at[origin],
            at_place(place + way),
        )

    def wait_table(origin):
        table_copy(origin, across, 0).wait_recv()

    routes_of_tables = (
        (place, -across),
        (place - across, across),
        (place + across, -across),
        (place + 2 * across, -across),
    )

    def pass_table(order):
        origin, way = routes_of_tables[order]
        if order:
            wait_table(origin)
        table_copy(origin, way, 1 + order).start()

    table_copy(place, across, 0).start()

    @pl.when(is_inner)
    def _():
        pass_table(0)

    def own_copy(stream, half):
        return remote(
            blocks.at[stream, half_of(place, half)],
            blocks.at[stream, half_of(place, half)],
            own_send.at[0],
            block_recv.at[stream, place, half],
            at_place(place + across),
        )

    def send_own(stream):
        for half in range(2):
            own_copy(stream, half).start()

    def wait_half(stream, origin, half):
        block = blocks.at[stream, half_of(origin, half)]
        remote(
            block, block, own_send.at[0], block_recv.at[stream, origin, half], partner
        ).wait_recv()

    def across_copy(stream, half):
        origin = place - across
        block = blocks.at[stream, half_of(origin, half)]
        return remote(
            block,
            block,
            across_send.at[0],
            block_recv.at[stream, origin, half],
            at_place(place + across),
        )

    def send_across(stream, half):
        @pl.when(is_inner)
        def _():
            wait_half(stream, place - across, half)
            across_copy(stream, half).start()

    def outer_copy(stream, steps):
        origin = place + across * steps
        return remote(
            picked.at[stream, steps],
            blocks.at[stream, pl.ds(pl.multiple_of(origin * tokens, tokens), capacity)],
            outer_send.at[0],
            block_recv.at[stream, origin, 0],
            at_place(place - across),
        )

    def table_row(member, kind, origin, expert):
        return tables[origin, pl.ds((member * 2 + kind) * experts + expert, 1), :]

    def send_outer(stream, steps):
        @pl.when(is_inner)
        def _():
            origin = place + across * steps
            if steps:
                for half in range(2):
                    wait_half(stream, origin, half)
            ranks = table_row(min(stream, 1), 1, origin, place - across)
            slots = lax.broadcasted_iota(jnp.int32, (capacity, tokens), 0).astype(jnp.float32)
            pick = jnp.where(slots == ranks, 1.0, 0.0).astype(jnp.bfloat16)

            @pl.loop(0, spans)
            def _(index):
                picked[stream, steps, :, span_of(index)] = jnp.dot(
                    pick,
                    blocks[stream, rows_of(origin), span_of(index)],
                    preferred_element_type=jnp.float32,
                ).astype(jnp.bfloat16)

            outer_copy(stream, steps).start()

    def wait_at_end(stream):
        @pl.when(is_end)
        def _():
            for steps in range(1, experts):
                origin = place + across * steps
                landed = blocks.at[
                    stream, pl.ds(pl.multiple_of(origin * tokens, tokens), capacity)
                ]
                remote(
                    landed,
                    landed,
                    own_send.at[0],
                    block_recv.at[stream, origin, 0],
                    partner,
                ).wait_recv()

    def up_copy(index):
        rows = span_of(index)
        return remote(
            up.at[rows], ups.at[1, rows], up_send.at[0], up_recv.at[0], partner
        )

    def split_piece(index, part):
        if part is None:
            return cut, pl.ds(0, cut), columns_of(index), index
        width = cut // 2
        start = pl.multiple_of(part * width, width)
        columns = pl.ds(pl.multiple_of(index * cut + part * width, width), width)
        return width, pl.ds(start, width), columns, index + part

    def down_copy(index, part=None):
        _, _, columns, order = split_piece(index, part)
        return remote(
            down.at[:, columns],
            downs.at[1, :, columns],
            down_send.at[0],
            down_recv.at[order],
            partner,
        )

    first_up = remote(
        ups.at[0, first_rows], ups.at[1, first_rows], up_send.at[0], up_recv.at[0], partner
    )
    whole_up = remote(up, ups.at[1], up_send.at[0], up_recv.at[0], partner)
    whole_down = remote(down, downs.at[1], down_send.at[0], down_recv.at[0], partner)
    local[0].wait()
    send_own(0)
    local[1].wait()
    first_up.start()

    @pl.loop(1, spans)
    def _(index):
        up_copy(index).start()

    @pl.loop(0, pieces - 1)
    def _(index):
        down_copy(index).start()

    for part in range(2):
        down_copy(pieces - 1, part).start()

    local[2].start()
    local[3].start()

    @pl.when(is_end)
    def _():
        for stream in range(3):
            for steps in range(1, experts):
                start = pl.multiple_of((place + across * steps) * tokens + capacity, 16)
                blocks[stream, pl.ds(start, tokens - capacity), :] = jnp.zeros(
                    (tokens - capacity, blocks.shape[2]), jnp.bfloat16
                )

    def wait_tables():
        @pl.when(is_inner)
        def _():
            pass_table(3)

        @pl.when(is_end)
        def _():
            for steps in range(1, experts):
                wait_table(place + across * steps)

    def make_expand():
        @pl.when(is_inner)
        def _():
            @pl.loop(0, 2 * experts)
            def _(index):
                member = index // experts
                origin = index - member * experts
                ranks = table_row(member, 1, origin, place - across)
                rank = jnp.sum(jnp.where(row_id == lane_id, ranks, 0.0), 1, keepdims=True)
                expand[member, origin] = jnp.where(
                    lane_id.astype(jnp.float32) == rank, 1.0, 0.0
                ).astype(jnp.bfloat16)

    def weight_of(member, origin):
        packed = is_end & (origin != place)
        slots = row_id.astype(jnp.float32)
        lanes = lane_id[:1].astype(jnp.float32)
        ranks = jnp.where(packed, table_row(member, 1, origin, place), lanes)
        share = table_row(member, 0, origin, place)
        return jnp.sum(jnp.where(slots == ranks, share, 0.0), 1, keepdims=True)

    def project(stream, half):
        total[...] = jnp.zeros(total.shape, jnp.float32)

        @pl.loop(0, spans)
        def _(index):
            total[...] += jnp.dot(
                blocks[stream, :, span_of(index)],
                ups[half, span_of(index), :],
                preferred_element_type=jnp.float32,
            )

    def make_hidden():
        @pl.loop(0, 2)
        def _(half):
            project(0, half)

            @pl.loop(0, experts)
            def _(origin):
                act = total[rows_of(origin), :]
                hidden[half, rows_of(origin), :] = (
                    act / (1.0 + jnp.exp(-act)) * weight_of(0, origin)
                ).astype(jnp.bfloat16)

    def make_slope():
        @pl.loop(0, 2)
        def _(half):
            project(1, half)

            @pl.loop(0, experts)
            def _(origin):
                weight = weight_of(1, origin)
                act = total[rows_of(origin), :]
                sigma = 1.0 / (1.0 + jnp.exp(-act))
                slope[half, rows_of(origin), :] = (
                    sigma * (1.0 + act * (1.0 - sigma))
                ) * weight

    def add_hidden_grad(half, index):
        hidden_grad[half] += lax.dot_general(
            blocks[2, :, span_of(index)],
            downs[half, :, span_of(index)],
            AGAINST_ROWS,
            preferred_element_type=jnp.float32,
        )

    def grow_hidden_grad(low, high):
        @pl.loop(low, high)
        def _(index):
            half = index // spans
            add_hidden_grad(half, index - half * spans)

    def make_pre_grad():
        add_hidden_grad(1, spans - 1)

        @pl.loop(0, 2 * experts)
        def _(index):
            half = index // experts
            origin = index - half * experts
            rows = rows_of(origin)
            pre_grad[half, rows, :] = (
                hidden_grad[half, rows, :] * slope[half, rows, :]
            ).astype(jnp.bfloat16)

    def serve(target, member, index, part=None):
        width, lanes, columns, order = split_piece(index, part)
        rows = rows_of(target)
        sum_ref = piece.at[:, pl.ds(0, width)]

        def arrival(slot, group):
            if member == 0:
                return forward_recv.at[group, order]
            return back_recv.at[slot, index]

        def back_copy(count):
            way = jnp.where(target > place, 1, -1)
            there = place + way
            slot = jnp.where((way < 0) & (target == there), experts, target)
            return remote(
                returned.at[member, target, index, pl.ds(0, count), lanes],
                returned.at[member, slot, index, pl.ds(0, count), lanes],
                back_send.at[member, target],
                arrival(slot, jnp.where(is_end, 0, 1)),
                at_place(there),
            )

        def wait_bytes(landed, semaphore):
            remote(landed, landed, back_send.at[member, 0], semaphore, partner).wait_recv()

        def wait_group(group, count, height):
            landed = returned.at[0, pl.ds(0, count), index, pl.ds(0, height), lanes]
            wait_bytes(landed, arrival(None, group))

        def wait_back(slot, height):
            landed = returned.at[member, slot, index, pl.ds(0, height), lanes]
            wait_bytes(landed, arrival(slot, None))

        def add_back(slot):
            if member == 0:

                @pl.when(is_end)
                def _():
                    wait_group(1, 1, tokens)

                @pl.when(is_inner & (target != place))
                def _():
                    wait_group(1, 2, tokens)

            else:
                wait_back(slot, tokens)
            sum_ref[...] += returned[member, slot, index, :, lanes].astype(jnp.float32)

        def add_packed_back(slot):
            if member == 0:

                @pl.when(target == place + across * reach)
                def _():
                    wait_group(0, last, capacity)

            else:
                wait_back(slot, capacity)
            sum_ref[...] += jnp.dot(
                expand[member, target, :, :capacity],
                returned[member, slot, index, pl.ds(0, capacity), lanes],
                preferred_element_type=jnp.float32,
            )

        def forward_product(half):
            return jnp.dot(
                hidden[half, rows, :],
                downs[half, :, columns],
                preferred_element_type=jnp.float32,
            )

        def backward_product(half):
            return lax.dot_general(
                pre_grad[half, rows, :],
                ups[half, columns, :],
                AGAINST_ROWS,
                preferred_element_type=jnp.float32,
            )

        if member == 0:
            sum_ref[...] = forward_product(0) + forward_product(1)
        else:
            sum_ref[...] = backward_product(0) + backward_product(1)

        @pl.when(target != place)
        def _():
            @pl.when(is_end)
            def _():
                returned[member, target, index, :, lanes] = sum_ref[...].astype(jnp.bfloat16)
                back_copy(capacity).start()

            @pl.when(is_inner)
            def _():
                beyond = (target - place) * across > 0

                @pl.when(beyond)
                def _():
                    add_packed_back(target)

                @pl.when(jnp.logical_not(beyond))
                def _():
                    add_back(target)

                returned[member, target, index, :, lanes] = sum_ref[...].astype(jnp.bfloat16)
                back_copy(tokens).start()

        @pl.when(target == place)
        def _():
            @pl.when(is_inner)
            def _():
                add_packed_back(jnp.where(across > 0, place, experts))

            add_back(jnp.where(across > 0, experts, place))
            final[member, index, :, lanes] = (
                sum_ref[...] + blocks[2 * member, rows, columns].astype(jnp.float32)
            ).astype(jnp.bfloat16)
            remote(
                final.at[member, index, :, lanes],
                (out_fwd, out_bwd)[member].at[:, columns],
                shift_send.at[member],
                shift_recv.at[member],
                (next_section, previous_section)[member],
            ).start()

    def serve_last(target):
        @pl.loop(0, 2)
        def _(part):
            serve(target, 0, pieces - 1, part)

    def serve_forward(target, index):
        @pl.when(index < pieces - 1)
        def _():
            serve(target, 0, index)

        @pl.when(index == pieces - 1)
        def _():
            serve_last(target)

    @pl.when(is_inner)
    def _():
        pass_table(1)
        pass_table(2)

    send_outer(0, 0)
    local[2].wait()
    send_outer(1, 0)
    send_across(0, 0)
    send_across(0, 1)
    send_own(1)
    local[4].start()
    local[5].start()
    wait_tables()
    send_outer(0, 1)
    send_across(1, 0)
    send_outer(0, 2)
    send_across(1, 1)
    local[3].wait()
    send_own(2)
    send_outer(2, 0)
    send_outer(1, 1)
    send_across(2, 0)
    send_across(2, 1)
    make_expand()
    send_outer(1, 2)
    local[4].wait()
    local[5].wait()
    wait_at_end(0)
    whole_up.wait_recv()

    make_hidden()

    gate = pieces // 2

    def arrived(tick):
        steady = jnp.where(tick < pieces, tick - 2, jnp.maximum(pieces - 3, tick - 6))
        return jnp.clip(jnp.minimum(2 * (tick - gate), steady), 0, pieces)

    def own_arrived(tick):
        early = arrived(jnp.minimum(tick, pieces - 3) - 2)
        at_end = jnp.where(tick < (1 + last) * pieces, early, pieces)
        return jnp.where(is_end, at_end, arrived(tick))

    @pl.loop(0, (2 + last) * pieces)
    def _(tick):
        @pl.when(tick < pieces - 1)
        def _():
            down_copy(tick).wait_recv()

        @pl.when(tick == pieces // 7)
        def _():
            send_outer(2, 1)

        @pl.when(tick == 3 * pieces // 7)
        def _():
            send_outer(2, 2)

        @pl.when(tick == pieces)
        def _():
            make_pre_grad()

        ready = jnp.where(is_end, tick, tick - 1)

        @pl.when((ready >= 0) & (ready < pieces - 1))
        def _():
            @pl.loop(0, reach)
            def _(nearer):
                serve(place + across * (reach - nearer), 0, ready)

        @pl.when((tick == pieces - 1) | (tick == pieces))
        def _():
            @pl.loop(0, 2)
            def _(part):
                @pl.when(tick == pieces - 1)
                def _():
                    down_copy(pieces - 1, part).wait_recv()

                @pl.when(ready == pieces - 1)
                def _():
                    @pl.loop(0, reach)
                    def _(nearer):
                        serve(place + across * (reach - nearer), 0, pieces - 1, part)

        later_step = tick - pieces - jnp.where(is_end, 0, 2)

        @pl.when((later_step >= 0) & (later_step < (reach + 1) * pieces))
        def _():
            nearer = later_step // pieces
            serve(place + across * (reach - nearer), 1, later_step - nearer * pieces)

        @pl.when(is_inner)
        def _():
            @pl.loop(arrived(tick - 1), arrived(tick))
            def _(index):
                serve_forward(place - across, index)

            outer_step = later_step - 3

            @pl.when((outer_step >= 0) & (outer_step < pieces))
            def _():
                serve(place - across, 1, outer_step)

        @pl.loop(own_arrived(tick - 1), own_arrived(tick))
        def _(index):
            serve_forward(place, index)

        @pl.when(tick == 2 * pieces // 7)
        def _():
            wait_at_end(1)
            make_slope()

        @pl.when(tick == pieces - 5)
        def _():
            wait_at_end(2)
            hidden_grad[...] = jnp.zeros(hidden_grad.shape, jnp.float32)

        @pl.when((tick >= pieces - 5) & (tick < pieces - 2))
        def _():
            third = tick - (pieces - 5)
            most = 2 * spans - 1
            grow_hidden_grad(third * most // 3, (third + 1) * most // 3)

    def wait_sent(sent, semaphore):
        remote(sent, sent, semaphore, back_recv.at[0, 0], partner).wait_send()

    wait_sent(blocks.at[:, rows_of(place)], own_send.at[0])

    @pl.when(is_inner)
    def _():
        wait_sent(blocks.at[:, rows_of(place)], across_send.at[0])
        wait_sent(picked, outer_send.at[0])

    table_copy(place, across, 0).wait_send()

    @pl.when(is_inner)
    def _():
        for order, (origin, way) in enumerate(routes_of_tables):
            table_copy(origin, way, 1 + order).wait_send()

    whole_up.wait_send()
    whole_down.wait_send()

    @pl.loop(1, experts)
    def _(ahead):
        target = lax.rem(place + ahead, experts)
        for member in range(2):

            @pl.when(is_end)
            def _(member=member):
                sent = returned.at[member, target, :, pl.ds(0, capacity)]
                wait_sent(sent, back_send.at[member, target])

            @pl.when(is_inner)
            def _(member=member):
                wait_sent(returned.at[member, target], back_send.at[member, target])

    for member, out in enumerate((out_fwd, out_bwd)):
        remote(
            final.at[member],
            final.at[member],
            shift_send.at[member],
            shift_recv.at[member],
            partner,
        ).wait_send()
        remote(
            out, out, shift_send.at[member], shift_recv.at[member], partner
        ).wait_recv()


def store_kernel(fwd, bwd, out_fwd, out_bwd, sems):
    parts = sems.shape[1]
    rows = fwd.shape[0] // parts
    copies = []
    for member, (source, target) in enumerate(((fwd, out_fwd), (bwd, out_bwd))):
        for part in range(parts):
            here = pl.ds(part * rows, rows)
            copies.append(
                pltpu.make_async_copy(
                    source.at[here], target.at[here], sems.at[member, part]
                )
            )
    for copy in copies:
        copy.start()
    for copy in copies:
        copy.wait()


def line_path(
    x_fwd,
    routes_fwd,
    affinity_fwd,
    x_bwd,
    grad_bwd,
    routes_bwd,
    affinity_bwd,
    up_weight,
    down_weight,
):
    devices = lax.axis_size("expert")
    sections = lax.axis_size("section")
    experts = devices // 2
    tokens, width = x_fwd.shape[1:]
    top_count = routes_fwd.shape[2]
    units = up_weight.shape[2]
    capacity = 3 * tokens * top_count // devices
    wide = piece_width(width)
    cut = wide // 2
    pieces = width // cut
    spans = width // wide
    rows = experts * tokens
    bf16, f32 = jnp.bfloat16, jnp.float32
    dma = pltpu.SemaphoreType.DMA
    in_vmem = pl.BlockSpec(memory_space=pltpu.VMEM)
    anywhere = pl.BlockSpec(memory_space=pl.ANY)
    outs = pl.pallas_call(
        functools.partial(line_kernel, (sections, experts, tokens, capacity, pieces, cut, wide)),
        name="expert_line",
        out_shape=[pltpu.VMEM((tokens, width), bf16)] * 2,
        in_specs=[anywhere] * 9,
        out_specs=[in_vmem] * 2,
        scratch_shapes=[
            pltpu.VMEM((2, top_count, tokens), jnp.int32),
            pltpu.VMEM((2, top_count, tokens), f32),
            pltpu.VMEM((3, rows, width), bf16),
            pltpu.VMEM((2, width, units), bf16),
            pltpu.VMEM((2, units, width), bf16),
            pltpu.VMEM((experts, 4 * experts, tokens), f32),
            pltpu.VMEM((rows, units), f32),
            pltpu.VMEM((2, rows, units), f32),
            pltpu.VMEM((2, rows, units), f32),
            pltpu.VMEM((2, rows, units), bf16),
            pltpu.VMEM((2, rows, units), bf16),
            pltpu.VMEM((2, experts + 1, pieces, tokens, cut), bf16),
            pltpu.VMEM((2, pieces, tokens, cut), bf16),
            pltpu.VMEM((3, experts - 1, capacity, width), bf16),
            pltpu.VMEM((2, experts, tokens, tokens), bf16),
            pltpu.VMEM((tokens, cut), f32),
            dma((6,)),
            dma((4,)),
            dma((5,)),
            dma((experts,)),
            dma((1,)),
            dma((1,)),
            dma((1,)),
            dma((3, experts, 2)),
            dma((1,)),
            dma((1,)),
            dma((1,)),
            dma((pieces + 1,)),
            dma((2, experts)),
            dma((experts + 1, pieces)),
            dma((2, pieces + 1)),
            dma((2,)),
            dma((2,)),
        ],
        compiler_params=pltpu.CompilerParams(
            collective_id=0, has_side_effects=True, vmem_limit_bytes=56 << 20
        ),
    )(
        routes_fwd[0].T,
        affinity_fwd[0].T,
        routes_bwd[0].T,
        affinity_bwd[0].T,
        x_fwd[0],
        x_bwd[0],
        grad_bwd[0],
        up_weight[0],
        down_weight[0],
    )
    stored = pl.pallas_call(
        store_kernel,
        name="store_outputs",
        out_shape=[jax.ShapeDtypeStruct((tokens, width), bf16)] * 2,
        in_specs=[in_vmem] * 2,
        out_specs=[anywhere] * 2,
        scratch_shapes=[dma((2, 4))],
    )(*[pltpu.with_memory_space_constraint(out, pltpu.VMEM) for out in outs])
    return tuple(out[None] for out in stored)


def piece_width(width):
    for wide in (512, 256):
        if width % wide == 0 and width >= 4 * wide:
            return wide
    return 0


def per_device(*args):
    experts = lax.axis_size("expert") // 2
    tokens, width = args[0].shape[1:]
    if experts == 4 and tokens == 128 and piece_width(width):
        return line_path(*args)
    return general_path(*args)


def solution(mesh):
    in_specs = (
        P("section", "expert", None),
        P("section", "expert", None),
        P("section", "expert", None),
        P("section", "expert", None),
        P("section", "expert", None),
        P("section", "expert", None),
        P("section", "expert", None),
        P("section", None, "expert"),
        P("section", "expert", None),
    )
    out_specs = (P("section", "expert", None), P("section", "expert", None))
    return jax.shard_map(
        per_device, mesh=mesh, in_specs=in_specs, out_specs=out_specs, check_vma=False
    )
```

```python
import functools

import jax
import jax.numpy as jnp
from jax import lax
from jax.experimental import pallas as pl
from jax.experimental.pallas import tpu as pltpu
from jax.sharding import PartitionSpec as P

AGAINST_ROWS = (((1,), (1,)), ((), ()))


def from_partner_2(block, axis, apart):
    count = lax.axis_size(axis)
    route = []
    for low in range(count):
        high = low | 1 << apart
        if high != low and high < count:
            route += [(low, high), (high, low)]
    return lax.ppermute(block, axis, route)


def shifted(shard, axis, by):
    size = lax.axis_size(axis)
    return lax.ppermute(shard, axis, [(i, (i + by) % size) for i in range(size)])


def silu_grad(values):
    sigma = jax.nn.sigmoid(values)
    return sigma * (1.0 + values * (1.0 - sigma))


def slot_table(routes, experts, capacity):
    flat_routes = routes.reshape(-1)
    entries = flat_routes.shape[0]
    onehot = (flat_routes[:, None] == jnp.arange(experts, dtype=jnp.int32)[None, :]).astype(
        jnp.int32
    )
    before = jnp.cumsum(onehot, 0) - onehot
    position = jnp.sum(before * onehot, 1)
    slot_of = flat_routes * capacity + position
    source = (
        jnp.full((experts * capacity,), entries, jnp.int32)
        .at[slot_of]
        .set(jnp.arange(entries, dtype=jnp.int32))
    )
    return (slot_of, source)


def serve_rows(received, up_half, down_half):
    sources = received.shape[0]
    slots = received.shape[2]
    model_width = received.shape[3]
    row_count = sources * slots
    rows_fwd = received[:, 0].reshape(row_count, model_width)
    rows_saved = received[:, 1].reshape(row_count, model_width)
    rows_grad = received[:, 2].reshape(row_count, model_width)
    against_rows = (((1,), (1,)), ((), ()))
    hidden = jax.nn.silu(jnp.dot(rows_fwd, up_half, preferred_element_type=jnp.float32)).astype(
        jnp.bfloat16
    )
    part_fwd = jnp.dot(hidden, down_half, preferred_element_type=jnp.float32).astype(jnp.bfloat16)
    pre_act = jnp.dot(rows_saved, up_half, preferred_element_type=jnp.float32)
    hidden_grad = lax.dot_general(
        rows_grad, down_half, against_rows, preferred_element_type=jnp.float32
    )
    pre_grad = (hidden_grad * silu_grad(pre_act)).astype(jnp.bfloat16)
    part_bwd = lax.dot_general(
        pre_grad, up_half, against_rows, preferred_element_type=jnp.float32
    ).astype(jnp.bfloat16)
    return jnp.stack(
        [
            part_fwd.reshape(sources, slots, model_width),
            part_bwd.reshape(sources, slots, model_width),
        ],
        1,
    )


def combine(inputs, routed_rows, affinity):
    tokens = inputs.shape[0]
    top_count = affinity.shape[1]
    weights = affinity / jnp.sum(affinity, -1, keepdims=True)
    routed = routed_rows.reshape(tokens, top_count, inputs.shape[1]).astype(jnp.float32)
    return (inputs.astype(jnp.float32) + jnp.sum(weights[..., None] * routed, 1)).astype(
        jnp.bfloat16
    )


def general_path(
    x_fwd,
    routes_fwd,
    affinity_fwd,
    x_bwd,
    grad_bwd,
    routes_bwd,
    affinity_bwd,
    up_weight,
    down_weight,
):
    devices = lax.axis_size("expert")
    experts = devices // 2
    tokens = x_fwd.shape[1]
    model_width = x_fwd.shape[2]
    top_count = routes_fwd.shape[2]
    capacity = 3 * tokens * top_count // devices
    half_slots = capacity // 2
    up_half = up_weight[0]
    down_half = down_weight[0]
    slot_fwd, source_fwd = slot_table(routes_fwd[0], experts, capacity)
    slot_bwd, source_bwd = slot_table(routes_bwd[0], experts, capacity)
    zero_row = jnp.zeros((1, model_width), jnp.bfloat16)
    row_table = jnp.concatenate([x_fwd[0], zero_row, x_bwd[0], zero_row, grad_bwd[0], zero_row], 0)
    stride = tokens + 1
    token_fwd = (source_fwd // top_count).reshape(experts, capacity)
    token_bwd = (source_bwd // top_count).reshape(experts, capacity)
    gather_index = jnp.stack([token_fwd, token_bwd + stride, token_bwd + 2 * stride], 1)
    send_index = (
        gather_index.reshape(experts, 3, 2, half_slots)
        .transpose(0, 2, 1, 3)
        .reshape(devices, 3, half_slots)
    )
    outgoing = row_table[send_index]
    received = lax.all_to_all(outgoing, "expert", split_axis=0, concat_axis=0, tiled=True)
    partner = from_partner_2(received, "expert", 0)
    result = serve_rows(jnp.concatenate([received, partner], 2), up_half, down_half)
    piece_slots = received.shape[2]
    from_partner = from_partner_2(result[:, :, piece_slots:], "expert", 0)
    summed = (
        result[:, :, :piece_slots].astype(jnp.float32) + from_partner.astype(jnp.float32)
    ).astype(jnp.bfloat16)
    returned = lax.all_to_all(summed, "expert", split_axis=0, concat_axis=0, tiled=True)
    flat_back = returned.reshape(-1, model_width)

    def back_index(slot_of, member):
        expert_id = slot_of // capacity
        within = slot_of % capacity
        return (
            (2 * expert_id + within // half_slots) * 2 + member
        ) * half_slots + within % half_slots

    index_fwd = back_index(slot_fwd, 0)
    index_bwd = back_index(slot_bwd, 1)
    layer_out = combine(x_fwd[0], flat_back[index_fwd], affinity_fwd[0])
    input_grad = combine(grad_bwd[0], flat_back[index_bwd], affinity_bwd[0])
    fwd_next = shifted(layer_out[None], "section", 1)
    bwd_next = shifted(input_grad[None], "section", -1)
    return (fwd_next, bwd_next)


def line_kernel(
    sizes,
    routes_fwd,
    affinity_fwd,
    routes_bwd,
    affinity_bwd,
    x_fwd,
    x_bwd,
    grad_bwd,
    up,
    down,
    out_fwd,
    out_bwd,
    routes,
    affinities,
    blocks,
    ups,
    downs,
    tables,
    total,
    slope,
    hidden_grad,
    hidden,
    pre_grad,
    returned,
    final,
    picked,
    expand,
    piece,
    local_sem,
    small_sem,
    table_send,
    table_recv,
    own_send,
    across_send,
    outer_send,
    block_recv,
    up_send,
    up_recv,
    down_send,
    down_recv,
    back_send,
    back_recv,
    forward_recv,
    shift_send,
    shift_recv,
):
    sections, experts, tokens, capacity, pieces, cut, wide = sizes
    spans = pieces * cut // wide
    half_rows = tokens // 2
    section = lax.axis_index("section")
    device = lax.axis_index("expert")
    place, side = device // 2, device % 2
    last = experts - 1
    is_inner = (place > 0) & (place < last)
    is_end = (place == 0) | (place == last)
    across = jnp.where(place < experts // 2, 1, -1)
    reach = jnp.where(is_end, last, last - 1)
    farthest = place + across * reach

    def at_place(where):
        return {"expert": where * 2 + side}

    def remote(src, dst, send, recv, target):
        return pltpu.make_async_remote_copy(
            src_ref=src,
            dst_ref=dst,
            send_sem=send,
            recv_sem=recv,
            device_id=target,
            device_id_type=pl.DeviceIdType.MESH,
        )

    partner = {"expert": place * 2 + 1 - side}
    next_section = {"section": lax.rem(section + 1, sections)}
    previous_section = {"section": lax.rem(section + sections - 1, sections)}

    barrier = pltpu.get_barrier_semaphore()

    def greet(peer):
        pl.semaphore_signal(
            barrier, inc=1, device_id=peer, device_id_type=pl.DeviceIdType.MESH
        )

    for peer in (partner, next_section, previous_section, at_place(place + across)):
        greet(peer)

    @pl.when(is_inner)
    def _():
        greet(at_place(place - across))


    def rows_of(origin):
        return pl.ds(pl.multiple_of(origin * tokens, tokens), tokens)

    def half_of(origin, half):
        return pl.ds(pl.multiple_of(origin * tokens + half * half_rows, half_rows), half_rows)

    def columns_of(index):
        return pl.ds(pl.multiple_of(index * cut, cut), cut)

    def span_of(index):
        return pl.ds(pl.multiple_of(index * wide, wide), wide)

    small = [
        pltpu.make_async_copy(source, target, small_sem.at[index])
        for index, (source, target) in enumerate(
            (
                (routes_fwd, routes.at[0]),
                (affinity_fwd, affinities.at[0]),
                (routes_bwd, routes.at[1]),
                (affinity_bwd, affinities.at[1]),
            )
        )
    ]
    for copy in small:
        copy.start()
    first_rows, other_rows = pl.ds(0, wide), pl.ds(wide, up.shape[0] - wide)
    local = [
        pltpu.make_async_copy(source, target, local_sem.at[index])
        for index, (source, target) in enumerate(
            (
                (x_fwd, blocks.at[0, rows_of(place)]),
                (up.at[first_rows], ups.at[0, first_rows]),
                (x_bwd, blocks.at[1, rows_of(place)]),
                (grad_bwd, blocks.at[2, rows_of(place)]),
                (up.at[other_rows], ups.at[0, other_rows]),
                (down, downs.at[0]),
            )
        )
    ]
    local[0].start()
    local[1].start()
    row_id = lax.broadcasted_iota(jnp.int32, (tokens, tokens), 0)
    lane_id = lax.broadcasted_iota(jnp.int32, (tokens, tokens), 1)
    later = jnp.where(row_id < lane_id, 1.0, 0.0).astype(jnp.bfloat16)
    expert_id = row_id[:16]
    for copy in small:
        copy.wait()
    for member in range(2):
        weights = affinities[member] / jnp.sum(affinities[member], 0, keepdims=True)
        share = jnp.zeros(expert_id.shape, jnp.float32)
        named = jnp.zeros(expert_id.shape, jnp.float32)
        for choice in range(routes.shape[1]):
            same = routes[member, choice : choice + 1, :] == expert_id
            share += jnp.where(same, weights[choice : choice + 1, :], 0.0)
            named += jnp.where(same, 1.0, 0.0)
        rank = jnp.dot(named.astype(jnp.bfloat16), later, preferred_element_type=jnp.float32)
        rank = jnp.where(named > 0.5, rank, -1.0)
        base = member * 2 * experts
        tables[place, base : base + experts, :] = share[:experts]
        tables[place, base + experts : base + 2 * experts, :] = rank[:experts]

    pl.semaphore_wait(barrier, jnp.where(is_end, 4, 5))
    def table_copy(origin, way, order):
        return remote(
            tables.at[origin],
            tables.at[origin],
            table_send.at[order],
            table_recv.at[origin],
            at_place(place + way),
        )

    def wait_table(origin):
        table_copy(origin, across, 0).wait_recv()

    routes_of_tables = (
        (place, -across),
        (place - across, across),
        (place + across, -across),
        (place + 2 * across, -across),
    )

    def pass_table(order):
        origin, way = routes_of_tables[order]
        if order:
            wait_table(origin)
        table_copy(origin, way, 1 + order).start()

    table_copy(place, across, 0).start()

    @pl.when(is_inner)
    def _():
        pass_table(0)

    def own_copy(stream, half):
        return remote(
            blocks.at[stream, half_of(place, half)],
            blocks.at[stream, half_of(place, half)],
            own_send.at[0],
            block_recv.at[stream, place, half],
            at_place(place + across),
        )

    def send_own(stream):
        for half in range(2):
            own_copy(stream, half).start()

    def wait_half(stream, origin, half):
        block = blocks.at[stream, half_of(origin, half)]
        remote(
            block, block, own_send.at[0], block_recv.at[stream, origin, half], partner
        ).wait_recv()

    def across_copy(stream, half):
        origin = place - across
        block = blocks.at[stream, half_of(origin, half)]
        return remote(
            block,
            block,
            across_send.at[0],
            block_recv.at[stream, origin, half],
            at_place(place + across),
        )

    def send_across(stream, half):
        @pl.when(is_inner)
        def _():
            wait_half(stream, place - across, half)
            across_copy(stream, half).start()

    def outer_copy(stream, steps):
        origin = place + across * steps
        return remote(
            picked.at[stream, steps],
            blocks.at[stream, pl.ds(pl.multiple_of(origin * tokens, tokens), capacity)],
            outer_send.at[0],
            block_recv.at[stream, origin, 0],
            at_place(place - across),
        )

    def table_row(member, kind, origin, expert):
        return tables[origin, pl.ds((member * 2 + kind) * experts + expert, 1), :]

    def send_outer(stream, steps):
        @pl.when(is_inner)
        def _():
            origin = place + across * steps
            if steps:
                for half in range(2):
                    wait_half(stream, origin, half)
            ranks = table_row(min(stream, 1), 1, origin, place - across)
            slots = lax.broadcasted_iota(jnp.int32, (capacity, tokens), 0).astype(jnp.float32)
            pick = jnp.where(slots == ranks, 1.0, 0.0).astype(jnp.bfloat16)

            @pl.loop(0, spans)
            def _(index):
                picked[stream, steps, :, span_of(index)] = jnp.dot(
                    pick,
                    blocks[stream, rows_of(origin), span_of(index)],
                    preferred_element_type=jnp.float32,
                ).astype(jnp.bfloat16)

            outer_copy(stream, steps).start()

    def wait_at_end(stream):
        @pl.when(is_end)
        def _():
            for steps in range(1, experts):
                origin = place + across * steps
                landed = blocks.at[
                    stream, pl.ds(pl.multiple_of(origin * tokens, tokens), capacity)
                ]
                remote(
                    landed,
                    landed,
                    own_send.at[0],
                    block_recv.at[stream, origin, 0],
                    partner,
                ).wait_recv()

    def up_copy(index):
        rows = span_of(index)
        return remote(
            up.at[rows], ups.at[1, rows], up_send.at[0], up_recv.at[0], partner
        )

    def split_piece(index, part):
        if part is None:
            return cut, pl.ds(0, cut), columns_of(index), index
        width = cut // 2
        start = pl.multiple_of(part * width, width)
        columns = pl.ds(pl.multiple_of(index * cut + part * width, width), width)
        return width, pl.ds(start, width), columns, index + part

    def down_copy(index, part=None):
        _, _, columns, order = split_piece(index, part)
        return remote(
            down.at[:, columns],
            downs.at[1, :, columns],
            down_send.at[0],
            down_recv.at[order],
            partner,
        )

    first_up = remote(
        ups.at[0, first_rows], ups.at[1, first_rows], up_send.at[0], up_recv.at[0], partner
    )
    whole_up = remote(up, ups.at[1], up_send.at[0], up_recv.at[0], partner)
    whole_down = remote(down, downs.at[1], down_send.at[0], down_recv.at[0], partner)
    local[0].wait()
    send_own(0)
    local[1].wait()
    first_up.start()

    @pl.loop(1, spans)
    def _(index):
        up_copy(index).start()

    @pl.loop(0, pieces - 1)
    def _(index):
        down_copy(index).start()

    for part in range(2):
        down_copy(pieces - 1, part).start()

    local[2].start()
    local[3].start()

    @pl.when(is_end)
    def _():
        for stream in range(3):
            for steps in range(1, experts):
                start = pl.multiple_of((place + across * steps) * tokens + capacity, 16)
                blocks[stream, pl.ds(start, tokens - capacity), :] = jnp.zeros(
                    (tokens - capacity, blocks.shape[2]), jnp.bfloat16
                )

    def wait_tables():
        @pl.when(is_inner)
        def _():
            pass_table(3)

        @pl.when(is_end)
        def _():
            for steps in range(1, experts):
                wait_table(place + across * steps)

    def make_expand():
        @pl.when(is_inner)
        def _():
            @pl.loop(0, 2 * experts)
            def _(index):
                member = index // experts
                origin = index - member * experts
                ranks = table_row(member, 1, origin, place - across)
                rank = jnp.sum(jnp.where(row_id == lane_id, ranks, 0.0), 1, keepdims=True)
                expand[member, origin] = jnp.where(
                    lane_id.astype(jnp.float32) == rank, 1.0, 0.0
                ).astype(jnp.bfloat16)

    def weight_of(member, origin):
        packed = is_end & (origin != place)
        slots = row_id.astype(jnp.float32)
        lanes = lane_id[:1].astype(jnp.float32)
        ranks = jnp.where(packed, table_row(member, 1, origin, place), lanes)
        share = table_row(member, 0, origin, place)
        return jnp.sum(jnp.where(slots == ranks, share, 0.0), 1, keepdims=True)

    def project(stream, half):
        total[...] = jnp.zeros(total.shape, jnp.float32)

        @pl.loop(0, spans)
        def _(index):
            total[...] += jnp.dot(
                blocks[stream, :, span_of(index)],
                ups[half, span_of(index), :],
                preferred_element_type=jnp.float32,
            )

    def make_hidden():
        @pl.loop(0, 2)
        def _(half):
            project(0, half)

            @pl.loop(0, experts)
            def _(origin):
                act = total[rows_of(origin), :]
                hidden[half, rows_of(origin), :] = (
                    act / (1.0 + jnp.exp(-act)) * weight_of(0, origin)
                ).astype(jnp.bfloat16)

    def make_slope():
        @pl.loop(0, 2)
        def _(half):
            project(1, half)

            @pl.loop(0, experts)
            def _(origin):
                weight = weight_of(1, origin)
                act = total[rows_of(origin), :]
                sigma = 1.0 / (1.0 + jnp.exp(-act))
                slope[half, rows_of(origin), :] = (
                    sigma * (1.0 + act * (1.0 - sigma))
                ) * weight

    def add_hidden_grad(half, index):
        hidden_grad[half] += lax.dot_general(
            blocks[2, :, span_of(index)],
            downs[half, :, span_of(index)],
            AGAINST_ROWS,
            preferred_element_type=jnp.float32,
        )

    def grow_hidden_grad(low, high):
        @pl.loop(low, high)
        def _(index):
            half = index // spans
            add_hidden_grad(half, index - half * spans)

    def make_pre_grad():
        add_hidden_grad(1, spans - 1)

        @pl.loop(0, 2 * experts)
        def _(index):
            half = index // experts
            origin = index - half * experts
            rows = rows_of(origin)
            pre_grad[half, rows, :] = (
                hidden_grad[half, rows, :] * slope[half, rows, :]
            ).astype(jnp.bfloat16)

    def serve(target, member, index, part=None):
        width, lanes, columns, order = split_piece(index, part)
        rows = rows_of(target)
        sum_ref = piece.at[:, pl.ds(0, width)]

        def arrival(slot, group):
            if member == 0:
                return forward_recv.at[group, order]
            return back_recv.at[slot, index]

        def back_copy(count):
            way = jnp.where(target > place, 1, -1)
            there = place + way
            slot = jnp.where((way < 0) & (target == there), experts, target)
            return remote(
                returned.at[member, target, index, pl.ds(0, count), lanes],
                returned.at[member, slot, index, pl.ds(0, count), lanes],
                back_send.at[member, target],
                arrival(slot, jnp.where(is_end, jnp.where(target == farthest, 0, 2), 1)),
                at_place(there),
            )

        def wait_bytes(landed, semaphore):
            remote(landed, landed, back_send.at[member, 0], semaphore, partner).wait_recv()

        def wait_group(group, count, height):
            landed = returned.at[0, pl.ds(0, count), index, pl.ds(0, height), lanes]
            wait_bytes(landed, arrival(None, group))

        def wait_back(slot, height):
            landed = returned.at[member, slot, index, pl.ds(0, height), lanes]
            wait_bytes(landed, arrival(slot, None))

        def add_back(slot):
            if member == 0:

                @pl.when(is_end)
                def _():
                    wait_group(1, 1, tokens)

                @pl.when(is_inner & (target != place))
                def _():
                    wait_group(1, 2, tokens)

            else:
                wait_back(slot, tokens)
            sum_ref[...] += returned[member, slot, index, :, lanes].astype(jnp.float32)

        def add_packed_back(slot):
            if member == 0:

                @pl.when(target == farthest)
                def _():
                    wait_group(0, 1, capacity)

                @pl.when(target == place + across)
                def _():
                    wait_group(2, last - 1, capacity)

            else:
                wait_back(slot, capacity)
            sum_ref[...] += jnp.dot(
                expand[member, target, :, :capacity],
                returned[member, slot, index, pl.ds(0, capacity), lanes],
                preferred_element_type=jnp.float32,
            )

        def forward_product(half):
            return jnp.dot(
                hidden[half, rows, :],
                downs[half, :, columns],
                preferred_element_type=jnp.float32,
            )

        def backward_product(half):
            return lax.dot_general(
                pre_grad[half, rows, :],
                ups[half, columns, :],
                AGAINST_ROWS,
                preferred_element_type=jnp.float32,
            )

        if member == 0:
            sum_ref[...] = forward_product(0) + forward_product(1)
        else:
            sum_ref[...] = backward_product(0) + backward_product(1)

        @pl.when(target != place)
        def _():
            @pl.when(is_end)
            def _():
                returned[member, target, index, :, lanes] = sum_ref[...].astype(jnp.bfloat16)
                back_copy(capacity).start()

            @pl.when(is_inner)
            def _():
                beyond = (target - place) * across > 0

                @pl.when(beyond)
                def _():
                    add_packed_back(target)

                @pl.when(jnp.logical_not(beyond))
                def _():
                    add_back(target)

                returned[member, target, index, :, lanes] = sum_ref[...].astype(jnp.bfloat16)
                back_copy(tokens).start()

        @pl.when(target == place)
        def _():
            @pl.when(is_inner)
            def _():
                add_packed_back(jnp.where(across > 0, place, experts))

            add_back(jnp.where(across > 0, experts, place))
            final[member, index, :, lanes] = (
                sum_ref[...] + blocks[2 * member, rows, columns].astype(jnp.float32)
            ).astype(jnp.bfloat16)
            remote(
                final.at[member, index, :, lanes],
                (out_fwd, out_bwd)[member].at[:, columns],
                shift_send.at[member],
                shift_recv.at[member],
                (next_section, previous_section)[member],
            ).start()

    def serve_last(target):
        @pl.loop(0, 2)
        def _(part):
            serve(target, 0, pieces - 1, part)

    def serve_forward(target, index):
        @pl.when(index < pieces - 1)
        def _():
            serve(target, 0, index)

        @pl.when(index == pieces - 1)
        def _():
            serve_last(target)

    @pl.when(is_inner)
    def _():
        pass_table(1)
        pass_table(2)

    send_outer(0, 0)
    local[2].wait()
    send_outer(1, 0)
    send_across(0, 0)
    send_across(0, 1)
    send_own(1)
    local[4].start()
    local[5].start()
    wait_tables()
    send_outer(0, 1)
    send_across(1, 0)
    send_outer(0, 2)
    send_across(1, 1)
    local[3].wait()
    send_own(2)
    send_outer(2, 0)
    send_outer(1, 1)
    send_across(2, 0)
    send_across(2, 1)
    make_expand()
    send_outer(1, 2)
    local[4].wait()
    local[5].wait()
    wait_at_end(0)
    whole_up.wait_recv()

    make_hidden()

    gate = pieces // 2

    def arrived(tick):
        steady = jnp.where(tick < pieces, tick - 2, jnp.maximum(pieces - 3, tick - 6))
        return jnp.clip(jnp.minimum(2 * (tick - gate), steady), 0, pieces)

    def own_arrived(tick):
        early = arrived(jnp.minimum(tick, pieces - 3) - 2)
        at_end = jnp.where(tick < (1 + last) * pieces, early, pieces)
        return jnp.where(is_end, at_end, arrived(tick))

    @pl.loop(0, (2 + last) * pieces)
    def _(tick):
        @pl.when(tick < pieces - 1)
        def _():
            down_copy(tick).wait_recv()

        @pl.when(tick == pieces // 7)
        def _():
            send_outer(2, 1)

        @pl.when(tick == 3 * pieces // 7)
        def _():
            send_outer(2, 2)

        @pl.when(tick == pieces)
        def _():
            make_pre_grad()

        ready = jnp.where(is_end, tick, tick - 1)

        @pl.when((ready >= 0) & (ready < pieces - 1))
        def _():
            @pl.loop(0, reach)
            def _(nearer):
                serve(place + across * (reach - nearer), 0, ready)

        @pl.when((tick == pieces - 1) | (tick == pieces))
        def _():
            @pl.loop(0, 2)
            def _(part):
                @pl.when(tick == pieces - 1)
                def _():
                    down_copy(pieces - 1, part).wait_recv()

                @pl.when(ready == pieces - 1)
                def _():
                    @pl.loop(0, reach)
                    def _(nearer):
                        serve(place + across * (reach - nearer), 0, pieces - 1, part)

        later_step = tick - pieces - jnp.where(is_end, 0, 2)

        @pl.when((later_step >= 0) & (later_step < (reach + 1) * pieces))
        def _():
            nearer = later_step // pieces
            serve(place + across * (reach - nearer), 1, later_step - nearer * pieces)

        @pl.when(is_inner)
        def _():
            @pl.loop(arrived(tick - 1), arrived(tick))
            def _(index):
                serve_forward(place - across, index)

            outer_step = later_step - 3

            @pl.when((outer_step >= 0) & (outer_step < pieces))
            def _():
                serve(place - across, 1, outer_step)

        @pl.loop(own_arrived(tick - 1), own_arrived(tick))
        def _(index):
            serve_forward(place, index)

        @pl.when(tick == 2 * pieces // 7)
        def _():
            wait_at_end(1)
            make_slope()

        @pl.when(tick == pieces - 5)
        def _():
            wait_at_end(2)
            hidden_grad[...] = jnp.zeros(hidden_grad.shape, jnp.float32)

        @pl.when((tick >= pieces - 5) & (tick < pieces - 2))
        def _():
            third = tick - (pieces - 5)
            most = 2 * spans - 1
            grow_hidden_grad(third * most // 3, (third + 1) * most // 3)

    def wait_sent(sent, semaphore):
        remote(sent, sent, semaphore, back_recv.at[0, 0], partner).wait_send()

    wait_sent(blocks.at[:, rows_of(place)], own_send.at[0])

    @pl.when(is_inner)
    def _():
        wait_sent(blocks.at[:, rows_of(place)], across_send.at[0])
        wait_sent(picked, outer_send.at[0])

    table_copy(place, across, 0).wait_send()

    @pl.when(is_inner)
    def _():
        for order, (origin, way) in enumerate(routes_of_tables):
            table_copy(origin, way, 1 + order).wait_send()

    whole_up.wait_send()
    whole_down.wait_send()

    @pl.loop(1, experts)
    def _(ahead):
        target = lax.rem(place + ahead, experts)
        for member in range(2):

            @pl.when(is_end)
            def _(member=member):
                sent = returned.at[member, target, :, pl.ds(0, capacity)]
                wait_sent(sent, back_send.at[member, target])

            @pl.when(is_inner)
            def _(member=member):
                wait_sent(returned.at[member, target], back_send.at[member, target])

    for member, out in enumerate((out_fwd, out_bwd)):
        remote(
            final.at[member],
            final.at[member],
            shift_send.at[member],
            shift_recv.at[member],
            partner,
        ).wait_send()
        remote(
            out, out, shift_send.at[member], shift_recv.at[member], partner
        ).wait_recv()


def store_kernel(fwd, bwd, out_fwd, out_bwd, sems):
    parts = sems.shape[1]
    rows = fwd.shape[0] // parts
    copies = []
    for member, (source, target) in enumerate(((fwd, out_fwd), (bwd, out_bwd))):
        for part in range(parts):
            here = pl.ds(part * rows, rows)
            copies.append(
                pltpu.make_async_copy(
                    source.at[here], target.at[here], sems.at[member, part]
                )
            )
    for copy in copies:
        copy.start()
    for copy in copies:
        copy.wait()


def line_path(
    x_fwd,
    routes_fwd,
    affinity_fwd,
    x_bwd,
    grad_bwd,
    routes_bwd,
    affinity_bwd,
    up_weight,
    down_weight,
):
    devices = lax.axis_size("expert")
    sections = lax.axis_size("section")
    experts = devices // 2
    tokens, width = x_fwd.shape[1:]
    top_count = routes_fwd.shape[2]
    units = up_weight.shape[2]
    capacity = 3 * tokens * top_count // devices
    wide = piece_width(width)
    cut = wide // 2
    pieces = width // cut
    spans = width // wide
    rows = experts * tokens
    bf16, f32 = jnp.bfloat16, jnp.float32
    dma = pltpu.SemaphoreType.DMA
    in_vmem = pl.BlockSpec(memory_space=pltpu.VMEM)
    anywhere = pl.BlockSpec(memory_space=pl.ANY)
    outs = pl.pallas_call(
        functools.partial(line_kernel, (sections, experts, tokens, capacity, pieces, cut, wide)),
        name="expert_line",
        out_shape=[pltpu.VMEM((tokens, width), bf16)] * 2,
        in_specs=[anywhere] * 9,
        out_specs=[in_vmem] * 2,
        scratch_shapes=[
            pltpu.VMEM((2, top_count, tokens), jnp.int32),
            pltpu.VMEM((2, top_count, tokens), f32),
            pltpu.VMEM((3, rows, width), bf16),
            pltpu.VMEM((2, width, units), bf16),
            pltpu.VMEM((2, units, width), bf16),
            pltpu.VMEM((experts, 4 * experts, tokens), f32),
            pltpu.VMEM((rows, units), f32),
            pltpu.VMEM((2, rows, units), f32),
            pltpu.VMEM((2, rows, units), f32),
            pltpu.VMEM((2, rows, units), bf16),
            pltpu.VMEM((2, rows, units), bf16),
            pltpu.VMEM((2, experts + 1, pieces, tokens, cut), bf16),
            pltpu.VMEM((2, pieces, tokens, cut), bf16),
            pltpu.VMEM((3, experts - 1, capacity, width), bf16),
            pltpu.VMEM((2, experts, tokens, tokens), bf16),
            pltpu.VMEM((tokens, cut), f32),
            dma((6,)),
            dma((4,)),
            dma((5,)),
            dma((experts,)),
            dma((1,)),
            dma((1,)),
            dma((1,)),
            dma((3, experts, 2)),
            dma((1,)),
            dma((1,)),
            dma((1,)),
            dma((pieces + 1,)),
            dma((2, experts)),
            dma((experts + 1, pieces)),
            dma((3, pieces + 1)),
            dma((2,)),
            dma((2,)),
        ],
        compiler_params=pltpu.CompilerParams(
            collective_id=0, has_side_effects=True, vmem_limit_bytes=56 << 20
        ),
    )(
        routes_fwd[0].T,
        affinity_fwd[0].T,
        routes_bwd[0].T,
        affinity_bwd[0].T,
        x_fwd[0],
        x_bwd[0],
        grad_bwd[0],
        up_weight[0],
        down_weight[0],
    )
    stored = pl.pallas_call(
        store_kernel,
        name="store_outputs",
        out_shape=[jax.ShapeDtypeStruct((tokens, width), bf16)] * 2,
        in_specs=[in_vmem] * 2,
        out_specs=[anywhere] * 2,
        scratch_shapes=[dma((2, 2))],
    )(*[pltpu.with_memory_space_constraint(out, pltpu.VMEM) for out in outs])
    return tuple(out[None] for out in stored)


def piece_width(width):
    for wide in (512, 256):
        if width % wide == 0 and width >= 4 * wide:
            return wide
    return 0


def per_device(*args):
    experts = lax.axis_size("expert") // 2
    tokens, width = args[0].shape[1:]
    if experts == 4 and tokens == 128 and piece_width(width):
        return line_path(*args)
    return general_path(*args)


def solution(mesh):
    in_specs = (
        P("section", "expert", None),
        P("section", "expert", None),
        P("section", "expert", None),
        P("section", "expert", None),
        P("section", "expert", None),
        P("section", "expert", None),
        P("section", "expert", None),
        P("section", None, "expert"),
        P("section", "expert", None),
    )
    out_specs = (P("section", "expert", None), P("section", "expert", None))
    return jax.shard_map(
        per_device, mesh=mesh, in_specs=in_specs, out_specs=out_specs, check_vma=False
    )
```
